256 devices in a mesh: rep: 1, dp: 256 (over x, y, z, core).
Axes of the slice: x: 4, y: 4, z: 8, core: 2. Of those that a mesh axis runs over, the one named last changes fastest.
Arguments:
- x: bfloat16 [256, 1024, 768], P(('rep', 'dp'))
- dy: bfloat16 [256, 1024, 768], P(('rep', 'dp'))
- w_gate: bfloat16 [2, 768, 3072], replicated
- w_up: bfloat16 [2, 768, 3072], replicated
- w_down: bfloat16 [2, 3072, 768], replicated
- m_w_gate: float32 [2, 768, 3072], replicated
- m_w_up: float32 [2, 768, 3072], replicated
- m_w_down: float32 [2, 3072, 768], replicated
- v_w_gate: float32 [2, 768, 3072], replicated
- v_w_up: float32 [2, 768, 3072], replicated
- v_w_down: float32 [2, 3072, 768], replicated
Outputs:
- output 1: bfloat16 [2, 768, 3072], P('rep')
- output 2: bfloat16 [2, 768, 3072], P('rep')
- output 3: bfloat16 [2, 3072, 768], P('rep')
- output 4: float32 [2, 768, 3072], P('rep')
- output 5: float32 [2, 768, 3072], P('rep')
- output 6: float32 [2, 3072, 768], P('rep')
- output 7: float32 [2, 768, 3072], P('rep')
- output 8: float32 [2, 768, 3072], P('rep')
- output 9: float32 [2, 3072, 768], P('rep')
All inputs are finite; a program needn't handle non-finite values.
Results may differ from the reference program's by a relative error of at most 0.022.
Values are sent between devices in bfloat16 or wider.
A program may use at most 768 MiB of HBM per device.

```python
import jax
import jax.numpy as jnp
from jax import lax

SEQUENCES = 256
TOKENS = 1024
D = 768
FF = 3072
LAYERS = 2
NAMES = ("w_gate", "w_up", "w_down")
SHAPES = {"w_gate": (LAYERS, D, FF), "w_up": (LAYERS, D, FF), "w_down": (LAYERS, FF, D)}


def bump(key, n, height):
    away = (jnp.arange(n, dtype=jnp.int32) - jax.random.randint(key, (), 0, n, jnp.int32)) % n
    return jnp.where(away < n // 8, height, 1.0)


def together(key, own, strength):
    shared = jax.random.normal(key, own.shape[1:], jnp.float32)
    return (own + strength * shared) * lax.rsqrt(1 + strength * strength)


def setup_inputs(seed: int = 0, part: int = 0) -> dict:
    kx, kdy, ka, kb, kz, kf, kh, kl, *keys = jax.random.split(jax.random.key(seed), 8 + 3 * len(NAMES))
    kx, kdy, ka, kb = (jax.random.fold_in(k, part) for k in (kx, kdy, ka, kb))
    kw, km, kv = (keys[i::3] for i in range(3))
    shape = (SEQUENCES, TOKENS, D)
    much_x, much_dy = jax.random.uniform(kz, (2,), jnp.float32, 0.0, 1.0)
    loud = 2.0 ** jax.random.uniform(jax.random.fold_in(kz, 1), (), jnp.float32, -1.0, 2.0)
    layers = 2.0 ** jax.random.uniform(kl, (LAYERS, 1, 1), jnp.float32, -1.0, 1.0)
    x = together(ka, jax.random.normal(kx, shape, jnp.float32), much_x) * bump(kf, D, 4.0)
    dy = together(kb, jax.random.normal(kdy, shape, jnp.float32), much_dy)
    drawn = {"x": x.astype(jnp.bfloat16), "dy": (loud * dy * (SEQUENCES * TOKENS) ** -0.5).astype(jnp.bfloat16)}
    for key, name in zip(kw, NAMES, strict=True):
        w = jax.random.normal(key, SHAPES[name], jnp.float32) * SHAPES[name][1] ** -0.5
        drawn[name] = (w * {"w_gate": 1.0, "w_up": bump(kh, FF, 4.0), "w_down": layers}[name]).astype(jnp.bfloat16)
    for key, name in zip(km, NAMES, strict=True):
        drawn[f"m_{name}"] = 0.1 * jax.random.normal(key, SHAPES[name], jnp.float32)
    for key, name in zip(kv, NAMES, strict=True):
        drawn[f"v_{name}"] = jax.random.uniform(key, SHAPES[name], jnp.float32, 0.005, 0.015)
    return drawn


def matmul(a, w):
    return jnp.dot(a, w, preferred_element_type=jnp.float32).astype(jnp.bfloat16)


def normed(h):
    wide = h.astype(jnp.float32)
    scale = lax.rsqrt(jnp.mean(wide**2, -1, keepdims=True) + 1e-6)
    return (wide * scale).astype(jnp.bfloat16)


def layer(h, w):
    a = normed(h)
    gate = jnp.dot(a, w["w_gate"], preferred_element_type=jnp.float32)
    up = jnp.dot(a, w["w_up"], preferred_element_type=jnp.float32)
    return h + matmul((jax.nn.silu(gate) * up).astype(jnp.bfloat16), w["w_down"])


def adamw(w, m, v, g):
    m = 0.9 * m + 0.1 * g
    v = 0.95 * v + 0.05 * g * g
    step = m * lax.rsqrt(v + 1e-8) + 0.1 * w
    return (w - 0.02 * step).astype(jnp.bfloat16), m, v


def clipped(gradients, sum_of_squares, count):
    factor = jnp.minimum(1.0, 0.5 * lax.rsqrt(sum_of_squares / count + 1e-30))
    return [g * factor for g in gradients]


def stack(weights, h):
    return lax.scan(lambda h, w: (layer(h, w), None), h, weights)[0]


def reference(x, dy, w_gate, w_up, w_down, m_w_gate, m_w_up, m_w_down, v_w_gate, v_w_up, v_w_down):
    weights = dict(zip(NAMES, (w_gate, w_up, w_down), strict=True))

    def take(so_far, sequence):
        h, by_y = sequence
        _, back = jax.vjp(lambda w: stack(w, h), weights)
        return jax.tree.map(lambda total, term: total + term.astype(jnp.float32), so_far, back(by_y)[0]), None

    none_yet = {name: jnp.zeros(w.shape, jnp.float32) for name, w in weights.items()}
    by_weights, _ = lax.scan(take, none_yet, (x, dy))
    gradients = [by_weights[name].astype(jnp.bfloat16).astype(jnp.float32) for name in NAMES]
    gradients = clipped(gradients, sum(jnp.sum(g * g) for g in gradients), sum(g.size for g in gradients))
    new = [
        adamw(w.astype(jnp.float32), m, v, g)
        for w, m, v, g in zip((w_gate, w_up, w_down), (m_w_gate, m_w_up, m_w_down), (v_w_gate, v_w_up, v_w_down), gradients, strict=True)
    ]
    return tuple(one[which] for which in range(3) for one in new)
```

```python
import functools

import jax
import jax.numpy as jnp
from jax import lax
from jax.experimental import pallas as pl
from jax.experimental.pallas import tpu as pltpu
from jax.sharding import PartitionSpec as P

NAMES = ("w_gate", "w_up", "w_down")
MESH = pl.DeviceIdType.MESH
NX, NY, NZ = 4, 4, 8
F32, BF16 = jnp.float32, jnp.bfloat16


def matmul(a, w):
    return jnp.dot(a, w, preferred_element_type=jnp.float32).astype(jnp.bfloat16)


def normed(h):
    wide = h.astype(jnp.float32)
    scale = lax.rsqrt(jnp.mean(wide**2, -1, keepdims=True) + 1e-6)
    return (wide * scale).astype(jnp.bfloat16)


def layer(h, w):
    a = normed(h)
    gate = jnp.dot(a, w["w_gate"], preferred_element_type=jnp.float32)
    up = jnp.dot(a, w["w_up"], preferred_element_type=jnp.float32)
    return h + matmul((jax.nn.silu(gate) * up).astype(jnp.bfloat16), w["w_down"])


def adamw(w, m, v, g):
    m = 0.9 * m + 0.1 * g
    v = 0.95 * v + 0.05 * g * g
    step = m * lax.rsqrt(v + 1e-8) + 0.1 * w
    return (w - 0.02 * step).astype(jnp.bfloat16), m, v


def div(a, b):
    return lax.div(a, jnp.int32(b))


def rem(a, b):
    return lax.rem(a, jnp.int32(b))


def first(s, i):
    return i + 1 - 2 * rem(i, 2) if s == 0 else 3 - i


def second(s, i):
    return first(1 - s, i)


def half(s, i):
    return rem(div(i + 1, 2), 2) if s == 0 else div(i, 2)


def part(s, i):
    return div(i, 2) if s == 0 else rem(i, 2)


def quarter(s, i):
    return 2 * half(s, i) + part(s, i)


class Xfer:
    def __init__(self, link, nbytes, src, dst, dev):
        self.link, self.nbytes, self.src, self.dst, self.dev = link, nbytes, src, dst, dev
        self.copy = None
        self.arrives = None


class Event:
    def __init__(self, waits, pre, work, cost, sends):
        self.waits, self.pre, self.work, self.cost, self.sends = waits, pre, work, cost, sends
        self.done = None


RATE = {"ici": 46.0e3, "d2d": 500.0e3}
DELAY = 2.2


def order_of(events):
    links, left, out, clock = {}, list(events), [], 0.0
    while left:
        best = None
        for e in left:
            if any(p.done is None for p in e.pre) or any(t.arrives is None for t in e.waits):
                continue
            ready = max([p.done for p in e.pre] + [t.arrives for t in e.waits] + [0.0])
            if best is None or max(ready, clock) < best[0]:
                best = (max(ready, clock), e)
        clock, e = best
        clock += e.cost
        e.done = clock
        for t in e.sends:
            begin = max(clock, links.get(t.link, 0.0))
            links[t.link] = begin + t.nbytes / RATE["d2d" if t.link == "d2d" else "ici"]
            t.arrives = links[t.link] + DELAY
        left.remove(e)
        out.append(e)
    return out, clock


def comm_kernel(ru, cu, *refs):
    (g1, u1, d1, g0, u0, d0, gu_out, dn_out, sq_out, own_ab, own_c, p_ab, p_c, r1, r2, r3, r4, rz, rc, rx1, rx2, ry, f_ab, acc, nz, ny, nx, nc,
     send_sem, recv_sem, load_sem, keep_sem) = refs
    grads = ((g0, u0, d0), (g1, u1, d1))
    me = lax.axis_index("dp")
    core = rem(me, 2)
    z = rem(div(me, 2), NZ)
    y = rem(div(me, 2 * NZ), NY)
    x = div(me, 2 * NZ * NY)
    other = 1 - core

    def at(x_=None, y_=None, z_=None, c_=None):
        pick = lambda v, d: d if v is None else v
        return ((pick(x_, x) * NY + pick(y_, y)) * NZ + pick(z_, z)) * 2 + pick(c_, core)

    R = lambda start, size: pl.ds(pl.multiple_of(start, 16), size)
    C = lambda start, size: pl.ds(pl.multiple_of(start, 128), size)

    barrier = pltpu.get_barrier_semaphore()
    peers = [at(c_=other)]
    peers += [at(x_=rem(x + d, NX)) for d in range(1, NX)]
    peers += [at(y_=rem(y + d, NY)) for d in range(1, NY)]
    peers += [at(z_=rem(z + d, NZ)) for d in range(1, NZ)]

    S = 4 * ru
    HC, QC = 4 * cu, 2 * cu
    DC = 2 * cu
    ZR = 2 * ru

    loads = {}
    for l in (1, 0):
        for c in range(2):
            loads[l, c] = pltpu.make_async_copy(grads[l][c].at[R(core * 2 * S, 2 * S), :], own_ab.at[l, c], load_sem.at[l, c])
        loads[l, 2] = pltpu.make_async_copy(grads[l][2].at[R(core * 16 * ZR, 16 * ZR), :], own_c.at[l], load_sem.at[l, 2])
        for k in range(3):
            loads[l, k].start()
    for p in peers:
        pl.semaphore_signal(barrier, inc=1, device_id={"dp": p}, device_id_type=MESH)
    pl.semaphore_wait(barrier, len(peers))

    xfers, events = [], []

    def xfer(link, rows, cols, src, dst, dev, hops=1):
        t = Xfer(link, rows * cols * 2 * hops, src, dst, dev)
        xfers.append(t)
        return t

    def event(waits, pre, work, cost, sends):
        e = Event(waits, pre, work, cost, sends)
        events.append(e)
        return e

    def total(dst, srcs, rows, cols):
        wide = min(cols, 2 * cu)
        across = cols // wide

        def block(i, _):
            r, c = (div(i, across), rem(i, across)) if across > 1 else (i, 0)

            def window(a):
                ref, lead, row, col = a
                return ref.at[(*lead, R(row + r * 16, 16), C(col + c * wide, wide))]

            s = window(srcs[0])[...].astype(F32)
            for a in srcs[1:]:
                s = s + window(a)[...].astype(F32)
            window(dst)[...] = s.astype(BF16)
            return 0

        lax.fori_loop(0, rows // 16 * across, block, 0)

    def add_squares(ref, lead, scale):
        for r in range(0, ru, 16):
            v = ref[(*lead, pl.ds(r, 16), slice(None))].astype(F32)
            v = v * v
            s = acc[...]
            for a in range(0, 16, 8):
                for b in range(0, cu, 128):
                    s = s + (scale * v[a : a + 8, b : b + 128])
            acc[...] = s

    adds = lambda rows, cols, n: rows * cols * n / 2.2e6 + 0.15

    acc[...] = jnp.zeros_like(acc)
    loaded = set()

    def need(*keys):
        for k in keys:
            if k not in loaded:
                loaded.add(k)
                loads[k].wait()

    d2d = {}
    firsts, seconds = [], []
    for l in (1, 0):
        for s in range(2):
            for c in range(2):
                ri = x if c == 0 else y
                for which, where, to in (("send", 1 - half(s, ri), firsts), ("keep", half(s, ri), seconds)):
                    row = s * S + where * 2 * ru
                    t = xfer("d2d", 2 * ru, 8 * cu,
                             functools.partial(lambda l, c, row: grads[l][c].at[R(other * 2 * S + row, 2 * ru), :], l, c, row),
                             functools.partial(lambda l, c, row: p_ab.at[l, c, R(row, 2 * ru), :], l, c, row), at(c_=other))
                    d2d[which, l, c, s] = t
                    to.append(t)
        for s in range(2):
            t = xfer("d2d", 8 * ZR, DC,
                     functools.partial(lambda l, s: grads[l][2].at[R(other * 16 * ZR + s * 8 * ZR, 8 * ZR), :], l, s),
                     functools.partial(lambda l, s: p_c.at[l, pl.ds(s * 8 * ZR, 8 * ZR), :], l, s), at(c_=other))
            d2d["c", l, s] = t
            firsts.append(t)
        firsts += seconds
        seconds = []
    begin = event([], [], lambda: None, 0.0, firsts)

    pieces_done = {}
    arrived = []
    for l in (1, 0):
        ends = []
        for c in range(2):
            ri, ci = (x, y) if c == 0 else (y, x)
            rax, cax = ("x", "y") if c == 0 else ("y", "x")
            rdev = (lambda i: at(x_=i)) if c == 0 else (lambda i: at(y_=i))
            cdev = (lambda i: at(y_=i)) if c == 0 else (lambda i: at(x_=i))
            for s in range(2):
                e1, e2 = ("e1", "e2") if s == 0 else ("e2", "e1")
                b1, b2, c1, c2 = half(s, ri), part(s, ri), half(s, ci), part(s, ci)
                out_rows, keep_rows = s * S + (1 - b1) * 2 * ru, s * S + b1 * 2 * ru
                q_out, q_keep = keep_rows + (1 - b2) * ru, keep_rows + b2 * ru
                k1 = functools.partial
                t1 = xfer(rax + e1, 2 * ru, 8 * cu, k1(lambda l, c, a: p_ab.at[l, c, R(a, 2 * ru), :], l, c, out_rows),
                          k1(lambda l, c, s: r1.at[l, c, s], l, c, s), rdev(first(s, ri)))
                t2 = xfer(rax + e2, ru, 8 * cu, k1(lambda l, c, a: p_ab.at[l, c, R(a, ru), :], l, c, q_out),
                          k1(lambda l, c, s: r2.at[l, c, s], l, c, s), rdev(second(s, ri)))
                t3 = xfer(cax + e1, ru, HC, k1(lambda l, c, a, b: p_ab.at[l, c, R(a, ru), C(b, HC)], l, c, q_keep, (1 - c1) * HC),
                          k1(lambda l, c, s: r3.at[l, c, s], l, c, s), cdev(first(s, ci)))
                t4 = xfer(cax + e2, ru, QC, k1(lambda l, c, a, b: p_ab.at[l, c, R(a, ru), C(b, QC)], l, c, q_keep, c1 * HC + (1 - c2) * QC),
                          k1(lambda l, c, s: r4.at[l, c, s], l, c, s), cdev(second(s, ci)))

                def w1(l=l, c=c, s=s, out_rows=out_rows):
                    need((l, c))
                    here = ((l, c), out_rows, 0)
                    total((p_ab, *here), [(p_ab, *here), (own_ab, *here)], 2 * ru, 8 * cu)

                def w2(l=l, c=c, s=s, q_out=q_out, b2=b2):
                    here = ((l, c), q_out, 0)
                    total((p_ab, *here), [(p_ab, *here), (own_ab, *here), (r1, (l, c, s), (1 - b2) * ru, 0)], ru, 8 * cu)

                def rest(cols_at, cols, more, l=l, c=c, s=s, q_keep=q_keep, b2=b2, c1=c1):
                    here = ((l, c), q_keep, cols_at)
                    srcs = [(p_ab, *here), (own_ab, *here), (r1, (l, c, s), b2 * ru, cols_at), (r2, (l, c, s), 0, cols_at)]
                    if more >= 1:
                        srcs.append((r3, (l, c, s), 0, cols_at - c1 * HC))
                    if more >= 2:
                        srcs.append((r4, (l, c, s), 0, 0))
                    total((p_ab, *here), srcs, ru, cols)

                w3 = functools.partial(rest, (1 - c1) * HC, HC, 0)
                w4 = functools.partial(rest, c1 * HC + (1 - c2) * QC, QC, 1)
                w5 = functools.partial(rest, c1 * HC + c2 * QC, QC, 2)
                ea = event([d2d["send", l, c, s]], [begin], w1, adds(2 * ru, 8 * cu, 2), [t1])
                eb = event([d2d["keep", l, c, s], t1], [ea], w2, adds(ru, 8 * cu, 3), [t2])
                ec = event([t2], [eb], w3, adds(ru, HC, 4), [t3])
                ed = event([t3], [ec], w4, adds(ru, QC, 5), [t4])
                ends.append(event([t4], [ed], w5, adds(ru, QC, 6), []))

        def piece(zz):
            c, k = div(zz, 4), rem(zz, 4)
            s, h = div(k, 2), rem(k, 2)
            qx = quarter(0, x) + s * (quarter(1, x) - quarter(0, x))
            qy = quarter(0, y) + s * (quarter(1, y) - quarter(0, y))
            q, cq = qx + c * (qy - qx), qy + c * (qx - qy)
            return c, s * S + q * ru, cq * QC + h * cu

        tz = []
        for d in range(1, NZ):
            zz = rem(z + d, NZ)
            c, a, b = piece(zz)
            tz.append(xfer("z+" if d <= 4 else "z-", ru, cu, functools.partial(lambda l, c, a, b: p_ab.at[l, c, R(a, ru), C(b, cu)], l, c, a, b),
                           functools.partial(lambda l, d: rz.at[l, d - 1], l, d), at(z_=zz), hops=min(d, NZ - d)))
        ez = event([], ends, lambda: None, 0.05, tz)
        mc, ma, mb = piece(z)
        keep_ab = pltpu.make_async_copy(f_ab.at[l], gu_out.at[mc, l, R(core * 2 * S + ma, ru), C(mb, cu)], keep_sem.at[l, 0])

        def wz(l=l, mc=mc, ma=ma, mb=mb, keep_ab=keep_ab):
            total((f_ab, (l,), 0, 0), [(p_ab, (l, mc), ma, mb)] + [(rz, (l, d), 0, 0) for d in range(NZ - 1)], ru, cu)
            add_squares(f_ab, (l,), 1.0)
            keep_ab.start()

        ta = [xfer("z+" if d <= 4 else "z-", ru, cu, functools.partial(lambda l: f_ab.at[l], l),
                   functools.partial(lambda l, c, a, b: gu_out.at[c, l, R(core * 2 * S + a, ru), C(b, cu)], l, mc, ma, mb), at(z_=rem(z + d, NZ)), hops=min(d, NZ - d))
              for d in range(1, NZ)]
        ef = event(tz, [ez], wz, 0.5, ta)
        pieces_done[l] = [ef]
        eg0 = event(ta, [ef], keep_ab.wait, 0.1, [])
        for c in range(2):
            ri, ci = (x, y) if c == 0 else (y, x)
            rax, cax = ("x", "y") if c == 0 else ("y", "x")
            rdev = (lambda i: at(x_=i)) if c == 0 else (lambda i: at(y_=i))
            cdev = (lambda i: at(y_=i)) if c == 0 else (lambda i: at(x_=i))
            for s in range(2):
                e1, e2 = ("e1", "e2") if s == 0 else ("e2", "e1")
                base = core * 2 * S + s * S

                def same(link, rows, cols, row, col, dev, l=l, c=c, base=base):
                    ref = functools.partial(lambda l, c, row, col, rows, cols: gu_out.at[c, l, R(row, rows), C(col, cols)], l, c, base + row, col, rows, cols)
                    return xfer(link, rows, cols, ref, ref, dev)

                q, q2 = quarter(s, ri), quarter(s, second(s, ri))
                ja = same(cax + e2, ru, QC, q * ru, quarter(s, ci) * QC, cdev(second(s, ci)))
                jb = same(cax + e1, ru, HC, q * ru, half(s, ci) * HC, cdev(first(s, ci)))
                jc = same(rax + e2, ru, 8 * cu, q * ru, 0, rdev(second(s, ri)))
                jd = same(rax + e1, ru, 8 * cu, q * ru, 0, rdev(first(s, ri)))
                je = same(rax + e1, ru, 8 * cu, q2 * ru, 0, rdev(first(s, ri)))
                f1 = quarter(s, first(s, ri))
                f2 = quarter(s, second(s, first(s, ri)))
                fw = [same("d2d", ru, 8 * cu, k * ru, 0, at(c_=other)) for k in (q, q2, f1, f2)]
                eg = event([], [eg0], lambda: None, 0.02, [ja])
                eh = event([ja], [eg], lambda: None, 0.02, [jb])
                ei = event([jb], [eh], lambda: None, 0.02, [jc, jd, fw[0]])
                ej = event([jc], [ei], lambda: None, 0.02, [je, fw[1]])
                ek = event([jd], [ej], lambda: None, 0.02, [fw[2]])
                event([je], [ek], lambda: None, 0.02, [fw[3]])
                arrived += fw

        for s in range(2):
            e1, e2 = ("xe1", "xe2") if s == 0 else ("xe2", "xe1")
            zl = "z+" if s == 0 else "z-"
            sg = 1 if s == 0 else -1
            nxt = at(z_=rem(z + sg + NZ, NZ))
            chunk = lambda t, sg=sg: rem(z - sg * (t + 1) + 2 * NZ, NZ)
            b1, b2 = half(s, x), part(s, x)
            base = s * 8 * ZR
            ring = []
            for t in range(NZ - 1):
                src = (functools.partial(lambda l, a: p_c.at[l, R(a, ZR), :], l, base + chunk(0) * ZR) if t == 0
                       else functools.partial(lambda l, s, t: rc.at[l, s, t - 1], l, s, t))
                ring.append(xfer(zl, ZR, DC, src, functools.partial(lambda l, s, t: rc.at[l, s, t], l, s, t), nxt))

            def wc0(l=l, a=base + chunk(0) * ZR):
                need((l, 2))
                here = ((l,), a, 0)
                total((p_c, *here), [(p_c, *here), (own_c, *here)], ZR, DC)

            def wcr(t, rows, cols, row, col, more, l=l, s=s, base=base, chunk=chunk):
                here = ((l,), base + chunk(t) * ZR + row, col)
                into = (rc, (l, s, t - 1), row, col)
                total(into, [into, (p_c, *here), (own_c, *here)] + more, rows, cols)

            ev = event([d2d["c", l, s]], [begin], wc0, adds(ZR, DC, 2), [ring[0]])
            for t in range(1, NZ - 1):
                ev = event([ring[t - 1]], [ev], functools.partial(wcr, t, ZR, DC, 0, 0, []), adds(ZR, DC, 3), [ring[t]])
            tx1 = xfer(e1, ru, DC, functools.partial(lambda l, s, a: rc.at[l, s, NZ - 2, R(a, ru), :], l, s, (1 - b1) * ru),
                       functools.partial(lambda l, s: rx1.at[l, s], l, s), at(x_=first(s, x)))
            tx2 = xfer(e2, ru, cu, functools.partial(lambda l, s, a, b: rc.at[l, s, NZ - 2, R(a, ru), C(b, cu)], l, s, b1 * ru, (1 - b2) * cu),
                       functools.partial(lambda l, s: rx2.at[l, s], l, s), at(x_=second(s, x)))
            ev = event([ring[NZ - 2]], [ev], functools.partial(wcr, NZ - 1, ru, DC, (1 - b1) * ru, 0, []), adds(ru, DC, 3), [tx1])
            ev = event([tx1], [ev], functools.partial(wcr, NZ - 1, ru, cu, b1 * ru, (1 - b2) * cu, [(rx1, (l, s), 0, (1 - b2) * cu)]), adds(ru, cu, 4), [tx2])

            def wx(l=l, s=s, base=base, b1=b1, b2=b2):
                row, col = b1 * ru, b2 * cu
                here = ((l,), base + z * ZR + row, col)
                total((ry, (l, s, y), 0, 0),
                      [(rc, (l, s, NZ - 2), row, col), (p_c, *here), (own_c, *here), (rx1, (l, s), 0, col), (rx2, (l, s), 0, 0)], ru, cu)

            mine = functools.partial(lambda l, s: ry.at[l, s, y], l, s)
            tys = [xfer("ye1" if d != 3 else "ye2", ru, cu, mine, mine, at(y_=rem(y + d, NY)), hops=2 if d == 2 else 1) for d in range(1, NY)]
            ev = event([tx2], [ev], wx, adds(ru, cu, 5), tys)
            g_base = core * 16 * ZR + base
            keep_c = pltpu.make_async_copy(rx2.at[l, s], dn_out.at[l, R(g_base + z * ZR + b1 * ru, ru), C(b2 * cu, cu)], keep_sem.at[l, 1 + s])

            def wy(l=l, s=s, keep_c=keep_c):
                total((rx2, (l, s), 0, 0), [(ry, (l, s, k), 0, 0) for k in range(NY)], ru, cu)
                add_squares(rx2, (l, s), 0.25)
                keep_c.start()

            def same_c(link, rows, cols, row, col, dev, src=None, l=l, g_base=g_base):
                ref = functools.partial(lambda l, row, col, rows, cols: dn_out.at[l, R(row, rows), C(col, cols)], l, g_base + row, col, rows, cols)
                return xfer(link, rows, cols, src or ref, ref, dev)

            ha = same_c(e2, ru, cu, z * ZR + b1 * ru, b2 * cu, at(x_=second(s, x)), src=functools.partial(lambda l, s: rx2.at[l, s], l, s))
            hb = same_c(e1, ru, DC, z * ZR + b1 * ru, 0, at(x_=first(s, x)))
            ev = event(tys, [ev], wy, 0.3, [ha])
            pieces_done[l].append(ev)
            ev = event([ha], [ev], keep_c.wait, 0.1, [hb])
            got, prev = hb, ev
            for t in range(NZ):
                held = rem(z - sg * t + 2 * NZ, NZ) * ZR
                fwd = [same_c("d2d", ZR, DC, held, 0, at(c_=other))]
                arrived += fwd
                go = [same_c(zl, ZR, DC, held, 0, nxt)] if t < NZ - 1 else []
                prev = event([got], [prev], lambda: None, 0.02, go + fwd)
                got = go[0] if go else None

    def stage(ref, slot, n, peers_, pre, waits, work):
        mine = lambda: ref.at[slot]
        ts = [Xfer("n", 4096, mine, mine, p) for p in peers_]
        xfers.extend(ts)
        return ts, event(waits, pre, work, 0.1, ts)

    def put(ref, slot, from_):
        def work():
            if from_ is None:
                ref[slot] = acc[...]
            else:
                r, n = from_
                s = r[0]
                for k in range(1, n):
                    s = s + r[k]
                ref[slot] = s
        return work

    ts, ev = stage(nz, z, NZ, [at(z_=rem(z + d, NZ)) for d in range(1, NZ)], pieces_done[0] + pieces_done[1], [], put(nz, z, None))
    ts, ev = stage(ny, y, NY, [at(y_=rem(y + d, NY)) for d in range(1, NY)], [ev], ts, put(ny, y, (nz, NZ)))
    ts, ev = stage(nx, x, NX, [at(x_=rem(x + d, NX)) for d in range(1, NX)], [ev], ts, put(nx, x, (ny, NY)))
    ts, ev = stage(nc, core, 2, [at(c_=other)], [ev], ts, put(nc, core, (nx, NX)))

    def last():
        sq_out[...] = nc[0] + nc[1]

    event(ts, [ev], last, 0.1, [])
    event(arrived, [], lambda: None, 0.1, [])

    ids = {id(t): k for k, t in enumerate(xfers)}
    assert len(ids) <= send_sem.shape[0], len(ids)
    ordered, _ = order_of(events)
    for e in ordered:
        for t in e.waits:
            t.copy.wait_recv()
        e.work()
        for t in e.sends:
            k = ids[id(t)]
            t.copy = pltpu.make_async_remote_copy(src_ref=t.src(), dst_ref=t.dst(), send_sem=send_sem.at[k], recv_sem=recv_sem.at[k],
                                                  device_id={"dp": t.dev}, device_id_type=MESH)
            t.copy.start()
    for t in xfers:
        t.copy.wait_send()


N_XFERS = 320


def all_reduce(ru, cu, g1, u1, d1, g0, u0, d0):
    rows, ff, d = 16 * ru // 2 * 1, 8 * cu, 2 * cu
    S, ZR, DC = 4 * ru, 2 * ru, 2 * cu
    any_ = pl.BlockSpec(memory_space=pl.ANY)
    V = pltpu.VMEM
    return pl.pallas_call(
        functools.partial(comm_kernel, ru, cu),
        name="grad_sum",
        out_shape=(jax.ShapeDtypeStruct((2, 2, *g1.shape), BF16), jax.ShapeDtypeStruct((2, *d1.shape), BF16), jax.ShapeDtypeStruct((8, 128), F32)),
        in_specs=[any_] * 6,
        out_specs=(any_, any_, pl.BlockSpec(memory_space=pltpu.VMEM)),
        scratch_shapes=[
            V((2, 2, 2 * S, 8 * cu), BF16), V((2, 16 * ZR, DC), BF16),
            V((2, 2, 2 * S, 8 * cu), BF16), V((2, 16 * ZR, DC), BF16),
            V((2, 2, 2, 2 * ru, 8 * cu), BF16), V((2, 2, 2, ru, 8 * cu), BF16), V((2, 2, 2, ru, 4 * cu), BF16), V((2, 2, 2, ru, 2 * cu), BF16),
            V((2, NZ - 1, ru, cu), BF16), V((2, 2, NZ - 1, ZR, DC), BF16), V((2, 2, ru, DC), BF16), V((2, 2, ru, cu), BF16), V((2, 2, NY, ru, cu), BF16),
            V((2, ru, cu), BF16), V((8, 128), F32), V((NZ, 8, 128), F32), V((NY, 8, 128), F32), V((NX, 8, 128), F32), V((2, 8, 128), F32),
            pltpu.SemaphoreType.DMA((N_XFERS,)), pltpu.SemaphoreType.DMA((N_XFERS,)), pltpu.SemaphoreType.DMA((2, 3)), pltpu.SemaphoreType.DMA((2, 3)),
        ],
        compiler_params=pltpu.CompilerParams(collective_id=0, has_side_effects=True, vmem_limit_bytes=50 * 2**20),
    )(g1, u1, d1, g0, u0, d0)


def solution(mesh):
    def step(x, dy, *arrays):
        weights, m, v = (arrays[i : i + 3] for i in (0, 3, 6))
        layers = weights[0].shape[0]
        h, kept = x[0], []
        for number in range(layers):
            kept.append(h)
            h = layer(h, {name: w[number] for name, w in zip(NAMES, weights, strict=True)})
        by_h, by_w = dy[0], [None] * layers
        for number in reversed(range(layers)):
            _, back = jax.vjp(lambda w, h: layer(h, w), {name: w[number] for name, w in zip(NAMES, weights, strict=True)}, kept[number])
            by_w[number], by_h = back(by_h)
        d, ff = weights[0].shape[1:]
        gu, down, squares = all_reduce(d // 16, ff // 8, *[by_w[number][name] for number in (1, 0) for name in NAMES])
        gradients = [gu[0], gu[1], down]
        count = sum(g.size for g in gradients)
        factor = jnp.minimum(1.0, 0.5 * lax.rsqrt(jnp.sum(squares) / count + 1e-30))
        new = [adamw(w.astype(jnp.float32), m, v, g.astype(jnp.float32) * factor) for w, m, v, g in zip(weights, m, v, gradients, strict=True)]
        return tuple(one[which] for which in range(3) for one in new)

    return jax.shard_map(
        step,
        mesh=mesh,
        in_specs=(P(("rep", "dp"), None, None),) * 2 + (P(None, None, None),) * 9,
        out_specs=(P("rep", None, None),) * 9,
        check_vma=False,
    )
```

```python
import functools

import jax
import jax.numpy as jnp
from jax import lax
from jax.experimental import pallas as pl
from jax.experimental.pallas import tpu as pltpu
from jax.sharding import PartitionSpec as P

MESH = pl.DeviceIdType.MESH
NX, NY, NZ = 4, 4, 8
F32, BF16 = jnp.float32, jnp.bfloat16


NN = (((1,), (0,)), ((), ()))
NT = (((1,), (1,)), ((), ()))
TN = (((0,), (0,)), ((), ()))


def dot(a, b, dims=NN):
    return lax.dot_general(a, b, dims, preferred_element_type=F32)


def scale_of(wide):
    return lax.rsqrt(jnp.mean(wide * wide, -1, keepdims=True) + 1e-6)


def normed_f(h):
    wide = h.astype(F32)
    return (wide * scale_of(wide)).astype(BF16)


def forward_kernel(blocks, tiles, x_ref, wg_ref, wu_ref, wd_ref, g_ref, u_ref, a0_ref, h_ref, a1_ref, total):
    j = pl.program_id(0)
    n = x_ref.shape[0]
    b = n // blocks

    @pl.when(j == 0)
    def _():
        def body(k, _):
            rows = pl.ds(pl.multiple_of(k * 64, 64), 64)
            a0_ref[rows, :] = normed_f(x_ref[rows, :])
            total[rows, :] = jnp.zeros((64, total.shape[1]), F32)
            return 0
        lax.fori_loop(0, n // 64, body, 0)

    for k in range(blocks):
        rows = pl.ds(k * b, b)
        a = a0_ref[rows, :]
        g = dot(a, wg_ref[0])
        u = dot(a, wu_ref[0])
        g_ref[rows, :] = g
        u_ref[rows, :] = u
        p = (g * jax.nn.sigmoid(g) * u).astype(BF16)
        total[rows, :] += dot(p, wd_ref[0])

    @pl.when(j == tiles - 1)
    def _():
        def body(k, _):
            rows = pl.ds(pl.multiple_of(k * 64, 64), 64)
            h = x_ref[rows, :] + total[rows, :].astype(BF16)
            h_ref[rows, :] = h
            a1_ref[rows, :] = normed_f(h)
            return 0
        lax.fori_loop(0, n // 64, body, 0)


def forward(x, wg, wu, wd, tile=512, blocks=4):
    n, d = x.shape
    ff = wg.shape[2]
    tiles = ff // tile
    whole = pl.BlockSpec((n, d), lambda j: (0, 0))
    return pl.pallas_call(
        functools.partial(forward_kernel, blocks, tiles),
        name="layer0_forward",
        grid=(tiles,),
        in_specs=[whole, pl.BlockSpec((1, d, tile), lambda j: (0, 0, j)), pl.BlockSpec((1, d, tile), lambda j: (0, 0, j)), pl.BlockSpec((1, tile, d), lambda j: (0, j, 0))],
        out_specs=[pl.BlockSpec((n, tile), lambda j: (0, j)), pl.BlockSpec((n, tile), lambda j: (0, j)), whole, whole, whole],
        out_shape=[jax.ShapeDtypeStruct((n, ff), F32)] * 2 + [jax.ShapeDtypeStruct((n, d), BF16)] * 3,
        scratch_shapes=[pltpu.VMEM((n, d), F32)],
        compiler_params=pltpu.CompilerParams(dimension_semantics=("arbitrary",), vmem_limit_bytes=60 * 2**20),
        cost_estimate=pl.CostEstimate(flops=6 * n * d * ff, bytes_accessed=8 * n * ff + 6 * d * ff + 8 * n * d, transcendentals=n * ff),
    )(x, wg, wu, wd)


def backward_tile(g, u, dp):
    sig = jax.nn.sigmoid(g)
    act = g * sig
    p = (act * u).astype(BF16)
    du = (dp * act).astype(BF16)
    dg = (dp * u * (sig + act * (1.0 - sig))).astype(BF16)
    return p, dg, du


def last_kernel(blocks, tiles, a_ref, h_ref, dy_ref, wg_ref, wu_ref, wd_ref, dwg_ref, dwu_ref, dwd_ref, dh_ref, p_s, dg_s, du_s, by_g, by_u):
    j = pl.program_id(0)
    n, d = a_ref.shape
    b = n // blocks

    @pl.when(j == 0)
    def _():
        def body(k, _):
            rows = pl.ds(pl.multiple_of(k * 64, 64), 64)
            by_g[rows, :] = jnp.zeros((64, d), F32)
            by_u[rows, :] = jnp.zeros((64, d), F32)
            return 0
        lax.fori_loop(0, n // 64, body, 0)

    for k in range(blocks):
        rows = pl.ds(k * b, b)
        a = a_ref[rows, :]
        g = dot(a, wg_ref[0])
        u = dot(a, wu_ref[0])
        dp = dot(dy_ref[rows, :], wd_ref[0], NT).astype(BF16).astype(F32)
        p, dg, du = backward_tile(g, u, dp)
        p_s[rows, :], dg_s[rows, :], du_s[rows, :] = p, dg, du
        by_g[rows, :] += dot(dg, wg_ref[0], NT)
        by_u[rows, :] += dot(du, wu_ref[0], NT)
    dwg_ref[...] = dot(a_ref[...], dg_s[...], TN).astype(BF16)
    dwu_ref[...] = dot(a_ref[...], du_s[...], TN).astype(BF16)
    dwd_ref[...] = dot(p_s[...], dy_ref[...], TN).astype(BF16)

    @pl.when(j == tiles - 1)
    def _():
        def body(k, _):
            rows = pl.ds(pl.multiple_of(k * 32, 32), 32)
            by_a = (by_g[rows, :].astype(BF16) + by_u[rows, :].astype(BF16)).astype(F32)
            wide = h_ref[rows, :].astype(F32)
            s = scale_of(wide)
            by_h = by_a * s - wide * (s * s * s * jnp.mean(by_a * wide, -1, keepdims=True))
            dh_ref[rows, :] = dy_ref[rows, :] + by_h.astype(BF16)
            return 0
        lax.fori_loop(0, n // 32, body, 0)


def last(a, h, dy, wg, wu, wd, tile=512, blocks=4):
    n, d = a.shape
    ff = wg.shape[2]
    tiles = ff // tile
    whole = pl.BlockSpec((n, d), lambda j: (0, 0))
    return pl.pallas_call(
        functools.partial(last_kernel, blocks, tiles),
        name="layer1_both",
        grid=(tiles,),
        in_specs=[whole] * 3 + [pl.BlockSpec((1, d, tile), lambda j: (1, 0, j)), pl.BlockSpec((1, d, tile), lambda j: (1, 0, j)), pl.BlockSpec((1, tile, d), lambda j: (1, j, 0))],
        out_specs=[pl.BlockSpec((d, tile), lambda j: (0, j)), pl.BlockSpec((d, tile), lambda j: (0, j)), pl.BlockSpec((tile, d), lambda j: (j, 0)), whole],
        out_shape=[jax.ShapeDtypeStruct((d, ff), BF16), jax.ShapeDtypeStruct((d, ff), BF16), jax.ShapeDtypeStruct((ff, d), BF16), jax.ShapeDtypeStruct((n, d), BF16)],
        scratch_shapes=[pltpu.VMEM((n, tile), BF16)] * 3 + [pltpu.VMEM((n, d), F32)] * 2,
        compiler_params=pltpu.CompilerParams(dimension_semantics=("arbitrary",), vmem_limit_bytes=60 * 2**20),
        cost_estimate=pl.CostEstimate(flops=16 * n * d * ff, bytes_accessed=12 * d * ff + 8 * n * d, transcendentals=n * ff),
    )(a, h, dy, wg, wu, wd)


def first_kernel(blocks, a_ref, dh_ref, g_ref, u_ref, wd_ref, dwg_ref, dwu_ref, dwd_ref, p_s, dg_s, du_s):
    n = a_ref.shape[0]
    b = n // blocks
    for k in range(blocks):
        rows = pl.ds(k * b, b)
        dp = dot(dh_ref[rows, :], wd_ref[0], NT).astype(BF16).astype(F32)
        p_s[rows, :], dg_s[rows, :], du_s[rows, :] = backward_tile(g_ref[rows, :], u_ref[rows, :], dp)
    dwd_ref[...] = dot(p_s[...], dh_ref[...], TN).astype(BF16)
    dwg_ref[...] = dot(a_ref[...], dg_s[...], TN).astype(BF16)
    dwu_ref[...] = dot(a_ref[...], du_s[...], TN).astype(BF16)


def first_backward(a, dh, g, u, wd, tile=512, blocks=4):
    n, d = a.shape
    ff = g.shape[1]
    whole = pl.BlockSpec((n, d), lambda j: (0, 0))
    return pl.pallas_call(
        functools.partial(first_kernel, blocks),
        name="layer0_backward",
        grid=(ff // tile,),
        in_specs=[whole] * 2 + [pl.BlockSpec((n, tile), lambda j: (0, j))] * 2 + [pl.BlockSpec((1, tile, d), lambda j: (0, j, 0))],
        out_specs=[pl.BlockSpec((d, tile), lambda j: (0, j)), pl.BlockSpec((d, tile), lambda j: (0, j)), pl.BlockSpec((tile, d), lambda j: (j, 0))],
        out_shape=[jax.ShapeDtypeStruct((d, ff), BF16), jax.ShapeDtypeStruct((d, ff), BF16), jax.ShapeDtypeStruct((ff, d), BF16)],
        scratch_shapes=[pltpu.VMEM((n, tile), BF16)] * 3,
        compiler_params=pltpu.CompilerParams(dimension_semantics=("arbitrary",), vmem_limit_bytes=60 * 2**20),
        cost_estimate=pl.CostEstimate(flops=8 * n * d * ff, bytes_accessed=8 * n * ff + 8 * d * ff + 4 * n * d, transcendentals=n * ff),
    )(a, dh, g, u, wd)


def adamw(w, m, v, g):
    m = 0.9 * m + 0.1 * g
    v = 0.95 * v + 0.05 * g * g
    step = m * lax.rsqrt(v + 1e-8) + 0.1 * w
    return (w - 0.02 * step).astype(jnp.bfloat16), m, v


def div(a, b):
    return lax.div(a, jnp.int32(b))


def rem(a, b):
    return lax.rem(a, jnp.int32(b))


def first(s, i):
    return i + 1 - 2 * rem(i, 2) if s == 0 else 3 - i


def second(s, i):
    return first(1 - s, i)


def half(s, i):
    return rem(div(i + 1, 2), 2) if s == 0 else div(i, 2)


def part(s, i):
    return div(i, 2) if s == 0 else rem(i, 2)


def quarter(s, i):
    return 2 * half(s, i) + part(s, i)


class Xfer:
    def __init__(self, link, nbytes, src, dst, dev):
        self.link, self.nbytes, self.src, self.dst, self.dev = link, nbytes, src, dst, dev
        self.copy = None
        self.arrives = None


class Event:
    def __init__(self, waits, pre, work, cost, sends):
        self.waits, self.pre, self.work, self.cost, self.sends = waits, pre, work, cost, sends
        self.done = None


RATE = {"ici": 46.0e3, "d2d": 500.0e3}
DELAY = 2.2


def order_of(events):
    links, left, out, clock = {}, list(events), [], 0.0
    while left:
        best = None
        for e in left:
            if any(p.done is None for p in e.pre) or any(t.arrives is None for t in e.waits):
                continue
            ready = max([p.done for p in e.pre] + [t.arrives for t in e.waits] + [0.0])
            if best is None or max(ready, clock) < best[0]:
                best = (max(ready, clock), e)
        clock, e = best
        clock += e.cost
        e.done = clock
        for t in e.sends:
            begin = max(clock, links.get(t.link, 0.0))
            links[t.link] = begin + t.nbytes / RATE["d2d" if t.link == "d2d" else "ici"]
            t.arrives = links[t.link] + DELAY
        left.remove(e)
        out.append(e)
    return out, clock


def comm_kernel(ru, cu, *refs):
    (g1, u1, d1, g0, u0, d0, gu_out, dn_out, sq_out, own_ab, own_c, p_ab, p_c, r1, r2, r3, r4, rz, rc, rx1, rx2, ry, f_ab, acc, nz, ny, nx, nc,
     send_sem, recv_sem, load_sem, keep_sem) = refs
    grads = ((g0, u0, d0), (g1, u1, d1))
    me = lax.axis_index("dp")
    core = rem(me, 2)
    z = rem(div(me, 2), NZ)
    y = rem(div(me, 2 * NZ), NY)
    x = div(me, 2 * NZ * NY)
    other = 1 - core

    def at(x_=None, y_=None, z_=None, c_=None):
        pick = lambda v, d: d if v is None else v
        return ((pick(x_, x) * NY + pick(y_, y)) * NZ + pick(z_, z)) * 2 + pick(c_, core)

    R = lambda start, size: pl.ds(pl.multiple_of(start, 16), size)
    C = lambda start, size: pl.ds(pl.multiple_of(start, 128), size)

    barrier = pltpu.get_barrier_semaphore()
    peers = [at(c_=other)]
    peers += [at(x_=rem(x + d, NX)) for d in range(1, NX)]
    peers += [at(y_=rem(y + d, NY)) for d in range(1, NY)]
    peers += [at(z_=rem(z + d, NZ)) for d in range(1, NZ)]

    S = 4 * ru
    HC, QC = 4 * cu, 2 * cu
    DC = 2 * cu
    ZR = 2 * ru

    loads = {}
    for l in (1, 0):
        for c in range(2):
            loads[l, c] = pltpu.make_async_copy(grads[l][c].at[R(core * 2 * S, 2 * S), :], own_ab.at[l, c], load_sem.at[l, c])
        loads[l, 2] = pltpu.make_async_copy(grads[l][2].at[R(core * 16 * ZR, 16 * ZR), :], own_c.at[l], load_sem.at[l, 2])
        for k in range(3):
            loads[l, k].start()
    for p in peers:
        pl.semaphore_signal(barrier, inc=1, device_id={"dp": p}, device_id_type=MESH)
    pl.semaphore_wait(barrier, len(peers))

    xfers, events = [], []

    def xfer(link, rows, cols, src, dst, dev, hops=1):
        t = Xfer(link, rows * cols * 2 * hops, src, dst, dev)
        xfers.append(t)
        return t

    def event(waits, pre, work, cost, sends):
        e = Event(waits, pre, work, cost, sends)
        events.append(e)
        return e

    def total(dst, srcs, rows, cols):
        wide = min(cols, 2 * cu)
        across = cols // wide

        def block(i, _):
            r, c = (div(i, across), rem(i, across)) if across > 1 else (i, 0)

            def window(a):
                ref, lead, row, col = a
                return ref.at[(*lead, R(row + r * 16, 16), C(col + c * wide, wide))]

            s = window(srcs[0])[...].astype(F32)
            for a in srcs[1:]:
                s = s + window(a)[...].astype(F32)
            window(dst)[...] = s.astype(BF16)
            return 0

        lax.fori_loop(0, rows // 16 * across, block, 0)

    def add_squares(ref, lead, scale):
        for r in range(0, ru, 16):
            v = ref[(*lead, pl.ds(r, 16), slice(None))].astype(F32)
            v = v * v
            s = acc[...]
            for a in range(0, 16, 8):
                for b in range(0, cu, 128):
                    s = s + (scale * v[a : a + 8, b : b + 128])
            acc[...] = s

    adds = lambda rows, cols, n: rows * cols * n / 2.2e6 + 0.15

    acc[...] = jnp.zeros_like(acc)
    loaded = set()

    def need(*keys):
        for k in keys:
            if k not in loaded:
                loaded.add(k)
                loads[k].wait()

    d2d = {}
    firsts, seconds = [], []
    for l in (1, 0):
        for s in range(2):
            for c in range(2):
                ri = x if c == 0 else y
                for which, where, to in (("send", 1 - half(s, ri), firsts), ("keep", half(s, ri), seconds)):
                    row = s * S + where * 2 * ru
                    t = xfer("d2d", 2 * ru, 8 * cu,
                             functools.partial(lambda l, c, row: grads[l][c].at[R(other * 2 * S + row, 2 * ru), :], l, c, row),
                             functools.partial(lambda l, c, row: p_ab.at[l, c, R(row, 2 * ru), :], l, c, row), at(c_=other))
                    d2d[which, l, c, s] = t
                    to.append(t)
        for s in range(2):
            t = xfer("d2d", 8 * ZR, DC,
                     functools.partial(lambda l, s: grads[l][2].at[R(other * 16 * ZR + s * 8 * ZR, 8 * ZR), :], l, s),
                     functools.partial(lambda l, s: p_c.at[l, pl.ds(s * 8 * ZR, 8 * ZR), :], l, s), at(c_=other))
            d2d["c", l, s] = t
            firsts.append(t)
        firsts += seconds
        seconds = []
    begin = event([], [], lambda: None, 0.0, firsts)

    pieces_done = {}
    arrived = []
    for l in (1, 0):
        ends = []
        for c in range(2):
            ri, ci = (x, y) if c == 0 else (y, x)
            rax, cax = ("x", "y") if c == 0 else ("y", "x")
            rdev = (lambda i: at(x_=i)) if c == 0 else (lambda i: at(y_=i))
            cdev = (lambda i: at(y_=i)) if c == 0 else (lambda i: at(x_=i))
            for s in range(2):
                e1, e2 = ("e1", "e2") if s == 0 else ("e2", "e1")
                b1, b2, c1, c2 = half(s, ri), part(s, ri), half(s, ci), part(s, ci)
                out_rows, keep_rows = s * S + (1 - b1) * 2 * ru, s * S + b1 * 2 * ru
                q_out, q_keep = keep_rows + (1 - b2) * ru, keep_rows + b2 * ru
                k1 = functools.partial
                t1 = xfer(rax + e1, 2 * ru, 8 * cu, k1(lambda l, c, a: p_ab.at[l, c, R(a, 2 * ru), :], l, c, out_rows),
                          k1(lambda l, c, s: r1.at[l, c, s], l, c, s), rdev(first(s, ri)))
                t2 = xfer(rax + e2, ru, 8 * cu, k1(lambda l, c, a: p_ab.at[l, c, R(a, ru), :], l, c, q_out),
                          k1(lambda l, c, s: r2.at[l, c, s], l, c, s), rdev(second(s, ri)))
                t3 = xfer(cax + e1, ru, HC, k1(lambda l, c, a, b: p_ab.at[l, c, R(a, ru), C(b, HC)], l, c, q_keep, (1 - c1) * HC),
                          k1(lambda l, c, s: r3.at[l, c, s], l, c, s), cdev(first(s, ci)))
                t4 = xfer(cax + e2, ru, QC, k1(lambda l, c, a, b: p_ab.at[l, c, R(a, ru), C(b, QC)], l, c, q_keep, c1 * HC + (1 - c2) * QC),
                          k1(lambda l, c, s: r4.at[l, c, s], l, c, s), cdev(second(s, ci)))

                def w1(l=l, c=c, s=s, out_rows=out_rows):
                    need((l, c))
                    here = ((l, c), out_rows, 0)
                    total((p_ab, *here), [(p_ab, *here), (own_ab, *here)], 2 * ru, 8 * cu)

                def w2(l=l, c=c, s=s, q_out=q_out, b2=b2):
                    here = ((l, c), q_out, 0)
                    total((p_ab, *here), [(p_ab, *here), (own_ab, *here), (r1, (l, c, s), (1 - b2) * ru, 0)], ru, 8 * cu)

                def rest(cols_at, cols, more, l=l, c=c, s=s, q_keep=q_keep, b2=b2, c1=c1):
                    here = ((l, c), q_keep, cols_at)
                    srcs = [(p_ab, *here), (own_ab, *here), (r1, (l, c, s), b2 * ru, cols_at), (r2, (l, c, s), 0, cols_at)]
                    if more >= 1:
                        srcs.append((r3, (l, c, s), 0, cols_at - c1 * HC))
                    if more >= 2:
                        srcs.append((r4, (l, c, s), 0, 0))
                    total((p_ab, *here), srcs, ru, cols)

                w3 = functools.partial(rest, (1 - c1) * HC, HC, 0)
                w4 = functools.partial(rest, c1 * HC + (1 - c2) * QC, QC, 1)
                w5 = functools.partial(rest, c1 * HC + c2 * QC, QC, 2)
                ea = event([d2d["send", l, c, s]], [begin], w1, adds(2 * ru, 8 * cu, 2), [t1])
                eb = event([d2d["keep", l, c, s], t1], [ea], w2, adds(ru, 8 * cu, 3), [t2])
                ec = event([t2], [eb], w3, adds(ru, HC, 4), [t3])
                ed = event([t3], [ec], w4, adds(ru, QC, 5), [t4])
                ends.append(event([t4], [ed], w5, adds(ru, QC, 6), []))

        def piece(zz):
            c, k = div(zz, 4), rem(zz, 4)
            s, h = div(k, 2), rem(k, 2)
            qx = quarter(0, x) + s * (quarter(1, x) - quarter(0, x))
            qy = quarter(0, y) + s * (quarter(1, y) - quarter(0, y))
            q, cq = qx + c * (qy - qx), qy + c * (qx - qy)
            return c, s * S + q * ru, cq * QC + h * cu

        tz = []
        for d in range(1, NZ):
            zz = rem(z + d, NZ)
            c, a, b = piece(zz)
            tz.append(xfer("z+" if d <= 4 else "z-", ru, cu, functools.partial(lambda l, c, a, b: p_ab.at[l, c, R(a, ru), C(b, cu)], l, c, a, b),
                           functools.partial(lambda l, d: rz.at[l, d - 1], l, d), at(z_=zz), hops=min(d, NZ - d)))
        ez = event([], ends, lambda: None, 0.05, tz)
        mc, ma, mb = piece(z)
        keep_ab = pltpu.make_async_copy(f_ab.at[l], gu_out.at[mc, l, R(core * 2 * S + ma, ru), C(mb, cu)], keep_sem.at[l, 0])

        def wz(l=l, mc=mc, ma=ma, mb=mb, keep_ab=keep_ab):
            total((f_ab, (l,), 0, 0), [(p_ab, (l, mc), ma, mb)] + [(rz, (l, d), 0, 0) for d in range(NZ - 1)], ru, cu)
            add_squares(f_ab, (l,), 1.0)
            keep_ab.start()

        ta = [xfer("z+" if d <= 4 else "z-", ru, cu, functools.partial(lambda l: f_ab.at[l], l),
                   functools.partial(lambda l, c, a, b: gu_out.at[c, l, R(core * 2 * S + a, ru), C(b, cu)], l, mc, ma, mb), at(z_=rem(z + d, NZ)), hops=min(d, NZ - d))
              for d in range(1, NZ)]
        ef = event(tz, [ez], wz, 0.5, ta)
        pieces_done[l] = [ef]
        eg0 = event(ta, [ef], keep_ab.wait, 0.1, [])
        for c in range(2):
            ri, ci = (x, y) if c == 0 else (y, x)
            rax, cax = ("x", "y") if c == 0 else ("y", "x")
            rdev = (lambda i: at(x_=i)) if c == 0 else (lambda i: at(y_=i))
            cdev = (lambda i: at(y_=i)) if c == 0 else (lambda i: at(x_=i))
            for s in range(2):
                e1, e2 = ("e1", "e2") if s == 0 else ("e2", "e1")
                base = core * 2 * S + s * S

                def same(link, rows, cols, row, col, dev, l=l, c=c, base=base):
                    ref = functools.partial(lambda l, c, row, col, rows, cols: gu_out.at[c, l, R(row, rows), C(col, cols)], l, c, base + row, col, rows, cols)
                    return xfer(link, rows, cols, ref, ref, dev)

                q, q2 = quarter(s, ri), quarter(s, second(s, ri))
                ja = same(cax + e2, ru, QC, q * ru, quarter(s, ci) * QC, cdev(second(s, ci)))
                jb = same(cax + e1, ru, HC, q * ru, half(s, ci) * HC, cdev(first(s, ci)))
                jc = same(rax + e2, ru, 8 * cu, q * ru, 0, rdev(second(s, ri)))
                jd = same(rax + e1, ru, 8 * cu, q * ru, 0, rdev(first(s, ri)))
                je = same(rax + e1, ru, 8 * cu, q2 * ru, 0, rdev(first(s, ri)))
                f1 = quarter(s, first(s, ri))
                f2 = quarter(s, second(s, first(s, ri)))
                fw = [same("d2d", ru, 8 * cu, k * ru, 0, at(c_=other)) for k in (q, q2, f1, f2)]
                eg = event([], [eg0], lambda: None, 0.02, [ja])
                eh = event([ja], [eg], lambda: None, 0.02, [jb])
                ei = event([jb], [eh], lambda: None, 0.02, [jc, jd, fw[0]])
                ej = event([jc], [ei], lambda: None, 0.02, [je, fw[1]])
                ek = event([jd], [ej], lambda: None, 0.02, [fw[2]])
                event([je], [ek], lambda: None, 0.02, [fw[3]])
                arrived += fw

        for s in range(2):
            e1, e2 = ("xe1", "xe2") if s == 0 else ("xe2", "xe1")
            zl = "z+" if s == 0 else "z-"
            sg = 1 if s == 0 else -1
            nxt = at(z_=rem(z + sg + NZ, NZ))
            chunk = lambda t, sg=sg: rem(z - sg * (t + 1) + 2 * NZ, NZ)
            b1, b2 = half(s, x), part(s, x)
            base = s * 8 * ZR
            ring = []
            for t in range(NZ - 1):
                src = (functools.partial(lambda l, a: p_c.at[l, R(a, ZR), :], l, base + chunk(0) * ZR) if t == 0
                       else functools.partial(lambda l, s, t: rc.at[l, s, t - 1], l, s, t))
                ring.append(xfer(zl, ZR, DC, src, functools.partial(lambda l, s, t: rc.at[l, s, t], l, s, t), nxt))

            def wc0(l=l, a=base + chunk(0) * ZR):
                need((l, 2))
                here = ((l,), a, 0)
                total((p_c, *here), [(p_c, *here), (own_c, *here)], ZR, DC)

            def wcr(t, rows, cols, row, col, more, l=l, s=s, base=base, chunk=chunk):
                here = ((l,), base + chunk(t) * ZR + row, col)
                into = (rc, (l, s, t - 1), row, col)
                total(into, [into, (p_c, *here), (own_c, *here)] + more, rows, cols)

            ev = event([d2d["c", l, s]], [begin], wc0, adds(ZR, DC, 2), [ring[0]])
            for t in range(1, NZ - 1):
                ev = event([ring[t - 1]], [ev], functools.partial(wcr, t, ZR, DC, 0, 0, []), adds(ZR, DC, 3), [ring[t]])
            tx1 = xfer(e1, ru, DC, functools.partial(lambda l, s, a: rc.at[l, s, NZ - 2, R(a, ru), :], l, s, (1 - b1) * ru),
                       functools.partial(lambda l, s: rx1.at[l, s], l, s), at(x_=first(s, x)))
            tx2 = xfer(e2, ru, cu, functools.partial(lambda l, s, a, b: rc.at[l, s, NZ - 2, R(a, ru), C(b, cu)], l, s, b1 * ru, (1 - b2) * cu),
                       functools.partial(lambda l, s: rx2.at[l, s], l, s), at(x_=second(s, x)))
            ev = event([ring[NZ - 2]], [ev], functools.partial(wcr, NZ - 1, ru, DC, (1 - b1) * ru, 0, []), adds(ru, DC, 3), [tx1])
            ev = event([tx1], [ev], functools.partial(wcr, NZ - 1, ru, cu, b1 * ru, (1 - b2) * cu, [(rx1, (l, s), 0, (1 - b2) * cu)]), adds(ru, cu, 4), [tx2])

            def wx(l=l, s=s, base=base, b1=b1, b2=b2):
                row, col = b1 * ru, b2 * cu
                here = ((l,), base + z * ZR + row, col)
                total((ry, (l, s, y), 0, 0),
                      [(rc, (l, s, NZ - 2), row, col), (p_c, *here), (own_c, *here), (rx1, (l, s), 0, col), (rx2, (l, s), 0, 0)], ru, cu)

            mine = functools.partial(lambda l, s: ry.at[l, s, y], l, s)
            tys = [xfer("ye1" if d != 3 else "ye2", ru, cu, mine, mine, at(y_=rem(y + d, NY)), hops=2 if d == 2 else 1) for d in range(1, NY)]
            ev = event([tx2], [ev], wx, adds(ru, cu, 5), tys)
            g_base = core * 16 * ZR + base
            keep_c = pltpu.make_async_copy(rx2.at[l, s], dn_out.at[l, R(g_base + z * ZR + b1 * ru, ru), C(b2 * cu, cu)], keep_sem.at[l, 1 + s])

            def wy(l=l, s=s, keep_c=keep_c):
                total((rx2, (l, s), 0, 0), [(ry, (l, s, k), 0, 0) for k in range(NY)], ru, cu)
                add_squares(rx2, (l, s), 0.25)
                keep_c.start()

            def same_c(link, rows, cols, row, col, dev, src=None, l=l, g_base=g_base):
                ref = functools.partial(lambda l, row, col, rows, cols: dn_out.at[l, R(row, rows), C(col, cols)], l, g_base + row, col, rows, cols)
                return xfer(link, rows, cols, src or ref, ref, dev)

            ha = same_c(e2, ru, cu, z * ZR + b1 * ru, b2 * cu, at(x_=second(s, x)), src=functools.partial(lambda l, s: rx2.at[l, s], l, s))
            hb = same_c(e1, ru, DC, z * ZR + b1 * ru, 0, at(x_=first(s, x)))
            ev = event(tys, [ev], wy, 0.3, [ha])
            pieces_done[l].append(ev)
            ev = event([ha], [ev], keep_c.wait, 0.1, [hb])
            got, prev = hb, ev
            for t in range(NZ):
                held = rem(z - sg * t + 2 * NZ, NZ) * ZR
                fwd = [same_c("d2d", ZR, DC, held, 0, at(c_=other))]
                arrived += fwd
                go = [same_c(zl, ZR, DC, held, 0, nxt)] if t < NZ - 1 else []
                prev = event([got], [prev], lambda: None, 0.02, go + fwd)
                got = go[0] if go else None

    def stage(ref, slot, n, peers_, pre, waits, work):
        mine = lambda: ref.at[slot]
        ts = [Xfer("n", 4096, mine, mine, p) for p in peers_]
        xfers.extend(ts)
        return ts, event(waits, pre, work, 0.1, ts)

    def put(ref, slot, from_):
        def work():
            if from_ is None:
                ref[slot] = acc[...]
            else:
                r, n = from_
                s = r[0]
                for k in range(1, n):
                    s = s + r[k]
                ref[slot] = s
        return work

    ts, ev = stage(nz, z, NZ, [at(z_=rem(z + d, NZ)) for d in range(1, NZ)], pieces_done[0] + pieces_done[1], [], put(nz, z, None))
    ts, ev = stage(ny, y, NY, [at(y_=rem(y + d, NY)) for d in range(1, NY)], [ev], ts, put(ny, y, (nz, NZ)))
    ts, ev = stage(nx, x, NX, [at(x_=rem(x + d, NX)) for d in range(1, NX)], [ev], ts, put(nx, x, (ny, NY)))
    ts, ev = stage(nc, core, 2, [at(c_=other)], [ev], ts, put(nc, core, (nx, NX)))

    def last():
        sq_out[...] = nc[0] + nc[1]

    event(ts, [ev], last, 0.1, [])
    event(arrived, [], lambda: None, 0.1, [])

    ids = {id(t): k for k, t in enumerate(xfers)}
    assert len(ids) <= send_sem.shape[0], len(ids)
    ordered, _ = order_of(events)
    for e in ordered:
        for t in e.waits:
            t.copy.wait_recv()
        e.work()
        for t in e.sends:
            k = ids[id(t)]
            t.copy = pltpu.make_async_remote_copy(src_ref=t.src(), dst_ref=t.dst(), send_sem=send_sem.at[k], recv_sem=recv_sem.at[k],
                                                  device_id={"dp": t.dev}, device_id_type=MESH)
            t.copy.start()
    for t in xfers:
        t.copy.wait_send()


N_XFERS = 320


def all_reduce(ru, cu, g1, u1, d1, g0, u0, d0):
    rows, ff, d = 16 * ru // 2 * 1, 8 * cu, 2 * cu
    S, ZR, DC = 4 * ru, 2 * ru, 2 * cu
    any_ = pl.BlockSpec(memory_space=pl.ANY)
    V = pltpu.VMEM
    return pl.pallas_call(
        functools.partial(comm_kernel, ru, cu),
        name="grad_sum",
        out_shape=(jax.ShapeDtypeStruct((2, 2, *g1.shape), BF16), jax.ShapeDtypeStruct((2, *d1.shape), BF16), jax.ShapeDtypeStruct((8, 128), F32)),
        in_specs=[any_] * 6,
        out_specs=(any_, any_, pl.BlockSpec(memory_space=pltpu.VMEM)),
        scratch_shapes=[
            V((2, 2, 2 * S, 8 * cu), BF16), V((2, 16 * ZR, DC), BF16),
            V((2, 2, 2 * S, 8 * cu), BF16), V((2, 16 * ZR, DC), BF16),
            V((2, 2, 2, 2 * ru, 8 * cu), BF16), V((2, 2, 2, ru, 8 * cu), BF16), V((2, 2, 2, ru, 4 * cu), BF16), V((2, 2, 2, ru, 2 * cu), BF16),
            V((2, NZ - 1, ru, cu), BF16), V((2, 2, NZ - 1, ZR, DC), BF16), V((2, 2, ru, DC), BF16), V((2, 2, ru, cu), BF16), V((2, 2, NY, ru, cu), BF16),
            V((2, ru, cu), BF16), V((8, 128), F32), V((NZ, 8, 128), F32), V((NY, 8, 128), F32), V((NX, 8, 128), F32), V((2, 8, 128), F32),
            pltpu.SemaphoreType.DMA((N_XFERS,)), pltpu.SemaphoreType.DMA((N_XFERS,)), pltpu.SemaphoreType.DMA((2, 3)), pltpu.SemaphoreType.DMA((2, 3)),
        ],
        compiler_params=pltpu.CompilerParams(collective_id=0, has_side_effects=True, vmem_limit_bytes=50 * 2**20),
    )(g1, u1, d1, g0, u0, d0)


def solution(mesh):
    def step(x, dy, *arrays):
        weights, m, v = (arrays[i : i + 3] for i in (0, 3, 6))
        gate, up, a0, h, a1 = forward(x[0], *weights)
        *by_1, by_h = last(a1, h, dy[0], *weights)
        by_0 = first_backward(a0, by_h, gate, up, weights[2])
        d, ff = weights[0].shape[1:]
        gu, down, squares = all_reduce(d // 16, ff // 8, *by_1, *by_0)
        gradients = [gu[0], gu[1], down]
        count = sum(g.size for g in gradients)
        factor = jnp.minimum(1.0, 0.5 * lax.rsqrt(jnp.sum(squares) / count + 1e-30))
        new = [adamw(w.astype(jnp.float32), m, v, g.astype(jnp.float32) * factor) for w, m, v, g in zip(weights, m, v, gradients, strict=True)]
        return tuple(one[which] for which in range(3) for one in new)

    return jax.shard_map(
        step,
        mesh=mesh,
        in_specs=(P(("rep", "dp"), None, None),) * 2 + (P(None, None, None),) * 9,
        out_specs=(P("rep", None, None),) * 9,
        check_vma=False,
    )
```

```python
import functools

import jax
import jax.numpy as jnp
from jax import lax
from jax.experimental import pallas as pl
from jax.experimental.pallas import tpu as pltpu
from jax.sharding import PartitionSpec as P

LOGICAL = pl.DeviceIdType.LOGICAL
NX, NY, NZ, CORES = 4, 4, 8, 2
F32, BF16 = jnp.float32, jnp.bfloat16
NN = (((1,), (0,)), ((), ()))
NT = (((1,), (1,)), ((), ()))
TN = (((0,), (0,)), ((), ()))
ANY = pl.BlockSpec(memory_space=pl.ANY)
VMEM = pl.BlockSpec(memory_space=pltpu.VMEM)
SUBLANES, LANES = 16, 128
TILES, PARTS = 12, 3
BLOCK = (8, LANES)
NUMBER_OF_XFERS = 680


def dot(a, b, dims=NN):
    return lax.dot_general(a, b, dims, preferred_element_type=F32)


def scale_of(wide):
    return lax.rsqrt(jnp.mean(wide * wide, -1, keepdims=True) + 1e-6)


def normed(h):
    wide = h.astype(F32)
    return (wide * scale_of(wide)).astype(BF16)


def by_rows(n, step, body):
    def at(k, _):
        body(pl.ds(pl.multiple_of(k * step, step), step))
        return _

    lax.fori_loop(0, n // step, at, 0)


def turned(a, a_t):
    def slab(k, _):
        at = pl.ds(pl.multiple_of(k * LANES, LANES), LANES)
        a_t[at, :] = a[:, at].T
        return _

    lax.fori_loop(0, a.shape[1] // LANES, slab, 0)


def forward_kernel(blocks, x_ref, wg_ref, wu_ref, wd_ref, g_ref, u_ref, a0_t, h_ref, a1_ref, a1_t, a0_ref, total):
    j = pl.program_id(0)
    n = x_ref.shape[0]
    b = n // blocks

    @pl.when(j == 0)
    def _():
        def body(rows):
            a0_ref[rows, :] = normed(x_ref[rows, :])
            total[rows, :] = jnp.zeros_like(total[rows, :])

        by_rows(n, 64, body)
        turned(a0_ref, a0_t)

    for k in range(blocks):
        rows = pl.ds(k * b, b)
        a = a0_ref[rows, :]
        g = dot(a, wg_ref[0])
        u = dot(a, wu_ref[0])
        for to, by in ((g_ref, g), (u_ref, u)):
            for t in range(to.shape[0]):
                to[t, rows, :] = by[:, t * to.shape[2] : (t + 1) * to.shape[2]]
        p = (g * jax.nn.sigmoid(g) * u).astype(BF16)
        total[rows, :] += dot(p, wd_ref[0])

    @pl.when(j == pl.num_programs(0) - 1)
    def _():
        def body(rows):
            h = x_ref[rows, :] + total[rows, :].astype(BF16)
            h_ref[rows, :] = h
            a1_ref[rows, :] = normed(h)

        by_rows(n, 64, body)
        turned(a1_ref, a1_t)


def blocks_of(shape, *index):
    return pl.BlockSpec(shape, lambda j: tuple(j if i is None else i for i in index))


def forward(x, wg, wu, wd, tile=512, blocks=4):
    (n, d), ff = x.shape, wg.shape[-1]
    whole, wide = blocks_of((n, d), 0, 0), blocks_of((tile * TILES // ff, n, ff // TILES), None, 0, 0)
    turned_ = blocks_of((d, n), 0, 0)
    return pl.pallas_call(
        functools.partial(forward_kernel, blocks),
        name="layer0_forward",
        grid=(ff // tile,),
        in_specs=[whole] + [blocks_of((1, d, tile), 0, 0, None)] * 2 + [blocks_of((1, tile, d), 0, None, 0)],
        out_specs=[wide, wide, turned_, whole, whole, turned_],
        out_shape=[jax.ShapeDtypeStruct((TILES, n, ff // TILES), F32)] * 2 + [jax.ShapeDtypeStruct(s, BF16) for s in ((d, n), (n, d), (n, d), (d, n))],
        scratch_shapes=[pltpu.VMEM((n, d), BF16), pltpu.VMEM((n, d), F32)],
        compiler_params=pltpu.CompilerParams(vmem_limit_bytes=60 << 20),
    )(x, wg, wu, wd)


def backward_tile(g, u, dp):
    sig = jax.nn.sigmoid(g)
    act = g * sig
    return (act * u).astype(BF16), (dp * u * (sig + act * (1.0 - sig))).astype(BF16), (dp * act).astype(BF16)


def div(a, b):
    return lax.div(a, jnp.int32(b))


def rem(a, b):
    return lax.rem(a, jnp.int32(b))


def once(f):
    known = {}

    def g(s, i):
        key = s, id(i)
        if key not in known:
            known[key] = i, f(s, i)
        return known[key][1]

    return g


@once
def first(s, i):
    return NX - 1 - i if s else i + 1 - 2 * rem(i, 2)


def second(s, i):
    return first(1 - s, i)


@once
def half(s, i):
    return div(i, 2) if s else rem(div(i + 1, 2), 2)


@once
def part(s, i):
    return rem(i, 2) if s else div(i, 2)


@once
def quarter(s, i):
    return 2 * half(s, i) + part(s, i)


def place(start, size, unit):
    return pl.ds(start if isinstance(start, int) else pl.multiple_of(start, unit), size)


class Xfer:
    def __init__(self, link, count, hops, src, dst, dev):
        self.link, self.count, self.size, self.src, self.dst, self.dev = link, count, 2 * count * hops, src, dst, dev
        self.arrives = None


class Event:
    def __init__(self, waits, pre, work, cost, sends):
        self.waits, self.pre, self.work, self.cost, self.sends = waits, pre, work, cost, sends
        self.done = None


RATE, CHIP_RATE, DELAY, SLACK = 45.0e3, 450.0e3, 2.2, 0.6
STEPS = ((0.8, 0.8, 0.55, 0.55, 0.55), (0.55, 0.55), (0.45, 0.45, 0.5, 0.5, 0.5))
SLOTS = [part for phase in STEPS for part in phase * TILES]


def order_of(events, slots):
    links, left, groups, clock, done = {}, list(events), [[]], 0.0, 0
    while left:
        best = None
        for e in left:
            if any(done < p if isinstance(p, int) else p.done is None for p in e.pre) or any(t.arrives is None for t in e.waits):
                continue
            ready = max([p.done for p in e.pre if not isinstance(p, int)] + [t.arrives + (SLACK if done < len(slots) else 0.0) for t in e.waits] + [0.0])
            if best is None or max(ready, clock) < best[0]:
                best = (max(ready, clock), e)
        if done < len(slots) and (best is None or best[0] > clock):
            clock += slots[done]
            done += 1
            groups.append([])
            continue
        clock, e = best
        clock += e.cost + 0.02 * (len(e.waits) + len(e.sends))
        e.done = clock
        for t in e.sends:
            begin = max(clock, links.get(t.link, 0.0))
            links[t.link] = begin + t.size / (CHIP_RATE if t.link == "chip" else RATE)
            t.arrives = links[t.link] + DELAY
        left.remove(e)
        groups[-1].append(e)
    return groups, clock


def plan(here, refs, ru, cu):
    x, y, z, core = here
    (own_ab, own_c, p_ab, p_c, r1, r2, r3, r4, rz, rc, rx, ry, f_ab, f_c, acc, norms, gu_out, dn_out, sq_out, total, squares, need, local) = refs
    other = 1 - core
    xfers, events = [], []
    part_of = functools.partial

    devices, me = {}, ((x * NY + y) * NZ + z) * CORES + core
    steps = dict(x=(x, NY * NZ * CORES), y=(y, NZ * CORES), z=(z, CORES), core=(core, 1))

    def at(**to):
        ((axis, there),) = to.items()
        if (axis, id(there)) not in devices:
            i, stride = steps[axis]
            devices[axis, id(there)] = there, me + (there - i) * stride
        return devices[axis, id(there)][1]

    def window(ref, lead, row, rows, col, cols):
        return lambda: ref.at[(*lead, place(row, rows, SUBLANES), place(col, cols, LANES))]

    def block(ref, *lead):
        return lambda: ref.at[lead]

    def xfer(link, count, src, dst, hops=1, **to):
        t = Xfer(link, count, hops, src, dst, at(**to))
        xfers.append(t)
        return t

    others = {axis: [rem(k + d, n) for d in range(1, n)] for axis, k, n in (("x", x, NX), ("y", y, NY), ("z", z, NZ), ("core", core, CORES))}

    def to_all(axis, n, size, src, dst):
        ts = []
        for d in range(1, n):
            to, back = others[axis][d - 1], d * 2 > n
            ts.append(xfer(axis + "+-"[back], size, src(d, to), dst(d, to), n - d if back else d, **{axis: to}))
        return ts

    def event(waits, pre, work=lambda: None, cost=0.03, sends=()):
        e = Event(waits, pre, work, cost, sends)
        events.append(e)
        return e

    def adds(size, n):
        return size * n / 1.6e6 + 0.1

    D, FF = SUBLANES * ru, NZ * cu
    HD, S = D // 2, D // 4
    HC, QC = FF // 2, FF // 4
    CR = cu // 2
    XR = CR // 4
    around = [z * CR] + [to * CR for to in others["z"]]
    arrived, pieces = [], []

    for i in range(2 * PARTS):
        l, f0 = 1 - i // PARTS, i % PARTS * FF
        begin = event([], [(TILES // PARTS) * (i % PARTS + 1) * len(STEPS[0]) + (0 if l else len(SLOTS) - TILES * len(STEPS[0]))], part_of(need, i), 0.3)

        ends = []
        for c in range(2):
            ri, ci, rax, cax = (y, x, "y", "x") if c else (x, y, "x", "y")
            for s in range(2):
                k1, k2, e1, e2 = (i, c), (i, c, s), "+-"[s], "-+"[s]
                b1, b2, c1, c2 = half(s, ri), part(s, ri), half(s, ci), part(s, ci)
                keep = s * S + b1 * 2 * ru
                away, out, q = s * S + (1 - b1) * 2 * ru, keep + (1 - b2) * ru, keep + b2 * ru
                col1, col2, mine = (1 - c1) * HC, c1 * HC + (1 - c2) * QC, c1 * HC + c2 * QC
                t1 = xfer(rax + e1, 2 * ru * FF, window(p_ab, k1, away, 2 * ru, 0, FF), block(r1, *k2), **{rax: first(s, ri)})
                t2 = xfer(rax + e2, ru * FF, window(p_ab, k1, out, ru, 0, FF), block(r2, *k2), **{rax: second(s, ri)})
                t3 = xfer(cax + e1, ru * HC, window(p_ab, k1, q, ru, col1, HC), block(r3, *k2), **{cax: first(s, ci)})
                t4 = xfer(cax + e2, ru * QC, window(p_ab, k1, q, ru, col2, QC), block(r4, *k2), **{cax: second(s, ci)})

                def work(row, col, rows, cols, n, k1=k1, k2=k2, b2=b2, c1=c1):
                    to = (k1, row, col)
                    more = [(r1, k2, (b2 if n > 1 else 1 - b2) * ru, col), (r2, k2, 0, col), (r3, k2, 0, col - c1 * HC), (r4, k2, 0, 0)]
                    total((p_ab, *to), [(p_ab, *to), (own_ab, *to)] + more[:n], rows, cols)

                e, prev = begin, []
                for n, (t, row, col, rows, cols) in enumerate(((t1, away, 0, 2 * ru, FF), (t2, out, 0, ru, FF), (t3, q, col1, ru, HC), (t4, q, col2, ru, QC), (None, q, mine, ru, QC))):
                    e = event(prev, [e], part_of(work, row, col, rows, cols, n), adds(rows * cols, n + 2), [t] if t else [])
                    prev = [t]
                ends.append(e)

        def piece(to):
            c, k = div(to, 4), rem(to, 4)
            s, h = div(k, 2), rem(k, 2)
            qx = quarter(0, x) + s * (quarter(1, x) - quarter(0, x))
            qy = quarter(0, y) + s * (quarter(1, y) - quarter(0, y))
            return c, s * S + (qx + c * (qy - qx)) * ru, (qy + c * (qx - qy)) * QC + h * cu

        def from_piece(d, to, i=i):
            c, a, b = piece(to)
            return window(p_ab, (i, c), a, ru, b, cu)

        tz = to_all("z", NZ, ru * cu, from_piece, lambda d, to, i=i: block(rz, i, d - 1))
        e = event([], ends, sends=tz)
        mc, ma, mb = piece(z)
        home, mine = window(gu_out, (mc, l), core * HD + ma, ru, f0 + mb, cu), block(f_ab, i)

        def work(i=i, mc=mc, ma=ma, mb=mb, mine=mine, home=home):
            total((f_ab, (i,), 0, 0), [(p_ab, (i, mc), ma, mb)] + [(rz, (i, d), 0, 0) for d in range(NZ - 1)], ru, cu)
            squares(f_ab, (i,), 1.0)
            local(i, 0, mine, home).start()

        ta = to_all("z", NZ, ru * cu, lambda d, to, m=mine: m, lambda d, to, h=home: h)
        e = event(tz, [e], work, 0.4, ta)
        pieces.append(e)
        spread = event(ta, [e], lambda i=i, mine=mine, home=home: local(i, 0, mine, home).wait(), 0.1)
        for c in range(2):
            ri, ci, rax, cax = (y, x, "y", "x") if c else (x, y, "x", "y")
            for s in range(2):
                e1, e2 = "+-"[s], "-+"[s]

                def same(link, row, rows, col, cols, l=l, c=c, f0=f0, s=s, **to):
                    ref = window(gu_out, (c, l), core * HD + s * S + row * ru, rows * ru, f0 + col, cols)
                    return xfer(link, rows * ru * cols, ref, ref, **to)

                q, b1 = quarter(s, ri), 2 * half(s, ri)
                ts = [same(cax + e2, q, 1, quarter(s, ci) * QC, QC, **{cax: second(s, ci)}), same(cax + e1, q, 1, half(s, ci) * HC, HC, **{cax: first(s, ci)}),
                      same(rax + e2, q, 1, 0, FF, **{rax: second(s, ri)}), same(rax + e1, b1, 2, 0, FF, **{rax: first(s, ri)})]
                fw = [same("chip", b, 2, 0, FF, core=other) for b in (b1, 2 - b1)]
                e = spread
                for n, t in enumerate(ts):
                    e = event(ts[n - 1 : n], [e], sends=[t] + fw[: n // 3])
                event(ts[-1:], [e], sends=fw[1:])
                arrived += fw

        for s in range(2):
            key, base = (i, s), s * HC
            arms = ((1, "z+", 0, 4 - s), (-1, "z-", 4 - s, 3 + s))
            chunk = lambda k, base=base: base + around[k % NZ]

            def work(slots, row, into, i=i, key=key):
                to = ((i,), row, 0)
                total(into or (p_c, *to), [(p_c, *to), (own_c, *to)] + [(rc, (*key, t), 0, 0) for t in slots], CR, HD)

            ends, lasts = [], []
            for sg, zl, slot, n in arms:
                nxt, e, prev = others["z"][-(sg < 0)], begin, []
                for t in range(n):
                    row, into = chunk(sg * (n - t)), (rc, (*key, slot + t - 1), 0, 0) if t else None
                    ring = xfer(zl, CR * HD, block(rc, *key, slot + t - 1) if t else window(p_c, (i,), row, CR, 0, HD), block(rc, *key, slot + t), z=nxt)
                    e = event(prev, [e], part_of(work, [slot + t - 1] if t else [], row, into), adds(CR * HD, 3), [ring])
                    prev = [ring]
                ends.append(e)
                lasts += prev
            tx = to_all("x", NX, XR * HD, lambda d, to, key=key: window(rc, (*key, 3 - key[1]), to * XR, XR, 0, HD), lambda d, to, key=key: block(rx, *key, d - 1))
            e = event(lasts, ends, part_of(work, [3 - s, NZ - 2], chunk(0), (rc, (*key, 3 - s), 0, 0)), adds(CR * HD, 4), tx)

            def work_x(key=key):
                total((ry, (*key, y), 0, 0), [(rc, (*key, 3 - key[1]), x * XR, 0)] + [(rx, (*key, d), 0, 0) for d in range(NX - 1)], XR, HD)

            mine = block(ry, *key, y)
            ty = to_all("y", NY, XR * HD, lambda d, to, m=mine: m, lambda d, to, m=mine: m)
            e = event(tx, [e], work_x, adds(XR * HD, 4), ty)
            home, mine = window(dn_out, (l,), f0 + base + z * CR + x * XR, XR, core * HD, HD), block(f_c, *key)

            def work_y(key=key, mine=mine, home=home):
                total((f_c, key, 0, 0), [(ry, (*key, k), 0, 0) for k in range(NY)], XR, HD)
                squares(f_c, key, 1.0 / NY)
                local(key[0], 1 + key[1], mine, home).start()

            hx = to_all("x", NX, XR * HD, lambda d, to, m=mine: m, lambda d, to, h=home: h)
            e = event(ty, [e], work_y, 0.3, hx)
            pieces.append(e)
            e = event(hx, [e], lambda key=key, mine=mine, home=home: local(key[0], 1 + key[1], mine, home).wait(), 0.1)
            prev, ends = [[], []], [e, e]
            for t in range(4):
                for k, (sg, zl, slot, n) in enumerate(arms):
                    if t < n:
                        ref = window(dn_out, (l,), f0 + chunk(-sg * t), CR, core * HD, HD)
                        ring = xfer(zl, CR * HD, ref, ref, z=others["z"][-(sg < 0)])
                        ends[k] = event(prev[k], [ends[k]], sends=[ring])
                        prev[k] = [ring]
            ref = window(dn_out, (l,), f0 + base, HC, core * HD, HD)
            arrived.append(xfer("chip", HC * HD, ref, ref, core=other))
            event(prev[0] + prev[1], ends, sends=arrived[-1:])

    e, ts, prev = None, [], None
    for axis, k, n, ref in (("z", z, NZ, norms[0]), ("y", y, NY, norms[1]), ("x", x, NX, norms[2]), ("core", core, CORES, norms[3])):
        def work(ref=ref, k=k, prev=prev):
            if prev is None:
                ref[k] = acc[...]
            else:
                ref[k] = functools.reduce(lambda a, b: a + b, [prev[0][j] for j in range(prev[1])])

        new = [xfer("n", SUBLANES * LANES, block(ref, k), block(ref, k), **{axis: to}) for to in others[axis]]
        e = event(ts, pieces if e is None else [e], work, 0.15, new)
        ts, prev = new, (ref, n)

    def finish():
        sq_out[...] = norms[3][0] + norms[3][1]

    event(ts, [e], finish, 0.1)
    event(arrived, [])
    return xfers, events


def sum_kernel(ru, cu, *refs):
    (a1, a1_t, h, dy, a0_t, gate, up, wg, wu, wd, gu_out, dn_out, sq_out, dg, du, own_ab, own_c, p_ab, p_c, r1, r2, r3, r4, rz, rc, rx, ry, f_ab, f_c,
     acc, nz, ny, nx, nc, dh, send_sem, recv_sem, load_sem, keep_sem, tile_sem, out_sem, in_sem) = refs
    me = lax.axis_index("dp")
    core, z, y, x = rem(me, CORES), rem(div(me, CORES), NZ), rem(div(me, CORES * NZ), NY), div(me, CORES * NZ * NY)
    other = 1 - core
    D = SUBLANES * ru
    HD = D // 2
    n = h.shape[0]
    per = TILES // PARTS
    tile = NZ * cu // per
    partner = me + 1 - 2 * core
    slice_of = lambda j: pl.ds(pl.multiple_of(j * tile, LANES), tile)

    barrier = pltpu.get_barrier_semaphore()
    dev = lambda x, y, z, core: ((x * NY + y) * NZ + z) * CORES + core
    peers = [dev(x, y, z, other)] + [dev(rem(x + d, NX), y, z, core) for d in range(1, NX)]
    peers += [dev(x, rem(y + d, NY), z, core) for d in range(1, NY)] + [dev(x, y, rem(z + d, NZ), core) for d in range(1, NZ)]
    for p in peers:
        pl.semaphore_signal(barrier, inc=1, device_id=p, device_id_type=LOGICAL)
    pl.semaphore_wait(barrier, len(peers))

    def tile_sends(j, srcs=None, slot=0):
        i, cols = div(j, per), slice_of(rem(j, per))
        dsts = [p_ab.at[i, c, :, cols] for c in range(2)] + [p_c.at[i, cols, :]]
        return [pltpu.make_async_remote_copy(src_ref=src, dst_ref=dst, send_sem=out_sem.at[slot, k], recv_sem=in_sem.at[j, k], device_id=partner,
                                             device_id_type=LOGICAL) for k, (src, dst) in enumerate(zip(srcs or dsts, dsts, strict=True))]

    def total(dst, srcs, rows, cols):
        wide = next(cols // k for k in range(1, cols) if cols % (k * LANES) == 0 and cols // k <= 4 * LANES)
        tall = next(rows // k for k in range(1, rows) if rows % (k * SUBLANES) == 0 and rows // k * wide <= SUBLANES * LANES * 16)
        across = cols // wide

        many = rows // tall * across

        def block(i, _):
            if many > 1:
                r, c = (div(i, across) * tall, rem(i, across) * wide) if across > 1 else (i * tall, None)

            def at(a):
                ref, lead, row, col = a
                row, col = (row, col) if many == 1 else (row + r, col if c is None else col + c)
                return ref.at[(*lead, place(row, tall, SUBLANES), place(col, wide, LANES))]

            s = at(srcs[0])[...].astype(F32)
            for a in srcs[1:]:
                s = s + at(a)[...].astype(F32)
            at(dst)[...] = s.astype(BF16)
            return _

        if many > 1:
            lax.fori_loop(0, many, block, 0)
        else:
            block(0, 0)

    def squares(ref, lead, weight):
        rows, cols = ref.shape[len(lead):]
        for r in range(0, rows, SUBLANES):
            v = ref[(*lead, pl.ds(r, SUBLANES), slice(None))].astype(F32)
            v = v * v
            s = acc[...]
            for a in range(0, SUBLANES, BLOCK[0]):
                for b in range(0, cols, LANES):
                    s = s + weight * v[a : a + BLOCK[0], b : b + LANES]
            acc[...] = s

    def need(i):
        def wait(j, _):
            for t in tile_sends(j):
                t.wait_recv()
            return _

        lax.fori_loop(i * per, (i + 1) * per, wait, 0)

    def local(l, k, src, dst):
        return pltpu.make_async_copy(src(), dst(), keep_sem.at[l, k])

    acc[...] = jnp.zeros_like(acc)
    xfers, events = plan((x, y, z, core), (own_ab, own_c, p_ab, p_c, r1, r2, r3, r4, rz, rc, rx, ry, f_ab, f_c, acc, (nz, ny, nx, nc),
                                           gu_out, dn_out, sq_out, total, squares, need, local), ru, cu)
    counts = sorted(t.count for t in xfers)
    ids = {id(t): k for k, t in enumerate(sorted(xfers, key=lambda t: t.count))}
    groups, _ = order_of(events, SLOTS)

    def copy_of(src, dst, k, dev):
        return pltpu.make_async_remote_copy(src_ref=src, dst_ref=dst, send_sem=send_sem.at[k], recv_sem=recv_sem.at[k], device_id=dev, device_id_type=LOGICAL)

    def wait_of(count, k):
        cols = next(c for c in range(NZ * cu, 0, -LANES) if count % (c * SUBLANES) == 0)
        some = p_ab.at[0, 0, pl.ds(0, count // cols), pl.ds(0, cols)]
        return copy_of(some, some, k, me)

    def emit(group):
        for e in group:
            for t in e.waits:
                wait_of(t.count, ids[id(t)]).wait_recv()
            e.work()
            for t in e.sends:
                copy_of(t.src(), t.dst(), ids[id(t)], t.dev).start()

    def choose(j, options):
        middle = len(options) // 2
        if middle == 0:
            emit(options[0])
        elif any(options):
            pl.when(j < middle)(lambda: choose(j, options[:middle]))
            pl.when(j >= middle)(lambda: choose(j - middle, options[middle:]))

    def steps(srcs, bufs, *parts):
        mine = groups[: TILES * len(parts)]
        del groups[: TILES * len(parts)]

        def copies(j, slot):
            return [pltpu.make_async_copy(src(j), buf.at[slot], tile_sem.at[slot, k]) for k, (src, buf) in enumerate(zip(srcs, bufs, strict=True))]

        for t in copies(0, 0):
            t.start()

        def step(j, carry):
            slot = rem(j, 2)
            for t in copies(j, slot):
                t.wait()

            @pl.when(j + 1 < TILES)
            def _():
                for t in copies(j + 1, 1 - slot):
                    t.start()

            for k, part in enumerate(parts):
                part(j, slot)
                choose(j, mine[k :: len(parts)])
            return carry

        lax.fori_loop(0, TILES, step, 0)

    emit(groups.pop(0))
    tail = groups.pop()
    groups.append([])

    def fetch(*pairs):
        copies = [pltpu.make_async_copy(src, dst, load_sem.at[k]) for k, (src, dst) in enumerate(pairs)]
        for t in copies:
            t.start()
        return lambda: [t.wait() for t in copies]

    mine, yours = (pl.ds(pl.multiple_of(c * HD, LANES), HD) for c in (core, other))
    rows_out = pl.ds(pl.multiple_of(other * HD, SUBLANES), HD)
    staged = lambda st_ab, st_c, slot: [st_ab.at[slot, 0, rows_out, :], st_ab.at[slot, 1, rows_out, :], st_c.at[slot, :, yours]]

    def sent(j, slot, st):
        for t in tile_sends(j, staged(*st, slot), slot):
            t.wait_send()

    def term(j, slot, c, a, b, st):
        i, cols = div(j, per), slice_of(rem(j, per))
        st_ab, st_c = st
        if c < 2:
            st_ab[slot, c] = dot(a[...], b[...]).astype(BF16)
            own_ab[i, c, :, cols] = st_ab[slot, c, pl.ds(pl.multiple_of(core * HD, SUBLANES), HD), :]
        else:
            st_c[slot] = dot(a[...], b[...], TN).astype(BF16)
            own_c[i, cols, :] = st_c[slot, :, mine]
            for t in tile_sends(j, staged(st_ab, st_c, slot), slot):
                t.start()

    blocks = [pl.ds(k * (n // 4), n // 4) for k in range(4)]

    def layer_1(wgbuf, wubuf, wdbuf, a_s, a_t, dy_s, p_s, dgbuf, dubuf, *st):
        fetch((a1, a_s), (dy, dy_s), (a1_t, a_t))()

        def outs(j, slot):
            return [pltpu.make_async_copy(buf.at[slot], to.at[j], keep_sem.at[2 * PARTS + slot, k]) for k, (buf, to) in enumerate(((dgbuf, dg), (dubuf, du)))]

        def through(which, j, slot):
            if which == 0:
                @pl.when(j > 1)
                def _():
                    sent(j - 2, slot, st)
                    for t in outs(j - 2, slot):
                        t.wait()

            for rows in blocks[which::2]:
                a = a_s[rows, :]
                dp = dot(dy_s[rows, :], wdbuf[slot], NT).astype(BF16).astype(F32)
                p_s[rows, :], dgbuf[slot, rows, :], dubuf[slot, rows, :] = backward_tile(dot(a, wgbuf[slot]), dot(a, wubuf[slot]), dp)

        def down(j, slot):
            term(j, slot, 2, p_s, dy_s, st)
            for t in outs(j, slot):
                t.start()

        steps([lambda j: wg.at[1, :, slice_of(j)], lambda j: wu.at[1, :, slice_of(j)], lambda j: wd.at[1, slice_of(j), :]], [wgbuf, wubuf, wdbuf], functools.partial(through, 0),
              functools.partial(through, 1), lambda j, slot: term(j, slot, 0, a_t, dgbuf.at[slot], st), lambda j, slot: term(j, slot, 1, a_t, dubuf.at[slot], st), down)
        for k in range(2):
            sent(TILES - 2 + k, k, st)
            for t in outs(TILES - 2 + k, k):
                t.wait()

    V = lambda *s: pltpu.VMEM(s, BF16)
    W = lambda *s: pltpu.VMEM(s, F32)
    stages = V(2, 2, D, tile), V(2, tile, D)
    pl.run_scoped(layer_1, V(2, D, tile), V(2, D, tile), V(2, tile, D), V(n, D), V(D, n), V(n, D), V(n, tile), V(2, n, tile), V(2, n, tile), *stages)

    def by_input(gbuf, ubuf, wgbuf, wubuf, by_g, by_u, h_s, dy_s):
        arrived = fetch((h, h_s), (dy, dy_s))

        def clear(rows):
            by_g[rows, :] = jnp.zeros_like(by_g[rows, :])
            by_u[rows, :] = jnp.zeros_like(by_u[rows, :])

        by_rows(n, 64, clear)

        def part(which, j, slot):
            for rows in blocks[which::2]:
                by_g[rows, :] += dot(gbuf[slot, rows, :], wgbuf[slot], NT)
                by_u[rows, :] += dot(ubuf[slot, rows, :], wubuf[slot], NT)

        steps([lambda j: dg.at[j], lambda j: du.at[j], lambda j: wg.at[1, :, slice_of(j)], lambda j: wu.at[1, :, slice_of(j)]], [gbuf, ubuf, wgbuf, wubuf],
              functools.partial(part, 0), functools.partial(part, 1))
        arrived()

        def back(rows):
            by_a = (by_g[rows, :].astype(BF16) + by_u[rows, :].astype(BF16)).astype(F32)
            wide = h_s[rows, :].astype(F32)
            s = scale_of(wide)
            by_h = by_a * s - wide * (s * s * s * jnp.mean(by_a * wide, -1, keepdims=True))
            dh[rows, :] = dy_s[rows, :] + by_h.astype(BF16)

        by_rows(n, 32, back)

    pl.run_scoped(by_input, V(2, n, tile), V(2, n, tile), V(2, D, tile), V(2, D, tile), W(n, D), W(n, D), V(n, D), V(n, D))

    def layer_0(gbuf, ubuf, wbuf, a_t, p_s, dg_s, du_s, *st):
        fetch((a0_t, a_t))()

        def through(which, j, slot):
            if which == 0:
                @pl.when(j > 1)
                def _():
                    sent(TILES + j - 2, slot, st)

            for rows in blocks[which::2]:
                dp = dot(dh[rows, :], wbuf[slot], NT).astype(BF16).astype(F32)
                p_s[rows, :], dg_s[rows, :], du_s[rows, :] = backward_tile(gbuf[slot, rows, :], ubuf[slot, rows, :], dp)

        steps([lambda j: gate.at[j], lambda j: up.at[j], lambda j: wd.at[0, slice_of(j), :]], [gbuf, ubuf, wbuf], functools.partial(through, 0),
              functools.partial(through, 1), *[lambda j, slot, k=k: term(TILES + j, slot, *k, st) for k in ((0, a_t, dg_s), (1, a_t, du_s), (2, p_s, dh))])
        for k in range(2):
            sent(2 * TILES - 2 + k, k, st)

    pl.run_scoped(layer_0, W(2, n, tile), W(2, n, tile), V(2, tile, D), V(D, n), V(n, tile), V(n, tile), V(n, tile), *stages)
    emit(tail)
    for count in sorted(set(counts)):
        def wait(k, carry, count=count):
            wait_of(count, k).wait_send()
            return carry

        lax.fori_loop(counts.index(count), counts.index(count) + counts.count(count), wait, 0)


def gradient_sums(a1, a1_t, h, dy, a0_t, gate, up, wg, wu, wd):
    (n, d), ff = h.shape, wg.shape[-1]
    ru, cu = d // SUBLANES, ff // NZ // PARTS
    HD, CR, fs, N = d // 2, cu // 2, ff // PARTS, 2 * PARTS
    V = lambda *s: pltpu.VMEM(s, BF16)
    W = lambda *s: pltpu.VMEM(s, F32)
    DMA = lambda *s: pltpu.SemaphoreType.DMA(s)
    return pl.pallas_call(
        functools.partial(sum_kernel, ru, cu),
        name="gradient_sums",
        out_shape=(jax.ShapeDtypeStruct((2, 2, d, ff), BF16), jax.ShapeDtypeStruct((2, ff, d), BF16), jax.ShapeDtypeStruct(BLOCK, F32)) + (jax.ShapeDtypeStruct((TILES, n, ff // TILES), BF16),) * 2,
        in_specs=[ANY] * 10,
        out_specs=(ANY, ANY, VMEM, ANY, ANY),
        scratch_shapes=[
            V(N, 2, HD, fs), V(N, fs, HD), V(N, 2, HD, fs), V(N, fs, HD),
            V(N, 2, 2, 2 * ru, fs), V(N, 2, 2, ru, fs), V(N, 2, 2, ru, fs // 2), V(N, 2, 2, ru, fs // 4),
            V(N, NZ - 1, ru, cu), V(N, 2, NZ - 1, CR, HD), V(N, 2, NX - 1, CR // 4, HD), V(N, 2, NY, CR // 4, HD), V(N, ru, cu), V(N, 2, CR // 4, HD),
            W(*BLOCK), W(NZ, *BLOCK), W(NY, *BLOCK), W(NX, *BLOCK), W(CORES, *BLOCK),
            V(n, d),
            DMA(NUMBER_OF_XFERS), DMA(NUMBER_OF_XFERS), DMA(3), DMA(N + 2, 3), DMA(2, 4), DMA(2, 3), DMA(2 * TILES, 3),
        ],
        compiler_params=pltpu.CompilerParams(collective_id=0, has_side_effects=True, vmem_limit_bytes=62 << 20),
    )(a1, a1_t, h, dy, a0_t, gate, up, wg, wu, wd)


def adamw(w, m, v, g):
    m = 0.9 * m + 0.1 * g
    v = 0.95 * v + 0.05 * g * g
    step = m * lax.rsqrt(v + 1e-8) + 0.1 * w
    return (w - 0.02 * step).astype(BF16), m, v


def solution(mesh):
    def step(x, dy, *arrays):
        weights, m, v = (arrays[i : i + 3] for i in (0, 3, 6))
        gate, up, a0_t, h, a1, a1_t = forward(x[0], *weights)
        gu, down, squares, *_ = gradient_sums(a1, a1_t, h, dy[0], a0_t, gate, up, *weights)
        gradients = [gu[0], gu[1], down]
        count = sum(g.size for g in gradients)
        factor = jnp.minimum(1.0, 0.5 * lax.rsqrt(jnp.sum(squares) / count + 1e-30))
        new = [adamw(w.astype(F32), m, v, g.astype(F32) * factor) for w, m, v, g in zip(weights, m, v, gradients, strict=True)]
        return tuple(one[which] for which in range(3) for one in new)

    whole = P(None, None, None)
    return jax.shard_map(
        step,
        mesh=mesh,
        in_specs=(P(("rep", "dp"), None, None),) * 2 + (whole,) * 9,
        out_specs=(P("rep", None, None),) * 9,
        check_vma=False,
    )
```

```python
import functools

import jax
import jax.numpy as jnp
from jax import lax
from jax.experimental import pallas as pl
from jax.experimental.pallas import tpu as pltpu
from jax.sharding import PartitionSpec as P

LOGICAL = pl.DeviceIdType.LOGICAL
NX, NY, NZ, CORES = 4, 4, 8, 2
F32, BF16 = jnp.float32, jnp.bfloat16
NN = (((1,), (0,)), ((), ()))
NT = (((1,), (1,)), ((), ()))
TN = (((0,), (0,)), ((), ()))
ANY = pl.BlockSpec(memory_space=pl.ANY)
VMEM = pl.BlockSpec(memory_space=pltpu.VMEM)
SUBLANES, LANES = 16, 128
TILES, PARTS = 12, 1
BLOCK = (8, LANES)
NUMBER_OF_XFERS = 680


def dot(a, b, dims=NN):
    return lax.dot_general(a, b, dims, preferred_element_type=F32)


def scale_of(wide):
    return lax.rsqrt(jnp.mean(wide * wide, -1, keepdims=True) + 1e-6)


def normed(h):
    wide = h.astype(F32)
    return (wide * scale_of(wide)).astype(BF16)


def by_rows(n, step, body):
    def at(k, _):
        body(pl.ds(pl.multiple_of(k * step, step), step))
        return _

    lax.fori_loop(0, n // step, at, 0)


def turned(a, a_t):
    def slab(k, _):
        at = pl.ds(pl.multiple_of(k * LANES, LANES), LANES)
        a_t[at, :] = a[:, at].T
        return _

    lax.fori_loop(0, a.shape[1] // LANES, slab, 0)


def blocks_of(shape, index):
    return pl.BlockSpec(shape, lambda j: index(j))


def backward_tile(g, u, dp):
    sig = jax.nn.sigmoid(g)
    act = g * sig
    return (act * u).astype(BF16), (dp * u * (sig + act * (1.0 - sig))).astype(BF16), (dp * act).astype(BF16)


def layers_kernel(tiles, x_ref, dy_ref, wg_ref, wu_ref, wd_ref, g_ref, u_ref, a0_t, dh_ref, dwg_ref, dwu_ref, dwd_ref, a_s, a_t, h_s, by_g, by_u, p_s, dg_s, du_s):
    j = pl.program_id(0)
    n, d = x_ref.shape
    blocks = [pl.ds(k * (n // 4), n // 4) for k in range(4)]

    def clear(rows):
        by_g[rows, :] = jnp.zeros_like(by_g[rows, :])

    @pl.when(j == 0)
    def _():
        def body(rows):
            a_s[rows, :] = normed(x_ref[rows, :])
            clear(rows)

        by_rows(n, 64, body)
        turned(a_s, a0_t)

    @pl.when(j < tiles)
    def _():
        for rows in blocks:
            a = a_s[rows, :]
            g = dot(a, wg_ref[0])
            u = dot(a, wu_ref[0])
            for to, by in ((g_ref, g), (u_ref, u)):
                for t in range(to.shape[0]):
                    to[t, rows, :] = by[:, t * to.shape[2] : (t + 1) * to.shape[2]]
            by_g[rows, :] += dot((g * jax.nn.sigmoid(g) * u).astype(BF16), wd_ref[0])

    @pl.when(j == tiles - 1)
    def _():
        def body(rows):
            h = x_ref[rows, :] + by_g[rows, :].astype(BF16)
            h_s[rows, :] = h
            a_s[rows, :] = normed(h)
            clear(rows)
            by_u[rows, :] = jnp.zeros_like(by_u[rows, :])

        by_rows(n, 64, body)
        turned(a_s, a_t)

    @pl.when(j >= tiles)
    def _():
        for rows in blocks:
            a = a_s[rows, :]
            dp = dot(dy_ref[rows, :], wd_ref[0], NT).astype(BF16).astype(F32)
            p_s[rows, :], dg, du = backward_tile(dot(a, wg_ref[0]), dot(a, wu_ref[0]), dp)
            dg_s[rows, :], du_s[rows, :] = dg, du
            by_g[rows, :] += dot(dg, wg_ref[0], NT)
            by_u[rows, :] += dot(du, wu_ref[0], NT)
        dwg_ref[...] = dot(a_t[...], dg_s[...]).astype(BF16)
        dwu_ref[...] = dot(a_t[...], du_s[...]).astype(BF16)
        dwd_ref[...] = dot(p_s[...], dy_ref[...], TN).astype(BF16)

    @pl.when(j == pl.num_programs(0) - 1)
    def _():
        def body(rows):
            by_a = (by_g[rows, :].astype(BF16) + by_u[rows, :].astype(BF16)).astype(F32)
            wide = h_s[rows, :].astype(F32)
            s = scale_of(wide)
            by_h = by_a * s - wide * (s * s * s * jnp.mean(by_a * wide, -1, keepdims=True))
            dh_ref[rows, :] = dy_ref[rows, :] + by_h.astype(BF16)

        by_rows(n, 32, body)


def layers(x, dy, wg, wu, wd, tile=512):
    (n, d), ff = x.shape, wg.shape[-1]
    tiles, per = ff // tile, tile * TILES // ff
    early, late = lambda j: jnp.minimum(j, tiles - 1), lambda j: jnp.maximum(j - tiles, 0)
    whole, turned_ = blocks_of((n, d), lambda j: (0, 0)), blocks_of((d, n), lambda j: (0, 0))
    wide = blocks_of((per, n, ff // TILES), lambda j: (early(j), 0, 0))
    weight = blocks_of((1, d, tile), lambda j: (j // tiles, 0, j % tiles))
    across = blocks_of((d, tile), lambda j: (0, late(j)))
    V = lambda *s: pltpu.VMEM(s, BF16)
    return pl.pallas_call(
        functools.partial(layers_kernel, tiles),
        name="layers",
        grid=(2 * tiles,),
        in_specs=[whole, whole, weight, weight, blocks_of((1, tile, d), lambda j: (j // tiles, j % tiles, 0))],
        out_specs=[wide, wide, turned_, whole, across, across, blocks_of((tile, d), lambda j: (late(j), 0))],
        out_shape=[jax.ShapeDtypeStruct((TILES, n, ff // TILES), F32)] * 2 + [jax.ShapeDtypeStruct(s, BF16) for s in ((d, n), (n, d), (d, ff), (d, ff), (ff, d))],
        scratch_shapes=[V(n, d), V(d, n), V(n, d), pltpu.VMEM((n, d), F32), pltpu.VMEM((n, d), F32), V(n, tile), V(n, tile), V(n, tile)],
        compiler_params=pltpu.CompilerParams(vmem_limit_bytes=62 << 20),
    )(x, dy, wg, wu, wd)


def div(a, b):
    return lax.div(a, jnp.int32(b))


def rem(a, b):
    return lax.rem(a, jnp.int32(b))


def once(f):
    known = {}

    def g(s, i):
        key = s, id(i)
        if key not in known:
            known[key] = i, f(s, i)
        return known[key][1]

    return g


@once
def first(s, i):
    return NX - 1 - i if s else i + 1 - 2 * rem(i, 2)


def second(s, i):
    return first(1 - s, i)


@once
def half(s, i):
    return div(i, 2) if s else rem(div(i + 1, 2), 2)


@once
def part(s, i):
    return rem(i, 2) if s else div(i, 2)


@once
def quarter(s, i):
    return 2 * half(s, i) + part(s, i)


def place(start, size, unit):
    return pl.ds(start if isinstance(start, int) else pl.multiple_of(start, unit), size)


class Xfer:
    def __init__(self, link, count, hops, src, dst, dev):
        self.link, self.count, self.size, self.src, self.dst, self.dev = link, count, 2 * count * hops, src, dst, dev
        self.arrives = None


class Event:
    def __init__(self, waits, pre, work, cost, sends, late):
        self.waits, self.pre, self.work, self.cost, self.sends, self.late = waits, pre, work, cost, sends, late
        self.done = None


RATE, CHIP_RATE, DELAY, GAP, SLACK = 46.0e3, 450.0e3, 2.3, 0.1, 0.5
LATE = {("share", 0): -2, ("share", 1): 2, ("across", 0): 1, ("across", 1): 2, ("halve", 0): 1, ("round", 0): -2}
STEP = (0.6, 0.6, 0.65, 0.65, 0.65)
SLOTS = STEP * TILES


def order_of(events, slots):
    links, left, groups, clock, done = {}, list(events), [[]], 0.0, 0
    while left:
        best = None
        for e in left:
            if any(done < p if isinstance(p, int) else p.done is None for p in e.pre) or any(t.arrives is None for t in e.waits):
                continue
            ready = max([p.done for p in e.pre if not isinstance(p, int)] + [t.arrives + (SLACK if done < len(slots) else 0.0) for t in e.waits] + [0.0])
            if best is None or max(ready, clock) + e.late < best[0] + best[1].late:
                best = (max(ready, clock), e)
        if done < len(slots) and (best is None or best[0] + best[1].late > clock):
            clock += slots[done]
            done += 1
            groups.append([])
            continue
        clock, e = best
        clock += e.cost
        e.done = clock
        for t in e.sends:
            begin = max(clock, links.get(t.link, 0.0))
            links[t.link] = begin + GAP + t.size / (CHIP_RATE if t.link == "chip" else RATE)
            t.arrives = links[t.link] + DELAY
        left.remove(e)
        groups[-1].append(e)
    return groups, clock


def plan(here, refs, ru, cu):
    x, y, z, core = here
    (grads, own_ab, own_c, p_ab, p_c, r1, r2, r3, r4, rz, rc, rx, ry, f_ab, f_c, acc, norms, gu_out, dn_out, sq_out, total, squares, need, local) = refs
    other = 1 - core
    xfers, events = [], []
    part_of = functools.partial

    devices, me = {}, ((x * NY + y) * NZ + z) * CORES + core
    steps = dict(x=(x, NY * NZ * CORES), y=(y, NZ * CORES), z=(z, CORES), core=(core, 1))

    def at(**to):
        ((axis, there),) = to.items()
        if (axis, id(there)) not in devices:
            i, stride = steps[axis]
            devices[axis, id(there)] = there, me + (there - i) * stride
        return devices[axis, id(there)][1]

    def window(ref, lead, row, rows, col, cols):
        return lambda: ref.at[(*lead, place(row, rows, SUBLANES), place(col, cols, LANES))]

    def block(ref, *lead):
        return lambda: ref.at[lead]

    def xfer(link, count, src, dst, hops=1, **to):
        t = Xfer(link, count, hops, src, dst, at(**to))
        xfers.append(t)
        return t

    others = {axis: [rem(k + d, n) for d in range(1, n)] for axis, k, n in (("x", x, NX), ("y", y, NY), ("z", z, NZ), ("core", core, CORES))}

    def to_all(axis, n, size, src, dst):
        ts = []
        for d in range(1, n):
            to, back = others[axis][d - 1], d * 2 > n
            ts.append(xfer(axis + "+-"[back], size, src(d, to), dst(d, to), n - d if back else d, **{axis: to}))
        return ts

    def event(waits, pre, work=lambda: None, cost=0.05, sends=()):
        e = Event(waits, pre, work, cost, sends, LATE.get(kind, 0))
        events.append(e)
        return e

    kind = None

    def adds(size, n):
        return size * n / 2.0e6 + 0.15

    D, FF = SUBLANES * ru, NZ * cu
    HD, S = D // 2, D // 4
    HC, QC = FF // 2, FF // 4
    CR = cu // 2
    XR = CR // 4
    around = [z * CR] + [to * CR for to in others["z"]]
    arrived, pieces = [], []

    for i in range(2 * PARTS):
        l, f0 = 1 - i // PARTS, i % PARTS * FF
        kind = "halve", l
        begins = {}
        if l:
            for s in range(2):
                for c in range(2):
                    begins[c, s] = xfer("chip", S * FF, window(grads[c], (), other * HD + s * S, S, f0, FF), window(p_ab, (i, c), s * S, S, 0, FF), core=other)
                begins[2, s] = xfer("chip", HC * HD, window(grads[2], (), f0 + s * HC, HC, other * HD, HD), window(p_c, (i,), s * HC, HC, 0, HD), core=other)
            e = event([], [], sends=list(begins.values()))
            begins = {k: event([t], [e], part_of(need, (i, *k))) for k, t in begins.items()}
        else:
            e = event([], [len(SLOTS) * (i % PARTS + 1) // PARTS], part_of(need, (i, 0, 0)), 0.3)
            begins = {(c, s): e for c in range(3) for s in range(2)}

        ends = []
        for c in range(2):
            ri, ci, rax, cax = (y, x, "y", "x") if c else (x, y, "x", "y")
            for s in range(2):
                k1, k2, e1, e2 = (i, c), (i, c, s), "+-"[s], "-+"[s]
                b1, b2, c1, c2 = half(s, ri), part(s, ri), half(s, ci), part(s, ci)
                keep = s * S + b1 * 2 * ru
                away, out, q = s * S + (1 - b1) * 2 * ru, keep + (1 - b2) * ru, keep + b2 * ru
                col1, col2, mine = (1 - c1) * HC, c1 * HC + (1 - c2) * QC, c1 * HC + c2 * QC
                t1 = xfer(rax + e1, 2 * ru * FF, window(p_ab, k1, away, 2 * ru, 0, FF), block(r1, *k2), **{rax: first(s, ri)})
                t2 = xfer(rax + e2, ru * FF, window(p_ab, k1, out, ru, 0, FF), block(r2, *k2), **{rax: second(s, ri)})
                t3 = xfer(cax + e1, ru * HC, window(p_ab, k1, q, ru, col1, HC), block(r3, *k2), **{cax: first(s, ci)})
                t4 = xfer(cax + e2, ru * QC, window(p_ab, k1, q, ru, col2, QC), block(r4, *k2), **{cax: second(s, ci)})

                def work(row, col, rows, cols, n, k1=k1, k2=k2, b2=b2, c1=c1):
                    to = (k1, row, col)
                    more = [(r1, k2, (b2 if n > 1 else 1 - b2) * ru, col), (r2, k2, 0, col), (r3, k2, 0, col - c1 * HC), (r4, k2, 0, 0)]
                    total((p_ab, *to), [(p_ab, *to), (own_ab, *to)] + more[:n], rows, cols)

                e, prev = begins[c, s], []
                for n, (t, row, col, rows, cols) in enumerate(((t1, away, 0, 2 * ru, FF), (t2, out, 0, ru, FF), (t3, q, col1, ru, HC), (t4, q, col2, ru, QC), (None, q, mine, ru, QC))):
                    e = event(prev, [e], part_of(work, row, col, rows, cols, n), adds(rows * cols, n + 2), [t] if t else [])
                    prev = [t]
                ends.append(e)

        def piece(to):
            c, k = div(to, 4), rem(to, 4)
            s, h = div(k, 2), rem(k, 2)
            qx = quarter(0, x) + s * (quarter(1, x) - quarter(0, x))
            qy = quarter(0, y) + s * (quarter(1, y) - quarter(0, y))
            return c, s * S + (qx + c * (qy - qx)) * ru, (qy + c * (qx - qy)) * QC + h * cu

        def from_piece(d, to, i=i):
            c, a, b = piece(to)
            return window(p_ab, (i, c), a, ru, b, cu)

        kind = "share", l
        tz = to_all("z", NZ, ru * cu, from_piece, lambda d, to, i=i: block(rz, i, d - 1))
        e = event([], ends, sends=tz)
        mc, ma, mb = piece(z)
        home, mine = window(gu_out, (mc, l), core * HD + ma, ru, f0 + mb, cu), block(f_ab, i)

        def work(i=i, mc=mc, ma=ma, mb=mb, mine=mine, home=home):
            total((f_ab, (i,), 0, 0), [(p_ab, (i, mc), ma, mb)] + [(rz, (i, d), 0, 0) for d in range(NZ - 1)], ru, cu)
            squares(f_ab, (i,), 1.0)
            local(i, 0, mine, home).start()

        ta = to_all("z", NZ, ru * cu, lambda d, to, m=mine: m, lambda d, to, h=home: h)
        e = event(tz, [e], work, 0.4, ta)
        pieces.append(e)
        spread = event(ta, [e], lambda i=i, mine=mine, home=home: local(i, 0, mine, home).wait(), 0.1)
        for c in range(2):
            ri, ci, rax, cax = (y, x, "y", "x") if c else (x, y, "x", "y")
            for s in range(2):
                e1, e2 = "+-"[s], "-+"[s]

                kind = "spread", l

                def same(link, row, rows, col, cols, l=l, c=c, f0=f0, s=s, **to):
                    ref = window(gu_out, (c, l), core * HD + s * S + row * ru, rows * ru, f0 + col, cols)
                    return xfer(link, rows * ru * cols, ref, ref, **to)

                q, b1 = quarter(s, ri), 2 * half(s, ri)
                ts = [same(cax + e2, q, 1, quarter(s, ci) * QC, QC, **{cax: second(s, ci)}), same(cax + e1, q, 1, half(s, ci) * HC, HC, **{cax: first(s, ci)}),
                      same(rax + e2, q, 1, 0, FF, **{rax: second(s, ri)}), same(rax + e1, b1, 2, 0, FF, **{rax: first(s, ri)})]
                fw = [same("chip", b, 2, 0, FF, core=other) for b in (b1, 2 - b1)]
                e = spread
                for n, t in enumerate(ts):
                    e = event(ts[n - 1 : n], [e], sends=[t] + fw[: n // 3])
                event(ts[-1:], [e], sends=fw[1:])
                arrived += fw

        for s in range(2):
            key, base, kind = (i, s), s * HC, ("down", l)
            arms = ((1, "z+", 0, 4 - s), (-1, "z-", 4 - s, 3 + s))
            chunk = lambda k, base=base: base + around[k % NZ]

            def work(slots, row, into, i=i, key=key):
                to = ((i,), row, 0)
                total(into or (p_c, *to), [(p_c, *to), (own_c, *to)] + [(rc, (*key, t), 0, 0) for t in slots], CR, HD)

            ends, lasts = [], []
            for sg, zl, slot, n in arms:
                nxt, e, prev = others["z"][-(sg < 0)], begins[2, s], []
                for t in range(n):
                    row, into = chunk(sg * (n - t)), (rc, (*key, slot + t - 1), 0, 0) if t else None
                    ring = xfer(zl, CR * HD, block(rc, *key, slot + t - 1) if t else window(p_c, (i,), row, CR, 0, HD), block(rc, *key, slot + t), z=nxt)
                    e = event(prev, [e], part_of(work, [slot + t - 1] if t else [], row, into), adds(CR * HD, 3), [ring])
                    prev = [ring]
                ends.append(e)
                lasts += prev
            tx = to_all("x", NX, XR * HD, lambda d, to, key=key: window(rc, (*key, 3 - key[1]), to * XR, XR, 0, HD), lambda d, to, key=key: block(rx, *key, d - 1))
            e = event(lasts, ends, part_of(work, [3 - s, NZ - 2], chunk(0), (rc, (*key, 3 - s), 0, 0)), adds(CR * HD, 4), tx)

            def work_x(key=key):
                total((ry, (*key, y), 0, 0), [(rc, (*key, 3 - key[1]), x * XR, 0)] + [(rx, (*key, d), 0, 0) for d in range(NX - 1)], XR, HD)

            mine, kind = block(ry, *key, y), ("across", l)
            ty = to_all("y", NY, XR * HD, lambda d, to, m=mine: m, lambda d, to, m=mine: m)
            e = event(tx, [e], work_x, adds(XR * HD, 4), ty)
            home, mine = window(dn_out, (l,), f0 + base + z * CR + x * XR, XR, core * HD, HD), block(f_c, *key)

            def work_y(key=key, mine=mine, home=home):
                total((f_c, key, 0, 0), [(ry, (*key, k), 0, 0) for k in range(NY)], XR, HD)
                squares(f_c, key, 1.0 / NY)
                local(key[0], 1 + key[1], mine, home).start()

            hx = to_all("x", NX, XR * HD, lambda d, to, m=mine: m, lambda d, to, h=home: h)
            e = event(ty, [e], work_y, 0.3, hx)
            pieces.append(e)
            e = event(hx, [e, spread], lambda key=key, mine=mine, home=home: local(key[0], 1 + key[1], mine, home).wait(), 0.1)
            prev, ends = [[], []], [e, e]
            kind = "round", l
            for t in range(4):
                for k, (sg, zl, slot, n) in enumerate(arms):
                    if t < n:
                        ref = window(dn_out, (l,), f0 + chunk(-sg * t), CR, core * HD, HD)
                        ring = xfer(zl, CR * HD, ref, ref, z=others["z"][-(sg < 0)])
                        ends[k] = event(prev[k], [ends[k]], sends=[ring])
                        prev[k] = [ring]
            ref = window(dn_out, (l,), f0 + base, HC, core * HD, HD)
            arrived.append(xfer("chip", HC * HD, ref, ref, core=other))
            event(prev[0] + prev[1], ends, sends=arrived[-1:])

    kind = None
    e, ts, prev = None, [], None
    for axis, k, n, ref in (("z", z, NZ, norms[0]), ("y", y, NY, norms[1]), ("x", x, NX, norms[2]), ("core", core, CORES, norms[3])):
        def work(ref=ref, k=k, prev=prev):
            if prev is None:
                ref[k] = acc[...]
            else:
                ref[k] = functools.reduce(lambda a, b: a + b, [prev[0][j] for j in range(prev[1])])

        new = [xfer("n", SUBLANES * LANES, block(ref, k), block(ref, k), **{axis: to}) for to in others[axis]]
        e = event(ts, pieces if e is None else [e], work, 0.15, new)
        ts, prev = new, (ref, n)

    def finish():
        sq_out[...] = norms[3][0] + norms[3][1]

    event(ts, [e], finish, 0.1)
    event(arrived, [])
    return xfers, events


def sum_kernel(ru, cu, *refs):
    (g1, u1, d1, a0_t, dh, gate, up, wd, gu_out, dn_out, sq_out, own_ab, own_c, p_ab, p_c, r1, r2, r3, r4, rz, rc, rx, ry, f_ab, f_c,
     acc, nz, ny, nx, nc, gbuf, ubuf, wbuf, p_s, dg_s, du_s, st_ab, st_c, send_sem, recv_sem, load_sem, keep_sem, tile_sem, out_sem, in_sem) = refs
    me = lax.axis_index("dp")
    core, z, y, x = rem(me, CORES), rem(div(me, CORES), NZ), rem(div(me, CORES * NZ), NY), div(me, CORES * NZ * NY)
    other = 1 - core
    D = SUBLANES * ru
    HD = D // 2
    n = dh.shape[0]
    per = TILES // PARTS
    tile = NZ * cu // per
    partner = me + 1 - 2 * core
    slice_of = lambda j: pl.ds(pl.multiple_of(j * tile, LANES), tile)

    mine, yours = (pl.ds(pl.multiple_of(c * HD, LANES), HD) for c in (core, other))
    loads = [pltpu.make_async_copy(src, dst, load_sem.at[k]) for k, (src, dst) in enumerate(((g1.at[mine, :], own_ab.at[0, 0]), (u1.at[mine, :], own_ab.at[0, 1]),
                                                                                             (d1.at[:, mine], own_c.at[0])))]
    for t in loads:
        t.start()

    barrier = pltpu.get_barrier_semaphore()
    dev = lambda x, y, z, core: ((x * NY + y) * NZ + z) * CORES + core
    peers = [dev(x, y, z, other)] + [dev(rem(x + d, NX), y, z, core) for d in range(1, NX)]
    peers += [dev(x, rem(y + d, NY), z, core) for d in range(1, NY)] + [dev(x, y, rem(z + d, NZ), core) for d in range(1, NZ)]
    for p in peers:
        pl.semaphore_signal(barrier, inc=1, device_id=p, device_id_type=LOGICAL)
    pl.semaphore_wait(barrier, len(peers))

    def tile_sends(j, srcs=None, slot=0):
        i, cols = PARTS + div(j, per), slice_of(rem(j, per))
        dsts = [p_ab.at[i, c, :, cols] for c in range(2)] + [p_c.at[i, cols, :]]
        return [pltpu.make_async_remote_copy(src_ref=src, dst_ref=dst, send_sem=out_sem.at[slot, k], recv_sem=in_sem.at[j, k], device_id=partner,
                                             device_id_type=LOGICAL) for k, (src, dst) in enumerate(zip(srcs or dsts, dsts, strict=True))]

    def total(dst, srcs, rows, cols):
        wide = next(cols // k for k in range(1, cols) if cols % (k * LANES) == 0 and cols // k <= 4 * LANES)
        tall = next(rows // k for k in range(1, rows) if rows % (k * SUBLANES) == 0 and rows // k * wide <= SUBLANES * LANES * 16)
        across = cols // wide

        many = rows // tall * across

        def block(i, _):
            if many > 1:
                r, c = (div(i, across) * tall, rem(i, across) * wide) if across > 1 else (i * tall, None)

            def at(a):
                ref, lead, row, col = a
                row, col = (row, col) if many == 1 else (row + r, col if c is None else col + c)
                return ref.at[(*lead, place(row, tall, SUBLANES), place(col, wide, LANES))]

            s = at(srcs[0])[...].astype(F32)
            for a in srcs[1:]:
                s = s + at(a)[...].astype(F32)
            at(dst)[...] = s.astype(BF16)
            return _

        if many > 1:
            lax.fori_loop(0, many, block, 0)
        else:
            block(0, 0)

    def squares(ref, lead, weight):
        rows, cols = ref.shape[len(lead):]
        for r in range(0, rows, SUBLANES):
            v = ref[(*lead, pl.ds(r, SUBLANES), slice(None))].astype(F32)
            v = v * v
            s = acc[...]
            for a in range(0, SUBLANES, BLOCK[0]):
                for b in range(0, cols, LANES):
                    s = s + weight * v[a : a + BLOCK[0], b : b + LANES]
            acc[...] = s

    def need(key):
        i, c, s = key
        if i < PARTS:
            if s == 0:
                loads[c].wait()
            return

        def wait(j, _):
            for t in tile_sends(j):
                t.wait_recv()
            return _

        lax.fori_loop((i - PARTS) * per, (i - PARTS + 1) * per, wait, 0)

    def local(l, k, src, dst):
        return pltpu.make_async_copy(src(), dst(), keep_sem.at[l, k])

    acc[...] = jnp.zeros_like(acc)
    xfers, events = plan((x, y, z, core), ((g1, u1, d1), own_ab, own_c, p_ab, p_c, r1, r2, r3, r4, rz, rc, rx, ry, f_ab, f_c, acc, (nz, ny, nx, nc),
                                           gu_out, dn_out, sq_out, total, squares, need, local), ru, cu)
    counts = sorted(t.count for t in xfers)
    ids = {id(t): k for k, t in enumerate(sorted(xfers, key=lambda t: t.count))}
    groups, _ = order_of(events, SLOTS)

    def copy_of(src, dst, k, dev):
        return pltpu.make_async_remote_copy(src_ref=src, dst_ref=dst, send_sem=send_sem.at[k], recv_sem=recv_sem.at[k], device_id=dev, device_id_type=LOGICAL)

    def wait_of(count, k):
        cols = next(c for c in range(NZ * cu, 0, -LANES) if count % (c * SUBLANES) == 0)
        some = p_ab.at[0, 0, pl.ds(0, count // cols), pl.ds(0, cols)]
        return copy_of(some, some, k, me)

    def emit(group):
        for e in group:
            for t in e.waits:
                wait_of(t.count, ids[id(t)]).wait_recv()
            e.work()
            for t in e.sends:
                copy_of(t.src(), t.dst(), ids[id(t)], t.dev).start()

    def choose(j, options):
        middle = len(options) // 2
        if middle == 0:
            emit(options[0])
        elif any(options):
            pl.when(j < middle)(lambda: choose(j, options[:middle]))
            pl.when(j >= middle)(lambda: choose(j - middle, options[middle:]))

    def steps(srcs, bufs, *parts):
        mine = groups[: TILES * len(parts)]
        del groups[: TILES * len(parts)]

        def copies(j, slot):
            return [pltpu.make_async_copy(src(j), buf.at[slot], tile_sem.at[slot, k]) for k, (src, buf) in enumerate(zip(srcs, bufs, strict=True))]

        for t in copies(0, 0):
            t.start()

        def step(j, carry):
            slot = rem(j, 2)
            for t in copies(j, slot):
                t.wait()

            @pl.when(j + 1 < TILES)
            def _():
                for t in copies(j + 1, 1 - slot):
                    t.start()

            for k, part in enumerate(parts):
                part(j, slot)
                choose(j, mine[k :: len(parts)])
            return carry

        lax.fori_loop(0, TILES, step, 0)

    emit(groups.pop(0))
    tail = groups.pop()
    groups.append([])

    rows_in, rows_out = (pl.ds(pl.multiple_of(c * HD, SUBLANES), HD) for c in (core, other))
    staged = lambda slot: [st_ab.at[slot, 0, rows_out, :], st_ab.at[slot, 1, rows_out, :], st_c.at[slot, :, yours]]
    blocks = [pl.ds(k * (n // 4), n // 4) for k in range(4)]

    def through(which, j, slot):
        if which == 0:
            @pl.when(j > 1)
            def _():
                for t in tile_sends(j - 2, staged(slot), slot):
                    t.wait_send()

        for rows in blocks[which::2]:
            dp = dot(dh[rows, :], wbuf[slot], NT).astype(BF16).astype(F32)
            p_s[rows, :], dg_s[rows, :], du_s[rows, :] = backward_tile(gbuf[slot, rows, :], ubuf[slot, rows, :], dp)

    def term(c, j, slot):
        i, cols = PARTS + div(j, per), slice_of(rem(j, per))
        if c < 2:
            st_ab[slot, c] = dot(a0_t[...], (dg_s, du_s)[c][...]).astype(BF16)
            own_ab[i, c, :, cols] = st_ab[slot, c, rows_in, :]
        else:
            st_c[slot] = dot(p_s[...], dh[...], TN).astype(BF16)
            own_c[i, cols, :] = st_c[slot, :, mine]
            for t in tile_sends(j, staged(slot), slot):
                t.start()

    steps([lambda j: gate.at[j], lambda j: up.at[j], lambda j: wd.at[0, slice_of(j), :]], [gbuf, ubuf, wbuf],
          *[functools.partial(f, k) for f, k in ((through, 0), (through, 1), (term, 0), (term, 1), (term, 2))])
    for k in range(2):
        for t in tile_sends(TILES - 2 + k, staged(k), k):
            t.wait_send()
    emit(tail)
    for count in sorted(set(counts)):
        def wait(k, carry, count=count):
            wait_of(count, k).wait_send()
            return carry

        lax.fori_loop(counts.index(count), counts.index(count) + counts.count(count), wait, 0)


def gradient_sums(g1, u1, d1, a0_t, dh, gate, up, wd):
    (n, d), ff = dh.shape, g1.shape[1]
    ru, cu = d // SUBLANES, ff // NZ // PARTS
    HD, CR, fs, N, tile = d // 2, cu // 2, ff // PARTS, 2 * PARTS, ff // TILES
    V = lambda *s: pltpu.VMEM(s, BF16)
    W = lambda *s: pltpu.VMEM(s, F32)
    DMA = lambda *s: pltpu.SemaphoreType.DMA(s)
    return pl.pallas_call(
        functools.partial(sum_kernel, ru, cu),
        name="gradient_sums",
        out_shape=(jax.ShapeDtypeStruct((2, 2, d, ff), BF16), jax.ShapeDtypeStruct((2, ff, d), BF16), jax.ShapeDtypeStruct(BLOCK, F32)),
        in_specs=[ANY] * 3 + [VMEM] * 2 + [ANY] * 3,
        out_specs=(ANY, ANY, VMEM),
        scratch_shapes=[
            V(N, 2, HD, fs), V(N, fs, HD), V(N, 2, HD, fs), V(N, fs, HD),
            V(N, 2, 2, 2 * ru, fs), V(N, 2, 2, ru, fs), V(N, 2, 2, ru, fs // 2), V(N, 2, 2, ru, fs // 4),
            V(N, NZ - 1, ru, cu), V(N, 2, NZ - 1, CR, HD), V(N, 2, NX - 1, CR // 4, HD), V(N, 2, NY, CR // 4, HD), V(N, ru, cu), V(N, 2, CR // 4, HD),
            W(*BLOCK), W(NZ, *BLOCK), W(NY, *BLOCK), W(NX, *BLOCK), W(CORES, *BLOCK),
            W(2, n, tile), W(2, n, tile), V(2, tile, d), V(n, tile), V(n, tile), V(n, tile), V(2, 2, d, tile), V(2, tile, d),
            DMA(NUMBER_OF_XFERS), DMA(NUMBER_OF_XFERS), DMA(3), DMA(N, 3), DMA(2, 3), DMA(2, 3), DMA(TILES, 3),
        ],
        compiler_params=pltpu.CompilerParams(collective_id=0, has_side_effects=True, vmem_limit_bytes=62 << 20),
    )(g1, u1, d1, a0_t, dh, gate, up, wd)


def adamw(w, m, v, g):
    m = 0.9 * m + 0.1 * g
    v = 0.95 * v + 0.05 * g * g
    step = m * lax.rsqrt(v + 1e-8) + 0.1 * w
    return (w - 0.02 * step).astype(BF16), m, v


def optimizer_kernel(count, sq, *refs):
    factor = jnp.minimum(1.0, 0.5 * lax.rsqrt(jnp.sum(sq[...], keepdims=True) / count + 1e-30))
    ws, ms, vs, gs, *outs = (refs[i : i + 3] for i in range(0, len(refs), 3))
    for k in range(3):
        wide = ws[k].shape[-1]

        def rows_of(i, _, k=k, wide=wide):
            at = 0, pl.ds(pl.multiple_of(i * SUBLANES, SUBLANES), SUBLANES), slice(None)
            g = gs[k][(0,) * (len(gs[k].shape) - 3) + at].astype(F32) * factor
            for out, new in zip(outs, adamw(ws[k][at].astype(F32), ms[k][at], vs[k][at], g), strict=True):
                out[k][at] = new
            return _

        lax.fori_loop(0, ws[k].shape[1] // SUBLANES, rows_of, 0)


def optimizer(sq, weights, m, v, gu, down, blocks=24):
    def spec(a, lead=()):
        l, rows, cols = a.shape[-3:]
        return pl.BlockSpec((1,) * len(lead) + (1, rows // blocks, cols), lambda j: (*lead, j // blocks, j % blocks, 0))

    plain = [spec(w) for w in weights]
    return pl.pallas_call(
        functools.partial(optimizer_kernel, sum(w.size for w in weights)),
        name="optimizer",
        grid=(2 * blocks,),
        in_specs=[pl.BlockSpec(sq.shape, lambda j: (0, 0))] + plain * 3 + [spec(gu, (0,)), spec(gu, (1,)), spec(down)],
        out_specs=plain * 3,
        out_shape=[jax.ShapeDtypeStruct(w.shape, t) for t in (BF16, F32, F32) for w in weights],
        compiler_params=pltpu.CompilerParams(vmem_limit_bytes=60 << 20),
    )(sq, *weights, *m, *v, gu, gu, down)


def solution(mesh):
    def step(x, dy, *arrays):
        weights, m, v = (arrays[i : i + 3] for i in (0, 3, 6))
        gate, up, a0_t, dh, *by_1 = layers(x[0], dy[0], *weights)
        gu, down, squares = gradient_sums(*by_1, a0_t, dh, gate, up, weights[2])
        return tuple(optimizer(squares, weights, m, v, gu, down))

    whole = P(None, None, None)
    return jax.shard_map(
        step,
        mesh=mesh,
        in_specs=(P(("rep", "dp"), None, None),) * 2 + (whole,) * 9,
        out_specs=(P("rep", None, None),) * 9,
        check_vma=False,
    )
```

```python
import functools

import jax
import jax.numpy as jnp
from jax import lax
from jax.experimental import pallas as pl
from jax.experimental.pallas import tpu as pltpu
from jax.sharding import PartitionSpec as P

LOGICAL = pl.DeviceIdType.LOGICAL
NX, NY, NZ, CORES = 4, 4, 8, 2
F32, BF16 = jnp.float32, jnp.bfloat16
NN = (((1,), (0,)), ((), ()))
NT = (((1,), (1,)), ((), ()))
TN = (((0,), (0,)), ((), ()))
ANY = pl.BlockSpec(memory_space=pl.ANY)
VMEM = pl.BlockSpec(memory_space=pltpu.VMEM)
SUBLANES, LANES = 16, 128
TILES, PARTS = 6, 1
BLOCK = (8, LANES)
NUMBER_OF_XFERS = 680


def dot(a, b, dims=NN):
    return lax.dot_general(a, b, dims, preferred_element_type=F32)


def scale_of(wide):
    return lax.rsqrt(jnp.mean(wide * wide, -1, keepdims=True) + 1e-6)


def normed(h):
    wide = h.astype(F32)
    return (wide * scale_of(wide)).astype(BF16)


def by_rows(n, step, body):
    def at(k, _):
        body(pl.ds(pl.multiple_of(k * step, step), step))
        return _

    lax.fori_loop(0, n // step, at, 0)


def turned(a, a_t):
    def slab(k, _):
        at = pl.ds(pl.multiple_of(k * LANES, LANES), LANES)
        a_t[at, :] = a[:, at].T
        return _

    lax.fori_loop(0, a.shape[1] // LANES, slab, 0)


def blocks_of(shape, index):
    return pl.BlockSpec(shape, lambda j: index(j))


def backward_tile(g, u, dp):
    sig = jax.nn.sigmoid(g)
    act = g * sig
    return (act * u).astype(BF16), (dp * u * (sig + act * (1.0 - sig))).astype(BF16), (dp * act).astype(BF16)


def layers_kernel(tiles, x_ref, dy_ref, wg_ref, wu_ref, wd_ref, g_ref, u_ref, a0_t, dh_ref, dwg_ref, dwu_ref, dwd_ref, a_s, a_t, h_s, by_g, by_u, p_s, dg_s, du_s):
    j = pl.program_id(0)
    n, d = x_ref.shape
    def clear(rows):
        by_g[rows, :] = jnp.zeros_like(by_g[rows, :])

    @pl.when(j == 0)
    def _():
        def body(rows):
            a_s[rows, :] = normed(x_ref[rows, :])
            clear(rows)

        by_rows(n, 64, body)
        turned(a_s, a0_t)

    @pl.when(j < tiles)
    def _():
        a = a_s[...]
        g = dot(a, wg_ref[0])
        u = dot(a, wu_ref[0])
        g_ref[0], u_ref[0] = g, u
        by_g[...] += dot((g * jax.nn.sigmoid(g) * u).astype(BF16), wd_ref[0])

    @pl.when(j == tiles - 1)
    def _():
        def body(rows):
            h = x_ref[rows, :] + by_g[rows, :].astype(BF16)
            h_s[rows, :] = h
            a_s[rows, :] = normed(h)
            clear(rows)
            by_u[rows, :] = jnp.zeros_like(by_u[rows, :])

        by_rows(n, 64, body)
        turned(a_s, a_t)

    @pl.when(j >= tiles)
    def _():
        a = a_s[...]
        dp = dot(dy_ref[...], wd_ref[0], NT).astype(BF16).astype(F32)
        p_s[...], dg_s[...], du_s[...] = backward_tile(dot(a, wg_ref[0]), dot(a, wu_ref[0]), dp)
        by_g[...] += dot(dg_s[...], wg_ref[0], NT)
        by_u[...] += dot(du_s[...], wu_ref[0], NT)
        dwg_ref[...] = dot(a_t[...], dg_s[...]).astype(BF16)
        dwu_ref[...] = dot(a_t[...], du_s[...]).astype(BF16)
        dwd_ref[...] = dot(p_s[...], dy_ref[...], TN).astype(BF16)

    @pl.when(j == pl.num_programs(0) - 1)
    def _():
        def body(rows):
            by_a = (by_g[rows, :].astype(BF16) + by_u[rows, :].astype(BF16)).astype(F32)
            wide = h_s[rows, :].astype(F32)
            s = scale_of(wide)
            by_h = by_a * s - wide * (s * s * s * jnp.mean(by_a * wide, -1, keepdims=True))
            dh_ref[rows, :] = dy_ref[rows, :] + by_h.astype(BF16)

        by_rows(n, 32, body)


def layers(x, dy, wg, wu, wd):
    (n, d), ff = x.shape, wg.shape[-1]
    tiles, tile = TILES, ff // TILES
    early, late = lambda j: jnp.minimum(j, tiles - 1), lambda j: jnp.maximum(j - tiles, 0)
    whole, turned_ = blocks_of((n, d), lambda j: (0, 0)), blocks_of((d, n), lambda j: (0, 0))
    wide = blocks_of((1, n, tile), lambda j: (early(j), 0, 0))
    weight = blocks_of((1, d, tile), lambda j: (j // tiles, 0, j % tiles))
    across = blocks_of((d, tile), lambda j: (0, late(j)))
    V = lambda *s: pltpu.VMEM(s, BF16)
    return pl.pallas_call(
        functools.partial(layers_kernel, tiles),
        name="layers",
        grid=(2 * tiles,),
        in_specs=[whole, whole, weight, weight, blocks_of((1, tile, d), lambda j: (j // tiles, j % tiles, 0))],
        out_specs=[wide, wide, turned_, whole, across, across, blocks_of((tile, d), lambda j: (late(j), 0))],
        out_shape=[jax.ShapeDtypeStruct((TILES, n, tile), F32)] * 2 + [jax.ShapeDtypeStruct(s, BF16) for s in ((d, n), (n, d), (d, ff), (d, ff), (ff, d))],
        scratch_shapes=[V(n, d), V(d, n), V(n, d), pltpu.VMEM((n, d), F32), pltpu.VMEM((n, d), F32), V(n, tile), V(n, tile), V(n, tile)],
        compiler_params=pltpu.CompilerParams(vmem_limit_bytes=62 << 20),
    )(x, dy, wg, wu, wd)


def div(a, b):
    return lax.div(a, jnp.int32(b))


def rem(a, b):
    return lax.rem(a, jnp.int32(b))


def once(f):
    known = {}

    def g(s, i):
        key = s, id(i)
        if key not in known:
            known[key] = i, f(s, i)
        return known[key][1]

    return g


@once
def first(s, i):
    return NX - 1 - i if s else i + 1 - 2 * rem(i, 2)


def second(s, i):
    return first(1 - s, i)


@once
def half(s, i):
    return div(i, 2) if s else rem(div(i + 1, 2), 2)


@once
def part(s, i):
    return rem(i, 2) if s else div(i, 2)


@once
def quarter(s, i):
    return 2 * half(s, i) + part(s, i)


def place(start, size, unit):
    return pl.ds(start if isinstance(start, int) else pl.multiple_of(start, unit), size)


class Xfer:
    def __init__(self, link, count, hops, src, dst, dev):
        self.link, self.count, self.size, self.src, self.dst, self.dev = link, count, 2 * count * hops, src, dst, dev
        self.arrives = None


class Event:
    def __init__(self, waits, pre, work, cost, sends, late):
        self.waits, self.pre, self.work, self.cost, self.sends, self.late = waits, pre, work, cost, sends, late
        self.done = None


RATE, CHIP_RATE, DELAY, GAP, SLACK = 43.0e3, 450.0e3, 2.0, 0.1, 0.5
LATE = {("share", 0): -2, ("share", 1): 2, ("across", 0): 1, ("across", 1): 2, ("halve", 0): 1, ("round", 0): -2}
STEP = (1.2, 1.2, 1.3, 1.3, 1.3)
SLOTS = STEP * TILES


def order_of(events, slots):
    links, left, groups, clock, done = {}, list(events), [[]], 0.0, 0
    while left:
        best = None
        for e in left:
            if any(done < p if isinstance(p, int) else p.done is None for p in e.pre) or any(t.arrives is None for t in e.waits):
                continue
            ready = max([p.done for p in e.pre if not isinstance(p, int)] + [t.arrives + (SLACK if done < len(slots) else 0.0) for t in e.waits] + [0.0])
            if best is None or max(ready, clock) + e.late < best[0] + best[1].late:
                best = (max(ready, clock), e)
        if done < len(slots) and (best is None or best[0] + best[1].late > clock):
            clock += slots[done]
            done += 1
            groups.append([])
            continue
        clock, e = best
        clock += e.cost
        e.done = clock
        for t in e.sends:
            begin = max(clock, links.get(t.link, 0.0))
            links[t.link] = begin + GAP + t.size / (CHIP_RATE if t.link == "chip" else RATE)
            t.arrives = links[t.link] + DELAY
        left.remove(e)
        groups[-1].append(e)
    return groups, clock


def plan(here, refs, ru, cu):
    x, y, z, core = here
    (grads, own_ab, own_c, p_ab, p_c, r1, r2, r3, r4, rz, rc, rx, ry, f_ab, f_c, acc, norms, gu_out, dn_out, sq_out, total, squares, need, local) = refs
    other = 1 - core
    xfers, events = [], []
    part_of = functools.partial

    devices, me = {}, ((x * NY + y) * NZ + z) * CORES + core
    steps = dict(x=(x, NY * NZ * CORES), y=(y, NZ * CORES), z=(z, CORES), core=(core, 1))

    def at(**to):
        ((axis, there),) = to.items()
        if (axis, id(there)) not in devices:
            i, stride = steps[axis]
            devices[axis, id(there)] = there, me + (there - i) * stride
        return devices[axis, id(there)][1]

    def window(ref, lead, row, rows, col, cols):
        return lambda: ref.at[(*lead, place(row, rows, SUBLANES), place(col, cols, LANES))]

    def block(ref, *lead):
        return lambda: ref.at[lead]

    def xfer(link, count, src, dst, hops=1, **to):
        t = Xfer(link, count, hops, src, dst, at(**to))
        xfers.append(t)
        return t

    others = {axis: [rem(k + d, n) for d in range(1, n)] for axis, k, n in (("x", x, NX), ("y", y, NY), ("z", z, NZ), ("core", core, CORES))}

    def to_all(axis, n, size, src, dst):
        ts = []
        for d in range(1, n):
            to, back = others[axis][d - 1], d * 2 > n
            ts.append(xfer(axis + "+-"[back], size, src(d, to), dst(d, to), n - d if back else d, **{axis: to}))
        return ts

    def event(waits, pre, work=lambda: None, cost=0.05, sends=()):
        e = Event(waits, pre, work, cost, sends, LATE.get(kind, 0))
        events.append(e)
        return e

    kind = None

    def adds(size, n):
        return size * n / 2.0e6 + 0.15

    D, FF = SUBLANES * ru, NZ * cu
    HD, S = D // 2, D // 4
    HC, QC = FF // 2, FF // 4
    CR = cu // 2
    XR = CR // 4
    around = [z * CR] + [to * CR for to in others["z"]]
    arrived, copies, pieces = [], [], []

    for i in range(2 * PARTS):
        l, f0 = 1 - i // PARTS, i % PARTS * FF
        kind = "halve", l
        begins = {}
        if l:
            for s in range(2):
                for c in range(2):
                    begins[c, s] = xfer("chip", S * FF, window(grads[c], (), other * HD + s * S, S, f0, FF), window(p_ab, (i, c), s * S, S, 0, FF), core=other)
                begins[2, s] = xfer("chip", HC * HD, window(grads[2], (), f0 + s * HC, HC, other * HD, HD), window(p_c, (i,), s * HC, HC, 0, HD), core=other)
            e = event([], [], sends=list(begins.values()))
            begins = {k: event([t], [e], part_of(need, (i, *k))) for k, t in begins.items()}
        else:
            e = event([], [len(SLOTS) * (i % PARTS + 1) // PARTS], part_of(need, (i, 0, 0)), 0.3)
            begins = {(c, s): e for c in range(3) for s in range(2)}

        ends = []
        for c in range(2):
            ri, ci, rax, cax = (y, x, "y", "x") if c else (x, y, "x", "y")
            for s in range(2):
                k1, k2, e1, e2 = (i, c), (i, c, s), "+-"[s], "-+"[s]
                b1, b2, c1, c2 = half(s, ri), part(s, ri), half(s, ci), part(s, ci)
                keep = s * S + b1 * 2 * ru
                away, out, q = s * S + (1 - b1) * 2 * ru, keep + (1 - b2) * ru, keep + b2 * ru
                col1, col2, mine = (1 - c1) * HC, c1 * HC + (1 - c2) * QC, c1 * HC + c2 * QC
                t1 = xfer(rax + e1, 2 * ru * FF, window(p_ab, k1, away, 2 * ru, 0, FF), block(r1, *k2), **{rax: first(s, ri)})
                t2 = xfer(rax + e2, ru * FF, window(p_ab, k1, out, ru, 0, FF), block(r2, *k2), **{rax: second(s, ri)})
                t3 = xfer(cax + e1, ru * HC, window(p_ab, k1, q, ru, col1, HC), block(r3, *k2), **{cax: first(s, ci)})
                t4 = xfer(cax + e2, ru * QC, window(p_ab, k1, q, ru, col2, QC), block(r4, *k2), **{cax: second(s, ci)})

                def work(row, col, rows, cols, n, k1=k1, k2=k2, b2=b2, c1=c1):
                    to = (k1, row, col)
                    more = [(r1, k2, (b2 if n > 1 else 1 - b2) * ru, col), (r2, k2, 0, col), (r3, k2, 0, col - c1 * HC), (r4, k2, 0, 0)]
                    total((p_ab, *to), [(p_ab, *to), (own_ab, *to)] + more[:n], rows, cols)

                e, prev = begins[c, s], []
                for n, (t, row, col, rows, cols) in enumerate(((t1, away, 0, 2 * ru, FF), (t2, out, 0, ru, FF), (t3, q, col1, ru, HC), (t4, q, col2, ru, QC), (None, q, mine, ru, QC))):
                    e = event(prev, [e], part_of(work, row, col, rows, cols, n), adds(rows * cols, n + 2), [t] if t else [])
                    prev = [t]
                ends.append(e)

        def piece(to):
            c, k = div(to, 4), rem(to, 4)
            s, h = div(k, 2), rem(k, 2)
            qx = quarter(0, x) + s * (quarter(1, x) - quarter(0, x))
            qy = quarter(0, y) + s * (quarter(1, y) - quarter(0, y))
            return c, s * S + (qx + c * (qy - qx)) * ru, (qy + c * (qx - qy)) * QC + h * cu

        def from_piece(d, to, i=i):
            c, a, b = piece(to)
            return window(p_ab, (i, c), a, ru, b, cu)

        kind = "share", l
        tz = to_all("z", NZ, ru * cu, from_piece, lambda d, to, i=i: block(rz, i, d - 1))
        e = event([], ends, sends=tz)
        mc, ma, mb = piece(z)
        home, mine = window(own_ab, (i, mc), ma, ru, mb, cu), block(f_ab, i)

        def work(i=i, mc=mc, ma=ma, mb=mb):
            total((f_ab, (i,), 0, 0), [(p_ab, (i, mc), ma, mb)] + [(rz, (i, d), 0, 0) for d in range(NZ - 1)], ru, cu)
            squares(f_ab, (i,), 1.0)
            total((own_ab, (i, mc), ma, mb), [(f_ab, (i,), 0, 0)], ru, cu)

        ta = to_all("z", NZ, ru * cu, lambda d, to, m=mine: m, lambda d, to, h=home: h)
        e = event(tz, [e], work, 0.4, ta)
        pieces.append(e)
        spread = event(ta, [e])
        for c in range(2):
            ri, ci, rax, cax = (y, x, "y", "x") if c else (x, y, "x", "y")
            for s in range(2):
                e1, e2 = "+-"[s], "-+"[s]

                kind = "spread", l

                def same(link, row, rows, col, cols, i=i, l=l, c=c, f0=f0, s=s, **to):
                    ref = window(own_ab, (i, c), s * S + row * ru, rows * ru, col, cols)
                    out = ref if link != "chip" else window(gu_out, (c, l), core * HD + s * S + row * ru, rows * ru, f0 + col, cols)
                    return xfer(link, rows * ru * cols, ref, out, **to)

                q, b1 = quarter(s, ri), 2 * half(s, ri)
                ts = [same(cax + e2, q, 1, quarter(s, ci) * QC, QC, **{cax: second(s, ci)}), same(cax + e1, q, 1, half(s, ci) * HC, HC, **{cax: first(s, ci)}),
                      same(rax + e2, q, 1, 0, FF, **{rax: second(s, ri)}), same(rax + e1, b1, 2, 0, FF, **{rax: first(s, ri)})]
                fw = [same("chip", b, 2, 0, FF, core=other) for b in (b1, 2 - b1)]
                e = spread
                for n, t in enumerate(ts):
                    e = event(ts[n - 1 : n], [e], sends=[t] + fw[: n // 3])
                copy = part_of(local, i, 2 * c + s, window(own_ab, (i, c), s * S, S, 0, FF), window(gu_out, (c, l), core * HD + s * S, S, f0, FF))
                event(ts[-1:], [e], lambda copy=copy: copy().start(), sends=fw[1:])
                arrived += fw
                copies.append(copy)

        for s in range(2):
            key, base, kind = (i, s), s * HC, ("down", l)
            arms = ((1, "z+", 0, 4 - s), (-1, "z-", 4 - s, 3 + s))
            chunk = lambda k, base=base: base + around[k % NZ]

            def work(slots, row, into, i=i, key=key):
                to = ((i,), row, 0)
                total(into or (p_c, *to), [(p_c, *to), (own_c, *to)] + [(rc, (*key, t), 0, 0) for t in slots], CR, HD)

            ends, lasts = [], []
            for sg, zl, slot, n in arms:
                nxt, e, prev = others["z"][-(sg < 0)], begins[2, s], []
                for t in range(n):
                    row, into = chunk(sg * (n - t)), (rc, (*key, slot + t - 1), 0, 0) if t else None
                    ring = xfer(zl, CR * HD, block(rc, *key, slot + t - 1) if t else window(p_c, (i,), row, CR, 0, HD), block(rc, *key, slot + t), z=nxt)
                    e = event(prev, [e], part_of(work, [slot + t - 1] if t else [], row, into), adds(CR * HD, 3), [ring])
                    prev = [ring]
                ends.append(e)
                lasts += prev
            tx = to_all("x", NX, XR * HD, lambda d, to, key=key: window(rc, (*key, 3 - key[1]), to * XR, XR, 0, HD), lambda d, to, key=key: block(rx, *key, d - 1))
            e = event(lasts, ends, part_of(work, [3 - s, NZ - 2], chunk(0), (rc, (*key, 3 - s), 0, 0)), adds(CR * HD, 4), tx)

            def work_x(key=key):
                total((ry, (*key, y), 0, 0), [(rc, (*key, 3 - key[1]), x * XR, 0)] + [(rx, (*key, d), 0, 0) for d in range(NX - 1)], XR, HD)

            mine, kind = block(ry, *key, y), ("across", l)
            ty = to_all("y", NY, XR * HD, lambda d, to, m=mine: m, lambda d, to, m=mine: m)
            e = event(tx, [e], work_x, adds(XR * HD, 4), ty)
            row, mine = base + z * CR + x * XR, block(f_c, *key)
            home = window(own_c, (i,), row, XR, 0, HD)

            def work_y(key=key, row=row):
                total((f_c, key, 0, 0), [(ry, (*key, k), 0, 0) for k in range(NY)], XR, HD)
                squares(f_c, key, 1.0 / NY)
                total((own_c, key[:1], row, 0), [(f_c, key, 0, 0)], XR, HD)

            hx = to_all("x", NX, XR * HD, lambda d, to, m=mine: m, lambda d, to, h=home: h)
            e = event(ty, [e], work_y, 0.3, hx)
            pieces.append(e)
            e = event(hx, [e, spread])
            prev, ends = [[], []], [e, e]
            kind = "round", l
            for t in range(4):
                for k, (sg, zl, slot, n) in enumerate(arms):
                    if t < n:
                        ref = window(own_c, (i,), chunk(-sg * t), CR, 0, HD)
                        ring = xfer(zl, CR * HD, ref, ref, z=others["z"][-(sg < 0)])
                        ends[k] = event(prev[k], [ends[k]], sends=[ring])
                        prev[k] = [ring]
            ref, out = window(own_c, (i,), base, HC, 0, HD), window(dn_out, (l,), f0 + base, HC, core * HD, HD)
            arrived.append(xfer("chip", HC * HD, ref, out, core=other))
            copies.append(part_of(local, i, 4 + s, ref, out))
            event(prev[0] + prev[1], ends, lambda copy=copies[-1]: copy().start(), sends=arrived[-1:])

    kind = None
    e, ts, prev = None, [], None
    for axis, k, n, ref in (("z", z, NZ, norms[0]), ("y", y, NY, norms[1]), ("x", x, NX, norms[2]), ("core", core, CORES, norms[3])):
        def work(ref=ref, k=k, prev=prev):
            if prev is None:
                ref[k] = acc[...]
            else:
                ref[k] = functools.reduce(lambda a, b: a + b, [prev[0][j] for j in range(prev[1])])

        new = [xfer("n", SUBLANES * LANES, block(ref, k), block(ref, k), **{axis: to}) for to in others[axis]]
        e = event(ts, pieces if e is None else [e], work, 0.15, new)
        ts, prev = new, (ref, n)

    def finish():
        sq_out[...] = norms[3][0] + norms[3][1]

    event(ts, [e], finish, 0.1)
    every = list(events)
    event(arrived, every, lambda: [copy().wait() for copy in copies])
    return xfers, events


def sum_kernel(ru, cu, *refs):
    (g1, u1, d1, a0_t, dh, gate, up, wd, gu_out, dn_out, sq_out, own_ab, own_c, p_ab, p_c, r1, r2, r3, r4, rz, rc, rx, ry, f_ab, f_c,
     acc, nz, ny, nx, nc, gbuf, ubuf, wbuf, p_s, dg_s, du_s, st_ab, st_c, send_sem, recv_sem, load_sem, keep_sem, tile_sem, out_sem, in_sem) = refs
    me = lax.axis_index("dp")
    core, z, y, x = rem(me, CORES), rem(div(me, CORES), NZ), rem(div(me, CORES * NZ), NY), div(me, CORES * NZ * NY)
    other = 1 - core
    D = SUBLANES * ru
    HD = D // 2
    n = dh.shape[0]
    per = TILES // PARTS
    tile = NZ * cu // per
    partner = me + 1 - 2 * core
    slice_of = lambda j: pl.ds(pl.multiple_of(j * tile, LANES), tile)

    mine, yours = (pl.ds(pl.multiple_of(c * HD, LANES), HD) for c in (core, other))
    loads = [pltpu.make_async_copy(src, dst, load_sem.at[k]) for k, (src, dst) in enumerate(((g1.at[mine, :], own_ab.at[0, 0]), (u1.at[mine, :], own_ab.at[0, 1]),
                                                                                             (d1.at[:, mine], own_c.at[0])))]
    for t in loads:
        t.start()

    barrier = pltpu.get_barrier_semaphore()
    dev = lambda x, y, z, core: ((x * NY + y) * NZ + z) * CORES + core
    peers = [dev(x, y, z, other)] + [dev(rem(x + d, NX), y, z, core) for d in range(1, NX)]
    peers += [dev(x, rem(y + d, NY), z, core) for d in range(1, NY)] + [dev(x, y, rem(z + d, NZ), core) for d in range(1, NZ)]
    for p in peers:
        pl.semaphore_signal(barrier, inc=1, device_id=p, device_id_type=LOGICAL)
    pl.semaphore_wait(barrier, len(peers))

    def tile_sends(j, srcs=None):
        i, cols = PARTS + div(j, per), slice_of(rem(j, per))
        dsts = [p_ab.at[i, c, :, cols] for c in range(2)] + [p_c.at[i, cols, :]]
        return [pltpu.make_async_remote_copy(src_ref=src, dst_ref=dst, send_sem=out_sem.at[k], recv_sem=in_sem.at[j, k], device_id=partner,
                                             device_id_type=LOGICAL) for k, (src, dst) in enumerate(zip(srcs or dsts, dsts, strict=True))]

    def total(dst, srcs, rows, cols):
        wide = next(cols // k for k in range(1, cols) if cols % (k * LANES) == 0 and cols // k <= 4 * LANES)
        tall = next(rows // k for k in range(1, rows) if rows % (k * SUBLANES) == 0 and rows // k * wide <= SUBLANES * LANES * 16)
        across = cols // wide

        many = rows // tall * across

        def block(i, _):
            if many > 1:
                r, c = (div(i, across) * tall, rem(i, across) * wide) if across > 1 else (i * tall, None)

            def at(a):
                ref, lead, row, col = a
                row, col = (row, col) if many == 1 else (row + r, col if c is None else col + c)
                return ref.at[(*lead, place(row, tall, SUBLANES), place(col, wide, LANES))]

            s = at(srcs[0])[...].astype(F32)
            for a in srcs[1:]:
                s = s + at(a)[...].astype(F32)
            at(dst)[...] = s.astype(BF16)
            return _

        if many > 1:
            lax.fori_loop(0, many, block, 0)
        else:
            block(0, 0)

    def squares(ref, lead, weight):
        rows, cols = ref.shape[len(lead):]
        for r in range(0, rows, SUBLANES):
            v = ref[(*lead, pl.ds(r, SUBLANES), slice(None))].astype(F32)
            v = v * v
            s = acc[...]
            for a in range(0, SUBLANES, BLOCK[0]):
                for b in range(0, cols, LANES):
                    s = s + weight * v[a : a + BLOCK[0], b : b + LANES]
            acc[...] = s

    def need(key):
        i, c, s = key
        if i < PARTS:
            if s == 0:
                loads[c].wait()
            return

        def wait(j, _):
            for t in tile_sends(j):
                t.wait_recv()
            return _

        lax.fori_loop((i - PARTS) * per, (i - PARTS + 1) * per, wait, 0)

    def local(l, k, src, dst):
        return pltpu.make_async_copy(src(), dst(), keep_sem.at[l, k])

    acc[...] = jnp.zeros_like(acc)
    xfers, events = plan((x, y, z, core), ((g1, u1, d1), own_ab, own_c, p_ab, p_c, r1, r2, r3, r4, rz, rc, rx, ry, f_ab, f_c, acc, (nz, ny, nx, nc),
                                           gu_out, dn_out, sq_out, total, squares, need, local), ru, cu)
    counts = sorted(t.count for t in xfers)
    ids = {id(t): k for k, t in enumerate(sorted(xfers, key=lambda t: t.count))}
    groups, _ = order_of(events, SLOTS)

    def copy_of(src, dst, k, dev):
        return pltpu.make_async_remote_copy(src_ref=src, dst_ref=dst, send_sem=send_sem.at[k], recv_sem=recv_sem.at[k], device_id=dev, device_id_type=LOGICAL)

    def wait_of(count, k):
        cols = next(c for c in range(NZ * cu, 0, -LANES) if count % (c * SUBLANES) == 0)
        some = p_ab.at[0, 0, pl.ds(0, count // cols), pl.ds(0, cols)]
        return copy_of(some, some, k, me)

    def emit(group):
        for e in group:
            for t in e.waits:
                wait_of(t.count, ids[id(t)]).wait_recv()
            e.work()
            for t in e.sends:
                copy_of(t.src(), t.dst(), ids[id(t)], t.dev).start()

    def choose(j, options):
        middle = len(options) // 2
        if middle == 0:
            emit(options[0])
        elif any(options):
            pl.when(j < middle)(lambda: choose(j, options[:middle]))
            pl.when(j >= middle)(lambda: choose(j - middle, options[middle:]))

    def steps(srcs, bufs, *parts):
        mine = groups[: TILES * len(parts)]
        del groups[: TILES * len(parts)]

        def copies(j, slot):
            return [pltpu.make_async_copy(src(j), buf.at[slot], tile_sem.at[slot, k]) for k, (src, buf) in enumerate(zip(srcs, bufs, strict=True))]

        for t in copies(0, 0):
            t.start()

        def step(j, carry):
            slot = rem(j, 2)
            for t in copies(j, slot):
                t.wait()

            @pl.when(j + 1 < TILES)
            def _():
                for t in copies(j + 1, 1 - slot):
                    t.start()

            for k, part in enumerate(parts):
                part(j, slot)
                choose(j, mine[k :: len(parts)])
            return carry

        lax.fori_loop(0, TILES, step, 0)

    emit(groups.pop(0))
    tail = groups.pop()
    groups.append([])

    rows_in, rows_out = (pl.ds(pl.multiple_of(c * HD, SUBLANES), HD) for c in (core, other))
    staged = lambda: [st_ab.at[0, rows_out, :], st_ab.at[1, rows_out, :], st_c.at[:, yours]]
    blocks = [pl.ds(k * (n // 2), n // 2) for k in range(2)]

    def through(which, j, slot):
        if which == 0:
            @pl.when(j > 0)
            def _():
                for t in tile_sends(j - 1, staged()):
                    t.wait_send()

        for rows in blocks[which::2]:
            dp = dot(dh[rows, :], wbuf[slot], NT).astype(BF16).astype(F32)
            p_s[rows, :], dg_s[rows, :], du_s[rows, :] = backward_tile(gbuf[slot, rows, :], ubuf[slot, rows, :], dp)

    def term(c, j, slot):
        i, cols = PARTS + div(j, per), slice_of(rem(j, per))
        if c < 2:
            st_ab[c] = dot(a0_t[...], (dg_s, du_s)[c][...]).astype(BF16)
            own_ab[i, c, :, cols] = st_ab[c, rows_in, :]
        else:
            st_c[...] = dot(p_s[...], dh[...], TN).astype(BF16)
            own_c[i, cols, :] = st_c[:, mine]
            for t in tile_sends(j, staged()):
                t.start()

    steps([lambda j: gate.at[j], lambda j: up.at[j], lambda j: wd.at[0, slice_of(j), :]], [gbuf, ubuf, wbuf],
          *[functools.partial(f, k) for f, k in ((through, 0), (through, 1), (term, 0), (term, 1), (term, 2))])
    for t in tile_sends(TILES - 1, staged()):
        t.wait_send()
    emit(tail)
    for count in sorted(set(counts)):
        def wait(k, carry, count=count):
            wait_of(count, k).wait_send()
            return carry

        lax.fori_loop(counts.index(count), counts.index(count) + counts.count(count), wait, 0)


def gradient_sums(g1, u1, d1, a0_t, dh, gate, up, wd):
    (n, d), ff = dh.shape, g1.shape[1]
    ru, cu = d // SUBLANES, ff // NZ // PARTS
    HD, CR, fs, N, tile = d // 2, cu // 2, ff // PARTS, 2 * PARTS, ff // TILES
    V = lambda *s: pltpu.VMEM(s, BF16)
    W = lambda *s: pltpu.VMEM(s, F32)
    DMA = lambda *s: pltpu.SemaphoreType.DMA(s)
    return pl.pallas_call(
        functools.partial(sum_kernel, ru, cu),
        name="gradient_sums",
        out_shape=(jax.ShapeDtypeStruct((2, 2, d, ff), BF16), jax.ShapeDtypeStruct((2, ff, d), BF16), jax.ShapeDtypeStruct(BLOCK, F32)),
        in_specs=[ANY] * 3 + [VMEM] * 2 + [ANY] * 3,
        out_specs=(ANY, ANY, VMEM),
        scratch_shapes=[
            V(N, 2, HD, fs), V(N, fs, HD), V(N, 2, HD, fs), V(N, fs, HD),
            V(N, 2, 2, 2 * ru, fs), V(N, 2, 2, ru, fs), V(N, 2, 2, ru, fs // 2), V(N, 2, 2, ru, fs // 4),
            V(N, NZ - 1, ru, cu), V(N, 2, NZ - 1, CR, HD), V(N, 2, NX - 1, CR // 4, HD), V(N, 2, NY, CR // 4, HD), V(N, ru, cu), V(N, 2, CR // 4, HD),
            W(*BLOCK), W(NZ, *BLOCK), W(NY, *BLOCK), W(NX, *BLOCK), W(CORES, *BLOCK),
            W(2, n, tile), W(2, n, tile), V(2, tile, d), V(n, tile), V(n, tile), V(n, tile), V(2, d, tile), V(tile, d),
            DMA(NUMBER_OF_XFERS), DMA(NUMBER_OF_XFERS), DMA(3), DMA(N, 6), DMA(2, 3), DMA(3), DMA(TILES, 3),
        ],
        compiler_params=pltpu.CompilerParams(collective_id=0, has_side_effects=True, vmem_limit_bytes=63 << 20),
    )(g1, u1, d1, a0_t, dh, gate, up, wd)


def adamw(w, m, v, g):
    m = 0.9 * m + 0.1 * g
    v = 0.95 * v + 0.05 * g * g
    step = m * lax.rsqrt(v + 1e-8) + 0.1 * w
    return (w - 0.02 * step).astype(BF16), m, v


def solution(mesh):
    def step(x, dy, *arrays):
        weights, m, v = (arrays[i : i + 3] for i in (0, 3, 6))
        gate, up, a0_t, dh, *by_1 = layers(x[0], dy[0], *weights)
        gu, down, squares = gradient_sums(*by_1, a0_t, dh, gate, up, weights[2])
        gradients = [gu[0], gu[1], down]
        count = sum(g.size for g in gradients)
        factor = jnp.minimum(1.0, 0.5 * lax.rsqrt(jnp.sum(squares) / count + 1e-30))
        new = [adamw(w.astype(F32), m, v, g.astype(F32) * factor) for w, m, v, g in zip(weights, m, v, gradients, strict=True)]
        return tuple(one[which] for which in range(3) for one in new)

    whole = P(None, None, None)
    return jax.shard_map(
        step,
        mesh=mesh,
        in_specs=(P(("rep", "dp"), None, None),) * 2 + (whole,) * 9,
        out_specs=(P("rep", None, None),) * 9,
        check_vma=False,
    )
```

```python
import functools

import jax
import jax.numpy as jnp
from jax import lax
from jax.experimental import pallas as pl
from jax.experimental.pallas import tpu as pltpu
from jax.sharding import PartitionSpec as P

LOGICAL = pl.DeviceIdType.LOGICAL
NX, NY, NZ, CORES = 4, 4, 8, 2
F32, BF16 = jnp.float32, jnp.bfloat16
NN = (((1,), (0,)), ((), ()))
NT = (((1,), (1,)), ((), ()))
TN = (((0,), (0,)), ((), ()))
ANY = pl.BlockSpec(memory_space=pl.ANY)
VMEM = pl.BlockSpec(memory_space=pltpu.VMEM)
SUBLANES, LANES = 16, 128
TILES, PARTS = 12, 1
BLOCK = (8, LANES)
NUMBER_OF_XFERS = 680


def dot(a, b, dims=NN):
    return lax.dot_general(a, b, dims, preferred_element_type=F32)


def scale_of(wide):
    return lax.rsqrt(jnp.mean(wide * wide, -1, keepdims=True) + 1e-6)


def normed(h):
    wide = h.astype(F32)
    return (wide * scale_of(wide)).astype(BF16)


def by_rows(n, step, body):
    def at(k, _):
        body(pl.ds(pl.multiple_of(k * step, step), step))
        return _

    lax.fori_loop(0, n // step, at, 0)


def turned(a, a_t):
    def slab(k, _):
        at = pl.ds(pl.multiple_of(k * LANES, LANES), LANES)
        a_t[at, :] = a[:, at].T
        return _

    lax.fori_loop(0, a.shape[1] // LANES, slab, 0)


def blocks_of(shape, index):
    return pl.BlockSpec(shape, lambda j: index(j))


def backward_tile(g, u, dp):
    sig = jax.nn.sigmoid(g)
    act = g * sig
    return (act * u).astype(BF16), (dp * u * (sig + act * (1.0 - sig))).astype(BF16), (dp * act).astype(BF16)


def layers_kernel(tiles, x_ref, dy_ref, wg_ref, wu_ref, wd_ref, g_ref, u_ref, a0_t, dh_ref, dwg_ref, dwu_ref, dwd_ref, a_s, a_t, h_s, by_g, by_u, p_s, dg_s, du_s):
    j = pl.program_id(0)
    n, d = x_ref.shape
    def clear(rows):
        by_g[rows, :] = jnp.zeros_like(by_g[rows, :])

    @pl.when(j == 0)
    def _():
        def body(rows):
            a_s[rows, :] = normed(x_ref[rows, :])
            clear(rows)

        by_rows(n, 64, body)
        turned(a_s, a0_t)

    @pl.when(j < tiles)
    def _():
        a = a_s[...]
        g = dot(a, wg_ref[0])
        u = dot(a, wu_ref[0])
        for to, by in ((g_ref, g), (u_ref, u)):
            for t in range(to.shape[0]):
                to[t] = by[:, t * to.shape[2] : (t + 1) * to.shape[2]]
        by_g[...] += dot((g * jax.nn.sigmoid(g) * u).astype(BF16), wd_ref[0])

    @pl.when(j == tiles - 1)
    def _():
        def body(rows):
            h = x_ref[rows, :] + by_g[rows, :].astype(BF16)
            h_s[rows, :] = h
            a_s[rows, :] = normed(h)
            clear(rows)
            by_u[rows, :] = jnp.zeros_like(by_u[rows, :])

        by_rows(n, 64, body)
        turned(a_s, a_t)

    @pl.when(j >= tiles)
    def _():
        a = a_s[...]
        dp = dot(dy_ref[...], wd_ref[0], NT).astype(BF16).astype(F32)
        p_s[...], dg_s[...], du_s[...] = backward_tile(dot(a, wg_ref[0]), dot(a, wu_ref[0]), dp)
        by_g[...] += dot(dg_s[...], wg_ref[0], NT)
        by_u[...] += dot(du_s[...], wu_ref[0], NT)
        dwg_ref[...] = dot(a_t[...], dg_s[...]).astype(BF16)
        dwu_ref[...] = dot(a_t[...], du_s[...]).astype(BF16)
        dwd_ref[...] = dot(p_s[...], dy_ref[...], TN).astype(BF16)

    @pl.when(j == pl.num_programs(0) - 1)
    def _():
        def body(rows):
            by_a = (by_g[rows, :].astype(BF16) + by_u[rows, :].astype(BF16)).astype(F32)
            wide = h_s[rows, :].astype(F32)
            s = scale_of(wide)
            by_h = by_a * s - wide * (s * s * s * jnp.mean(by_a * wide, -1, keepdims=True))
            dh_ref[rows, :] = dy_ref[rows, :] + by_h.astype(BF16)

        by_rows(n, 32, body)


def layers(x, dy, wg, wu, wd, tile=512):
    (n, d), ff = x.shape, wg.shape[-1]
    tiles, per = ff // tile, tile * TILES // ff
    early, late = lambda j: jnp.minimum(j, tiles - 1), lambda j: jnp.maximum(j - tiles, 0)
    whole, turned_ = blocks_of((n, d), lambda j: (0, 0)), blocks_of((d, n), lambda j: (0, 0))
    wide = blocks_of((per, n, ff // TILES), lambda j: (early(j), 0, 0))
    weight = blocks_of((1, d, tile), lambda j: (j // tiles, 0, j % tiles))
    across = blocks_of((d, tile), lambda j: (0, late(j)))
    V = lambda *s: pltpu.VMEM(s, BF16)
    return pl.pallas_call(
        functools.partial(layers_kernel, tiles),
        name="layers",
        grid=(2 * tiles,),
        in_specs=[whole, whole, weight, weight, blocks_of((1, tile, d), lambda j: (j // tiles, j % tiles, 0))],
        out_specs=[wide, wide, turned_, whole, across, across, blocks_of((tile, d), lambda j: (late(j), 0))],
        out_shape=[jax.ShapeDtypeStruct((TILES, n, ff // TILES), F32)] * 2 + [jax.ShapeDtypeStruct(s, BF16) for s in ((d, n), (n, d), (d, ff), (d, ff), (ff, d))],
        scratch_shapes=[V(n, d), V(d, n), V(n, d), pltpu.VMEM((n, d), F32), pltpu.VMEM((n, d), F32), V(n, tile), V(n, tile), V(n, tile)],
        compiler_params=pltpu.CompilerParams(vmem_limit_bytes=62 << 20),
    )(x, dy, wg, wu, wd)


def div(a, b):
    return lax.div(a, jnp.int32(b))


def rem(a, b):
    return lax.rem(a, jnp.int32(b))


def once(f):
    known = {}

    def g(s, i):
        key = s, id(i)
        if key not in known:
            known[key] = i, f(s, i)
        return known[key][1]

    return g


@once
def first(s, i):
    return NX - 1 - i if s else i + 1 - 2 * rem(i, 2)


def second(s, i):
    return first(1 - s, i)


@once
def half(s, i):
    return div(i, 2) if s else rem(div(i + 1, 2), 2)


@once
def part(s, i):
    return rem(i, 2) if s else div(i, 2)


@once
def quarter(s, i):
    return 2 * half(s, i) + part(s, i)


def place(start, size, unit):
    return pl.ds(start if isinstance(start, int) else pl.multiple_of(start, unit), size)


class Xfer:
    def __init__(self, link, count, hops, src, dst, dev):
        self.link, self.count, self.size, self.src, self.dst, self.dev = link, count, 2 * count * hops, src, dst, dev
        self.arrives = None


class Event:
    def __init__(self, waits, pre, work, cost, sends, late):
        self.waits, self.pre, self.work, self.cost, self.sends, self.late = waits, pre, work, cost, sends, late
        self.done = None


RATE, CHIP_RATE, DELAY, GAP, SLACK = 46.0e3, 450.0e3, 2.3, 0.1, 0.5
LATE = {("share", 0): -2, ("share", 1): 2, ("across", 0): 1, ("across", 1): 2, ("halve", 0): 1, ("round", 0): -2}
STEP = (0.6, 0.6, 0.65, 0.65, 0.65)
SLOTS = STEP * TILES


def order_of(events, slots):
    links, left, groups, clock, done = {}, list(events), [[]], 0.0, 0
    while left:
        best = None
        for e in left:
            if any(done < p if isinstance(p, int) else p.done is None for p in e.pre) or any(t.arrives is None for t in e.waits):
                continue
            ready = max([p.done for p in e.pre if not isinstance(p, int)] + [t.arrives + (SLACK if done < len(slots) else 0.0) for t in e.waits] + [0.0])
            if best is None or max(ready, clock) + e.late < best[0] + best[1].late:
                best = (max(ready, clock), e)
        if done < len(slots) and (best is None or best[0] + best[1].late > clock):
            clock += slots[done]
            done += 1
            groups.append([])
            continue
        clock, e = best
        clock += e.cost
        e.done = clock
        for t in e.sends:
            begin = max(clock, links.get(t.link, 0.0))
            links[t.link] = begin + GAP + t.size / (CHIP_RATE if t.link == "chip" else RATE)
            t.arrives = links[t.link] + DELAY
        left.remove(e)
        groups[-1].append(e)
    return groups, clock


def plan(here, refs, ru, cu):
    x, y, z, core = here
    (grads, own_ab, own_c, p_ab, p_c, r1, r2, r3, r4, rz, rc, rx, ry, f_ab, f_c, acc, norms, gu_out, dn_out, sq_out, total, squares, need, local) = refs
    other = 1 - core
    xfers, events = [], []
    part_of = functools.partial

    devices, me = {}, ((x * NY + y) * NZ + z) * CORES + core
    steps = dict(x=(x, NY * NZ * CORES), y=(y, NZ * CORES), z=(z, CORES), core=(core, 1))

    def at(**to):
        ((axis, there),) = to.items()
        if (axis, id(there)) not in devices:
            i, stride = steps[axis]
            devices[axis, id(there)] = there, me + (there - i) * stride
        return devices[axis, id(there)][1]

    def window(ref, lead, row, rows, col, cols):
        return lambda: ref.at[(*lead, place(row, rows, SUBLANES), place(col, cols, LANES))]

    def block(ref, *lead):
        return lambda: ref.at[lead]

    def xfer(link, count, src, dst, hops=1, **to):
        t = Xfer(link, count, hops, src, dst, at(**to))
        xfers.append(t)
        return t

    others = {axis: [rem(k + d, n) for d in range(1, n)] for axis, k, n in (("x", x, NX), ("y", y, NY), ("z", z, NZ), ("core", core, CORES))}

    def to_all(axis, n, size, src, dst):
        ts = []
        for d in range(1, n):
            to, back = others[axis][d - 1], d * 2 > n
            ts.append(xfer(axis + "+-"[back], size, src(d, to), dst(d, to), n - d if back else d, **{axis: to}))
        return ts

    def event(waits, pre, work=lambda: None, cost=0.05, sends=()):
        e = Event(waits, pre, work, cost, sends, LATE.get(kind, 0))
        events.append(e)
        return e

    kind = None

    def adds(size, n):
        return size * n / 2.0e6 + 0.15

    D, FF = SUBLANES * ru, NZ * cu
    HD, S = D // 2, D // 4
    HC, QC = FF // 2, FF // 4
    CR = cu // 2
    XR = CR // 4
    around = [z * CR] + [to * CR for to in others["z"]]
    arrived, pieces = [], []

    for i in range(2 * PARTS):
        l, f0 = 1 - i // PARTS, i % PARTS * FF
        kind = "halve", l
        begins = {}
        if l:
            for s in range(2):
                for c in range(2):
                    begins[c, s] = xfer("chip", S * FF, window(grads[c], (), other * HD + s * S, S, f0, FF), window(p_ab, (i, c), s * S, S, 0, FF), core=other)
                begins[2, s] = xfer("chip", HC * HD, window(grads[2], (), f0 + s * HC, HC, other * HD, HD), window(p_c, (i,), s * HC, HC, 0, HD), core=other)
            e = event([], [], sends=list(begins.values()))
            begins = {k: event([t], [e], part_of(need, (i, *k))) for k, t in begins.items()}
        else:
            e = event([], [len(SLOTS) * (i % PARTS + 1) // PARTS], part_of(need, (i, 0, 0)), 0.3)
            begins = {(c, s): e for c in range(3) for s in range(2)}

        ends = []
        for c in range(2):
            ri, ci, rax, cax = (y, x, "y", "x") if c else (x, y, "x", "y")
            for s in range(2):
                k1, k2, e1, e2 = (i, c), (i, c, s), "+-"[s], "-+"[s]
                b1, b2, c1, c2 = half(s, ri), part(s, ri), half(s, ci), part(s, ci)
                keep = s * S + b1 * 2 * ru
                away, out, q = s * S + (1 - b1) * 2 * ru, keep + (1 - b2) * ru, keep + b2 * ru
                col1, col2, mine = (1 - c1) * HC, c1 * HC + (1 - c2) * QC, c1 * HC + c2 * QC
                t1 = xfer(rax + e1, 2 * ru * FF, window(p_ab, k1, away, 2 * ru, 0, FF), block(r1, *k2), **{rax: first(s, ri)})
                t2 = xfer(rax + e2, ru * FF, window(p_ab, k1, out, ru, 0, FF), block(r2, *k2), **{rax: second(s, ri)})
                t3 = xfer(cax + e1, ru * HC, window(p_ab, k1, q, ru, col1, HC), block(r3, *k2), **{cax: first(s, ci)})
                t4 = xfer(cax + e2, ru * QC, window(p_ab, k1, q, ru, col2, QC), block(r4, *k2), **{cax: second(s, ci)})

                def work(row, col, rows, cols, n, k1=k1, k2=k2, b2=b2, c1=c1):
                    to = (k1, row, col)
                    more = [(r1, k2, (b2 if n > 1 else 1 - b2) * ru, col), (r2, k2, 0, col), (r3, k2, 0, col - c1 * HC), (r4, k2, 0, 0)]
                    total((p_ab, *to), [(p_ab, *to), (own_ab, *to)] + more[:n], rows, cols)

                e, prev = begins[c, s], []
                for n, (t, row, col, rows, cols) in enumerate(((t1, away, 0, 2 * ru, FF), (t2, out, 0, ru, FF), (t3, q, col1, ru, HC), (t4, q, col2, ru, QC), (None, q, mine, ru, QC))):
                    e = event(prev, [e], part_of(work, row, col, rows, cols, n), adds(rows * cols, n + 2), [t] if t else [])
                    prev = [t]
                ends.append(e)

        def piece(to):
            c, k = div(to, 4), rem(to, 4)
            s, h = div(k, 2), rem(k, 2)
            qx = quarter(0, x) + s * (quarter(1, x) - quarter(0, x))
            qy = quarter(0, y) + s * (quarter(1, y) - quarter(0, y))
            return c, s * S + (qx + c * (qy - qx)) * ru, (qy + c * (qx - qy)) * QC + h * cu

        def from_piece(d, to, i=i):
            c, a, b = piece(to)
            return window(p_ab, (i, c), a, ru, b, cu)

        kind = "share", l
        tz = to_all("z", NZ, ru * cu, from_piece, lambda d, to, i=i: block(rz, i, d - 1))
        e = event([], ends, sends=tz)
        mc, ma, mb = piece(z)
        home, mine = window(gu_out, (mc, l), core * HD + ma, ru, f0 + mb, cu), block(f_ab, i)

        def work(i=i, mc=mc, ma=ma, mb=mb, mine=mine, home=home):
            total((f_ab, (i,), 0, 0), [(p_ab, (i, mc), ma, mb)] + [(rz, (i, d), 0, 0) for d in range(NZ - 1)], ru, cu)
            squares(f_ab, (i,), 1.0)
            local(i, 0, mine, home).start()

        ta = to_all("z", NZ, ru * cu, lambda d, to, m=mine: m, lambda d, to, h=home: h)
        e = event(tz, [e], work, 0.4, ta)
        pieces.append(e)
        spread = event(ta, [e], lambda i=i, mine=mine, home=home: local(i, 0, mine, home).wait(), 0.1)
        for c in range(2):
            ri, ci, rax, cax = (y, x, "y", "x") if c else (x, y, "x", "y")
            for s in range(2):
                e1, e2 = "+-"[s], "-+"[s]

                kind = "spread", l

                def same(link, row, rows, col, cols, l=l, c=c, f0=f0, s=s, **to):
                    ref = window(gu_out, (c, l), core * HD + s * S + row * ru, rows * ru, f0 + col, cols)
                    return xfer(link, rows * ru * cols, ref, ref, **to)

                q, b1 = quarter(s, ri), 2 * half(s, ri)
                ts = [same(cax + e2, q, 1, quarter(s, ci) * QC, QC, **{cax: second(s, ci)}), same(cax + e1, q, 1, half(s, ci) * HC, HC, **{cax: first(s, ci)}),
                      same(rax + e2, q, 1, 0, FF, **{rax: second(s, ri)}), same(rax + e1, b1, 2, 0, FF, **{rax: first(s, ri)})]
                fw = [same("chip", b, 2, 0, FF, core=other) for b in (b1, 2 - b1)]
                e = spread
                for n, t in enumerate(ts):
                    e = event(ts[n - 1 : n], [e], sends=[t] + fw[: n // 3])
                event(ts[-1:], [e], sends=fw[1:])
                arrived += fw

        for s in range(2):
            key, base, kind = (i, s), s * HC, ("down", l)
            arms = ((1, "z+", 0, 4 - s), (-1, "z-", 4 - s, 3 + s))
            chunk = lambda k, base=base: base + around[k % NZ]

            def work(slots, row, into, i=i, key=key):
                to = ((i,), row, 0)
                total(into or (p_c, *to), [(p_c, *to), (own_c, *to)] + [(rc, (*key, t), 0, 0) for t in slots], CR, HD)

            ends, lasts = [], []
            for sg, zl, slot, n in arms:
                nxt, e, prev = others["z"][-(sg < 0)], begins[2, s], []
                for t in range(n):
                    row, into = chunk(sg * (n - t)), (rc, (*key, slot + t - 1), 0, 0) if t else None
                    ring = xfer(zl, CR * HD, block(rc, *key, slot + t - 1) if t else window(p_c, (i,), row, CR, 0, HD), block(rc, *key, slot + t), z=nxt)
                    e = event(prev, [e], part_of(work, [slot + t - 1] if t else [], row, into), adds(CR * HD, 3), [ring])
                    prev = [ring]
                ends.append(e)
                lasts += prev
            tx = to_all("x", NX, XR * HD, lambda d, to, key=key: window(rc, (*key, 3 - key[1]), to * XR, XR, 0, HD), lambda d, to, key=key: block(rx, *key, d - 1))
            e = event(lasts, ends, part_of(work, [3 - s, NZ - 2], chunk(0), (rc, (*key, 3 - s), 0, 0)), adds(CR * HD, 4), tx)

            def work_x(key=key):
                total((ry, (*key, y), 0, 0), [(rc, (*key, 3 - key[1]), x * XR, 0)] + [(rx, (*key, d), 0, 0) for d in range(NX - 1)], XR, HD)

            mine, kind = block(ry, *key, y), ("across", l)
            ty = to_all("y", NY, XR * HD, lambda d, to, m=mine: m, lambda d, to, m=mine: m)
            e = event(tx, [e], work_x, adds(XR * HD, 4), ty)
            home, mine = window(dn_out, (l,), f0 + base + z * CR + x * XR, XR, core * HD, HD), block(f_c, *key)

            def work_y(key=key, mine=mine, home=home):
                total((f_c, key, 0, 0), [(ry, (*key, k), 0, 0) for k in range(NY)], XR, HD)
                squares(f_c, key, 1.0 / NY)
                local(key[0], 1 + key[1], mine, home).start()

            hx = to_all("x", NX, XR * HD, lambda d, to, m=mine: m, lambda d, to, h=home: h)
            e = event(ty, [e], work_y, 0.3, hx)
            pieces.append(e)
            e = event(hx, [e, spread], lambda key=key, mine=mine, home=home: local(key[0], 1 + key[1], mine, home).wait(), 0.1)
            prev, ends = [[], []], [e, e]
            kind = "round", l
            for t in range(4):
                for k, (sg, zl, slot, n) in enumerate(arms):
                    if t < n:
                        ref = window(dn_out, (l,), f0 + chunk(-sg * t), CR, core * HD, HD)
                        ring = xfer(zl, CR * HD, ref, ref, z=others["z"][-(sg < 0)])
                        ends[k] = event(prev[k], [ends[k]], sends=[ring])
                        prev[k] = [ring]
            ref = window(dn_out, (l,), f0 + base, HC, core * HD, HD)
            arrived.append(xfer("chip", HC * HD, ref, ref, core=other))
            event(prev[0] + prev[1], ends, sends=arrived[-1:])

    kind = None
    e, ts, prev = None, [], None
    for axis, k, n, ref in (("z", z, NZ, norms[0]), ("y", y, NY, norms[1]), ("x", x, NX, norms[2]), ("core", core, CORES, norms[3])):
        def work(ref=ref, k=k, prev=prev):
            if prev is None:
                ref[k] = acc[...]
            else:
                ref[k] = functools.reduce(lambda a, b: a + b, [prev[0][j] for j in range(prev[1])])

        new = [xfer("n", SUBLANES * LANES, block(ref, k), block(ref, k), **{axis: to}) for to in others[axis]]
        e = event(ts, pieces if e is None else [e], work, 0.15, new)
        ts, prev = new, (ref, n)

    def finish():
        sq_out[...] = jnp.broadcast_to(jnp.sum(norms[3][0] + norms[3][1], keepdims=True), BLOCK)

    event(ts, [e], finish, 0.1)
    event(arrived, [])
    return xfers, events


def sum_kernel(ru, cu, *refs):
    (g1, u1, d1, a0_t, dh, gate, up, wd, gu_out, dn_out, sq_out, own_ab, own_c, p_ab, p_c, r1, r2, r3, r4, rz, rc, rx, ry, f_ab, f_c,
     acc, nz, ny, nx, nc, gbuf, ubuf, wbuf, p_s, dg_s, du_s, st_ab, st_c, send_sem, recv_sem, load_sem, keep_sem, tile_sem, out_sem, in_sem) = refs
    me = lax.axis_index("dp")
    core, z, y, x = rem(me, CORES), rem(div(me, CORES), NZ), rem(div(me, CORES * NZ), NY), div(me, CORES * NZ * NY)
    other = 1 - core
    D = SUBLANES * ru
    HD = D // 2
    n = dh.shape[0]
    per = TILES // PARTS
    tile = NZ * cu // per
    partner = me + 1 - 2 * core
    slice_of = lambda j: pl.ds(pl.multiple_of(j * tile, LANES), tile)

    mine, yours = (pl.ds(pl.multiple_of(c * HD, LANES), HD) for c in (core, other))
    loads = [pltpu.make_async_copy(src, dst, load_sem.at[k]) for k, (src, dst) in enumerate(((g1.at[mine, :], own_ab.at[0, 0]), (u1.at[mine, :], own_ab.at[0, 1]),
                                                                                             (d1.at[:, mine], own_c.at[0])))]
    for t in loads:
        t.start()

    barrier = pltpu.get_barrier_semaphore()
    dev = lambda x, y, z, core: ((x * NY + y) * NZ + z) * CORES + core
    peers = [dev(x, y, z, other)] + [dev(rem(x + d, NX), y, z, core) for d in range(1, NX)]
    peers += [dev(x, rem(y + d, NY), z, core) for d in range(1, NY)] + [dev(x, y, rem(z + d, NZ), core) for d in range(1, NZ)]
    for p in peers:
        pl.semaphore_signal(barrier, inc=1, device_id=p, device_id_type=LOGICAL)
    pl.semaphore_wait(barrier, len(peers))

    def tile_sends(j, srcs=None, slot=0):
        i, cols = PARTS + div(j, per), slice_of(rem(j, per))
        dsts = [p_ab.at[i, c, :, cols] for c in range(2)] + [p_c.at[i, cols, :]]
        return [pltpu.make_async_remote_copy(src_ref=src, dst_ref=dst, send_sem=out_sem.at[slot, k], recv_sem=in_sem.at[j, k], device_id=partner,
                                             device_id_type=LOGICAL) for k, (src, dst) in enumerate(zip(srcs or dsts, dsts, strict=True))]

    def total(dst, srcs, rows, cols):
        wide = next(cols // k for k in range(1, cols) if cols % (k * LANES) == 0 and cols // k <= 4 * LANES)
        tall = next(rows // k for k in range(1, rows) if rows % (k * SUBLANES) == 0 and rows // k * wide <= SUBLANES * LANES * 16)
        across = cols // wide

        many = rows // tall * across

        def block(i, _):
            if many > 1:
                r, c = (div(i, across) * tall, rem(i, across) * wide) if across > 1 else (i * tall, None)

            def at(a):
                ref, lead, row, col = a
                row, col = (row, col) if many == 1 else (row + r, col if c is None else col + c)
                return ref.at[(*lead, place(row, tall, SUBLANES), place(col, wide, LANES))]

            s = at(srcs[0])[...].astype(F32)
            for a in srcs[1:]:
                s = s + at(a)[...].astype(F32)
            at(dst)[...] = s.astype(BF16)
            return _

        if many > 1:
            lax.fori_loop(0, many, block, 0)
        else:
            block(0, 0)

    def squares(ref, lead, weight):
        rows, cols = ref.shape[len(lead):]
        for r in range(0, rows, SUBLANES):
            v = ref[(*lead, pl.ds(r, SUBLANES), slice(None))].astype(F32)
            v = v * v
            s = acc[...]
            for a in range(0, SUBLANES, BLOCK[0]):
                for b in range(0, cols, LANES):
                    s = s + weight * v[a : a + BLOCK[0], b : b + LANES]
            acc[...] = s

    def need(key):
        i, c, s = key
        if i < PARTS:
            if s == 0:
                loads[c].wait()
            return

        def wait(j, _):
            for t in tile_sends(j):
                t.wait_recv()
            return _

        lax.fori_loop((i - PARTS) * per, (i - PARTS + 1) * per, wait, 0)

    def local(l, k, src, dst):
        return pltpu.make_async_copy(src(), dst(), keep_sem.at[l, k])

    acc[...] = jnp.zeros_like(acc)
    xfers, events = plan((x, y, z, core), ((g1, u1, d1), own_ab, own_c, p_ab, p_c, r1, r2, r3, r4, rz, rc, rx, ry, f_ab, f_c, acc, (nz, ny, nx, nc),
                                           gu_out, dn_out, sq_out, total, squares, need, local), ru, cu)
    counts = sorted(t.count for t in xfers)
    ids = {id(t): k for k, t in enumerate(sorted(xfers, key=lambda t: t.count))}
    groups, _ = order_of(events, SLOTS)

    def copy_of(src, dst, k, dev):
        return pltpu.make_async_remote_copy(src_ref=src, dst_ref=dst, send_sem=send_sem.at[k], recv_sem=recv_sem.at[k], device_id=dev, device_id_type=LOGICAL)

    def wait_of(count, k):
        cols = next(c for c in range(NZ * cu, 0, -LANES) if count % (c * SUBLANES) == 0)
        some = p_ab.at[0, 0, pl.ds(0, count // cols), pl.ds(0, cols)]
        return copy_of(some, some, k, me)

    def emit(group):
        for e in group:
            for t in e.waits:
                wait_of(t.count, ids[id(t)]).wait_recv()
            e.work()
            for t in e.sends:
                copy_of(t.src(), t.dst(), ids[id(t)], t.dev).start()

    def choose(j, options):
        middle = len(options) // 2
        if middle == 0:
            emit(options[0])
        elif any(options):
            pl.when(j < middle)(lambda: choose(j, options[:middle]))
            pl.when(j >= middle)(lambda: choose(j - middle, options[middle:]))

    def steps(srcs, bufs, *parts):
        mine = groups[: TILES * len(parts)]
        del groups[: TILES * len(parts)]

        def copies(j, slot):
            return [pltpu.make_async_copy(src(j), buf.at[slot], tile_sem.at[slot, k]) for k, (src, buf) in enumerate(zip(srcs, bufs, strict=True))]

        for t in copies(0, 0):
            t.start()

        def step(j, carry):
            slot = rem(j, 2)
            for t in copies(j, slot):
                t.wait()

            @pl.when(j + 1 < TILES)
            def _():
                for t in copies(j + 1, 1 - slot):
                    t.start()

            for k, part in enumerate(parts):
                part(j, slot)
                choose(j, mine[k :: len(parts)])
            return carry

        lax.fori_loop(0, TILES, step, 0)

    emit(groups.pop(0))
    tail = groups.pop()
    groups.append([])

    rows_in, rows_out = (pl.ds(pl.multiple_of(c * HD, SUBLANES), HD) for c in (core, other))
    staged = lambda slot: [st_ab.at[slot, 0, rows_out, :], st_ab.at[slot, 1, rows_out, :], st_c.at[slot, :, yours]]
    blocks = [pl.ds(k * (n // 4), n // 4) for k in range(4)]

    def through(which, j, slot):
        if which == 0:
            @pl.when(j > 1)
            def _():
                for t in tile_sends(j - 2, staged(slot), slot):
                    t.wait_send()

        for rows in blocks[which::2]:
            dp = dot(dh[rows, :], wbuf[slot], NT).astype(BF16).astype(F32)
            p_s[rows, :], dg_s[rows, :], du_s[rows, :] = backward_tile(gbuf[slot, rows, :], ubuf[slot, rows, :], dp)

    def term(c, j, slot):
        i, cols = PARTS + div(j, per), slice_of(rem(j, per))
        if c < 2:
            st_ab[slot, c] = dot(a0_t[...], (dg_s, du_s)[c][...]).astype(BF16)
            own_ab[i, c, :, cols] = st_ab[slot, c, rows_in, :]
        else:
            st_c[slot] = dot(p_s[...], dh[...], TN).astype(BF16)
            own_c[i, cols, :] = st_c[slot, :, mine]
            for t in tile_sends(j, staged(slot), slot):
                t.start()

    steps([lambda j: gate.at[j], lambda j: up.at[j], lambda j: wd.at[0, slice_of(j), :]], [gbuf, ubuf, wbuf],
          *[functools.partial(f, k) for f, k in ((through, 0), (through, 1), (term, 0), (term, 1), (term, 2))])
    for k in range(2):
        for t in tile_sends(TILES - 2 + k, staged(k), k):
            t.wait_send()
    emit(tail)
    for count in sorted(set(counts)):
        def wait(k, carry, count=count):
            wait_of(count, k).wait_send()
            return carry

        lax.fori_loop(counts.index(count), counts.index(count) + counts.count(count), wait, 0)


def gradient_sums(g1, u1, d1, a0_t, dh, gate, up, wd):
    (n, d), ff = dh.shape, g1.shape[1]
    ru, cu = d // SUBLANES, ff // NZ // PARTS
    HD, CR, fs, N, tile = d // 2, cu // 2, ff // PARTS, 2 * PARTS, ff // TILES
    V = lambda *s: pltpu.VMEM(s, BF16)
    W = lambda *s: pltpu.VMEM(s, F32)
    DMA = lambda *s: pltpu.SemaphoreType.DMA(s)
    return pl.pallas_call(
        functools.partial(sum_kernel, ru, cu),
        name="gradient_sums",
        out_shape=(jax.ShapeDtypeStruct((2, 2, d, ff), BF16), jax.ShapeDtypeStruct((2, ff, d), BF16), jax.ShapeDtypeStruct(BLOCK, F32)),
        in_specs=[ANY] * 3 + [VMEM] * 2 + [ANY] * 3,
        out_specs=(ANY, ANY, VMEM),
        scratch_shapes=[
            V(N, 2, HD, fs), V(N, fs, HD), V(N, 2, HD, fs), V(N, fs, HD),
            V(N, 2, 2, 2 * ru, fs), V(N, 2, 2, ru, fs), V(N, 2, 2, ru, fs // 2), V(N, 2, 2, ru, fs // 4),
            V(N, NZ - 1, ru, cu), V(N, 2, NZ - 1, CR, HD), V(N, 2, NX - 1, CR // 4, HD), V(N, 2, NY, CR // 4, HD), V(N, ru, cu), V(N, 2, CR // 4, HD),
            W(*BLOCK), W(NZ, *BLOCK), W(NY, *BLOCK), W(NX, *BLOCK), W(CORES, *BLOCK),
            W(2, n, tile), W(2, n, tile), V(2, tile, d), V(n, tile), V(n, tile), V(n, tile), V(2, 2, d, tile), V(2, tile, d),
            DMA(NUMBER_OF_XFERS), DMA(NUMBER_OF_XFERS), DMA(3), DMA(N, 3), DMA(2, 3), DMA(2, 3), DMA(TILES, 3),
        ],
        compiler_params=pltpu.CompilerParams(collective_id=0, has_side_effects=True, vmem_limit_bytes=62 << 20),
    )(g1, u1, d1, a0_t, dh, gate, up, wd)


def adamw(w, m, v, g):
    m = 0.9 * m + 0.1 * g
    v = 0.95 * v + 0.05 * g * g
    step = m * lax.rsqrt(v + 1e-8) + 0.1 * w
    return (w - 0.02 * step).astype(BF16), m, v


def solution(mesh):
    def step(x, dy, *arrays):
        weights, m, v = (arrays[i : i + 3] for i in (0, 3, 6))
        gate, up, a0_t, dh, *by_1 = layers(x[0], dy[0], *weights)
        gu, down, squares = gradient_sums(*by_1, a0_t, dh, gate, up, weights[2])
        gradients = [gu[0], gu[1], down]
        count = sum(g.size for g in gradients)
        factor = jnp.minimum(1.0, 0.5 * lax.rsqrt(squares[0, 0] / count + 1e-30))
        new = [adamw(w.astype(F32), m, v, g.astype(F32) * factor) for w, m, v, g in zip(weights, m, v, gradients, strict=True)]
        return tuple(one[which] for which in range(3) for one in new)

    whole = P(None, None, None)
    return jax.shard_map(
        step,
        mesh=mesh,
        in_specs=(P(("rep", "dp"), None, None),) * 2 + (whole,) * 9,
        out_specs=(P("rep", None, None),) * 9,
        check_vma=False,
    )
```
